128 devices in a mesh: blk: 32 (over y, x, core), rep: 4 (over z).
Axes of the slice: x: 4, y: 4, z: 4, core: 2. Of those that a mesh axis runs over, the one named last changes fastest.
Arguments:
- anchors: float32 [3, 81920], P(None, ('blk', 'rep')), may hold values from -1 to 1
- directions: float32 [3, 81920], P(None, ('blk', 'rep')), may hold values from -4 to 4
- app_ids: int32 [81920], P(('blk', 'rep')), may hold values from 0 to 8191
- block_ids: int32 [640, 3], P(('blk', 'rep')), may hold values from 0 to 31, as said below
- color_grad: float32 [3, 81920], P(None, ('blk', 'rep')), may hold values from -6 to 6
- block_centers: float32 [3, 32], P(None, 'blk'), may hold values from -1 to 1
- pos_weight: bfloat16 [32, 256, 63], P('blk'), may hold values from -1 to 1
- trunk_weight: bfloat16 [32, 2, 256, 256], P('blk'), may hold values from -0.5 to 0.5
- density_weight: bfloat16 [32, 256], P('blk'), may hold values from -0.5 to 0.5
- feature_weight: bfloat16 [32, 128, 256], P('blk'), may hold values from -0.5 to 0.5
- view_weight: bfloat16 [32, 128, 27], P('blk'), may hold values from -1.25 to 1.25
- code_weight: bfloat16 [32, 128, 32], P('blk'), may hold values from -1 to 1
- radiance_weight: bfloat16 [32, 3, 128], P('blk'), may hold values from -0.75 to 0.75
- code_table: bfloat16 [32, 32, 8192], P('blk'), may hold values from -5 to 5
Outputs:
- colors: float32 [3, 81920], P(None, ('blk', 'rep'))
- grad_pos_weight: float32 [32, 256, 63], P('blk')
- grad_trunk_weight: float32 [32, 2, 256, 256], P('blk')
- grad_density_weight: float32 [32, 256], P('blk')
- grad_feature_weight: float32 [32, 128, 256], P('blk')
- grad_view_weight: float32 [32, 128, 27], P('blk')
- grad_code_weight: float32 [32, 128, 32], P('blk')
- grad_radiance_weight: float32 [32, 3, 128], P('blk')
- grad_code_table: float32 [32, 32, 8192], P('blk')
The draws below stay inside these ranges and needn't reach their ends.
Inputs may be any that keep to these rules, and one draw needn't show every extreme that they name: `block_ids`: each tile names three different blocks; the tiles of one device never name the same block twice; among the devices that share an index along rep, every block is named by at most 30 tiles, and some block by exactly 30 tiles.
All inputs are finite; a program needn't handle non-finite values.
Results may differ from the reference program's by a relative error of at most 0.015.
Values sent between devices are 32-bit elements; how exact they have to be, the bound alone decides.
A program may use at most 64 MiB of HBM per device.

```python
import jax
import jax.numpy as jnp
from jax import lax

TILE = 128
SAMPLES = 4
HID = 256
DEPTH = 2
CHID = 128
FREQ = 10
VFREQ = 4
E = 32
APP = 8192
ENC = 63
VENC = 27
BLOCKS = 32
TILES_DEV = 5
LOAD = 30
RAYS = 81920
N_BLK = 32
N_REP = 4


def draw_block_ids(key, part):
    per_device = 3 * TILES_DEV
    block_range = jnp.arange(N_BLK, dtype=jnp.int32)

    def one_group(group_index):
        group_key = jax.random.fold_in(key, group_index + 17)
        group_keys = jax.random.split(group_key, 5)
        hottest = jax.random.randint(group_keys[0], (), 0, N_BLK)
        source_order = jax.random.permutation(group_keys[2], N_BLK)
        jitter = jax.random.randint(group_keys[3], (N_BLK, N_BLK), 0, 1 << 14)

        def choose(remaining, step_index):
            scores = (remaining > 0).astype(jnp.int32) * (1 << 28) + ((block_range == hottest) & (remaining > 0)).astype(jnp.int32) * (1 << 27) + jnp.maximum(remaining, 0) * (1 << 20) + jitter[step_index] * 64 + block_range
            _, chosen = lax.top_k(scores, per_device)
            chosen = chosen.astype(jnp.int32)
            used_now = jnp.sum((chosen[:, None] == block_range[None, :]).astype(jnp.int32), 0)
            shuffled = jax.random.permutation(jax.random.fold_in(group_keys[4], step_index), chosen)
            return (remaining - used_now, shuffled)
        _, chosen_all = lax.scan(choose, jnp.full((N_BLK,), LOAD, jnp.int32), jnp.arange(N_BLK, dtype=jnp.int32))
        return jnp.zeros((N_BLK, per_device), jnp.int32).at[source_order].set(chosen_all)
    groups = lax.map(one_group, jnp.arange(N_REP, dtype=jnp.int32))
    return groups.transpose(1, 0, 2).reshape(N_BLK * N_REP * TILES_DEV, 3)


def plant(result, key, low, top_value):
    longest = result.shape.index(max(result.shape))
    spots = []
    for shift in (0, 1):
        where = [jax.random.randint(jax.random.fold_in(key, axis), (), 0, length) for axis, length in enumerate(result.shape)]
        where[longest] = (where[longest] + shift) % result.shape[longest]
        spots.append(tuple(where))
    return result.at[spots[0]].set(low).at[spots[1]].set(top_value)


def block_levels(key, dims, cuts, least, largest):
    factor_of, own = 1.0, jax.random.fold_in(key, 6)
    for position, parts in cuts:
        draws = jnp.exp(jax.random.uniform(jax.random.fold_in(own, position), (parts,), jnp.float32, least / len(cuts), largest / len(cuts)))
        factor_of = factor_of * jnp.repeat(draws, dims[position] // parts).reshape([-1 if axis == position else 1 for axis in range(len(dims))])
    return factor_of


def gaussian(stream_key, extent, deviation, reach, shards=(), kind=jnp.bfloat16):
    loudness = block_levels(stream_key, extent, shards, -0.22, 0.18) if shards else 1.0
    values = jax.random.normal(stream_key, extent, jnp.float32) * deviation * loudness
    return jnp.minimum(jnp.maximum(values, -reach), reach).astype(kind)


def setup_inputs(seed: int = 0) -> dict:
    arg_keys = jax.random.split(jax.random.key(seed), 15)
    anchors = jnp.clip(jax.random.uniform(arg_keys[0], (3, RAYS), jnp.float32, -1.0, 1.0) * block_levels(arg_keys[0], (3, RAYS), ((1, 128),), -0.4, 0.0), -1.0, 1.0)
    directions = gaussian(arg_keys[1], (3, RAYS), 0.7, 4.0, ((1, 128),), jnp.float32)
    app_ids = plant(jax.random.randint(arg_keys[2], (RAYS,), 0, APP), jax.random.fold_in(arg_keys[2], 1), 0, APP - 1).astype(jnp.int32)
    block_ids = draw_block_ids(jax.random.fold_in(arg_keys[14], 71), 0)
    color_grad = gaussian(arg_keys[4], (3, RAYS), 1.0, 6.0, ((1, 128),), jnp.float32)
    block_centers = jnp.clip(jax.random.uniform(arg_keys[5], (3, BLOCKS), jnp.float32, -1.0, 1.0) * block_levels(arg_keys[5], (3, BLOCKS), ((1, 32),), -0.4, 0.0), -1.0, 1.0)
    pos_weight = gaussian(arg_keys[6], (BLOCKS, HID, ENC), (ENC // 2) ** -0.5, 1.0, ((0, 32),))
    trunk_weight = gaussian(arg_keys[7], (BLOCKS, DEPTH, HID, HID), (HID // 2) ** -0.5, 0.5, ((0, 32),))
    density_weight = gaussian(arg_keys[8], (BLOCKS, HID), (HID // 2) ** -0.5, 0.5, ((0, 32),))
    feature_weight = gaussian(arg_keys[9], (BLOCKS, CHID, HID), (HID // 2) ** -0.5, 0.5, ((0, 32),))
    view_weight = gaussian(arg_keys[10], (BLOCKS, CHID, VENC), VENC ** -0.5, 1.25, ((0, 32),))
    code_weight = gaussian(arg_keys[11], (BLOCKS, CHID, E), E ** -0.5, 1.0, ((0, 32),))
    radiance_weight = gaussian(arg_keys[12], (BLOCKS, 3, CHID), (CHID // 2) ** -0.5, 0.75, ((0, 32),))
    code_table = gaussian(arg_keys[13], (BLOCKS, E, APP), 1.0, 5.0, ((0, 32),))
    return {"anchors": anchors, "directions": directions, "app_ids": app_ids, "block_ids": block_ids, "color_grad": color_grad, "block_centers": block_centers, "pos_weight": pos_weight, "trunk_weight": trunk_weight, "density_weight": density_weight, "feature_weight": feature_weight, "view_weight": view_weight, "code_weight": code_weight, "radiance_weight": radiance_weight, "code_table": code_table}


ray_span = 2.0
loss_scale = 0.03125

def encode(values, levels):
    scales = 2.0 ** jnp.arange(levels).astype(values.dtype)
    angles = (scales[:, None, None] * values[None]).reshape(levels * 3, values.shape[1])
    return jnp.concatenate([values, jnp.sin(angles), jnp.cos(angles)], 0)

def render(params, code_block, center, anchor, direction, codes_row):
    pos_weight, trunk_weight, density_weight, feature_weight, view_weight, code_weight, radiance_weight = params
    ray_count = anchor.shape[1]
    spacing = ray_span / SAMPLES
    depths = (jnp.arange(SAMPLES).astype(anchor.dtype) + 0.5) * spacing
    points = anchor[:, None, :] + depths[None, :, None] * direction[:, None, :] - center[:, None, None]
    points = points.reshape(3, SAMPLES * ray_count)
    pos_code = encode(points, FREQ).astype(jnp.bfloat16)
    hidden = jax.nn.softplus(jnp.dot(pos_weight, pos_code, preferred_element_type=jnp.float32)).astype(jnp.bfloat16)
    for level_index in range(trunk_weight.shape[0]):
        hidden = jax.nn.softplus(jnp.dot(trunk_weight[level_index], hidden, preferred_element_type=jnp.float32)).astype(jnp.bfloat16)
    density = jax.nn.softplus(jnp.dot(density_weight[None, :], hidden, preferred_element_type=jnp.float32)).reshape(SAMPLES, ray_count)
    view_code = encode(direction, VFREQ).astype(jnp.bfloat16)
    app_code = jnp.take(code_block, codes_row.astype(jnp.int32), axis=1)
    per_ray = jnp.dot(view_weight, view_code, preferred_element_type=jnp.float32) + jnp.dot(code_weight, app_code, preferred_element_type=jnp.float32)
    feature = jnp.dot(feature_weight, hidden, preferred_element_type=jnp.float32).reshape(-1, SAMPLES, ray_count)
    shaded = jax.nn.softplus(feature + per_ray[:, None, :]).astype(jnp.bfloat16).reshape(-1, SAMPLES * ray_count)
    radiance = jax.nn.sigmoid(jnp.dot(radiance_weight, shaded, preferred_element_type=jnp.float32)).reshape(3, SAMPLES, ray_count)
    optical = density * spacing
    passed = jnp.exp(-(jnp.cumsum(optical, 0) - optical))
    sample_weight = passed * (1.0 - jnp.exp(-optical))
    ray_color = lax.optimization_barrier(jnp.sum(sample_weight[None] * radiance, 1))
    opacity = lax.optimization_barrier(jnp.sum(sample_weight, 0))
    offset = anchor - center[:, None]
    blend_weight = (0.1 + opacity) / (1.0 + lax.optimization_barrier(jnp.sum(offset * offset, 0)))
    return jnp.concatenate([ray_color * blend_weight[None], blend_weight[None]], 0)

def blend_colors(partials):
    return partials[:, :3] / partials[:, 3:4]

def reference(anchors, directions, app_ids, block_ids, color_grad, block_centers, pos_weight, trunk_weight, density_weight, feature_weight, view_weight, code_weight, radiance_weight, code_table):
    float_type = anchors.dtype
    tile_count = block_ids.shape[0]
    ray_tiles = jnp.concatenate([anchors, directions], 0).reshape(6, tile_count, TILE).transpose(1, 0, 2)
    code_tiles = app_ids.astype(jnp.int32).reshape(tile_count, TILE)
    block_rows = block_ids.astype(jnp.int32)
    grad_tiles = color_grad.reshape(3, tile_count, TILE).transpose(1, 0, 2)
    every_block = (pos_weight, trunk_weight, density_weight, feature_weight, view_weight, code_weight, radiance_weight)

    def block_params(block_index):
        return tuple((member[block_index] for member in every_block))

    def forward_tile(inputs):
        ray_rows, codes_row, blocks_row = inputs
        running = jnp.zeros((4, TILE), float_type)
        for slot_index in range(3):
            block_index = blocks_row[slot_index].astype(jnp.int32)
            piece = render(block_params(block_index), code_table[block_index], block_centers[:, block_index], ray_rows[:3], ray_rows[3:], codes_row)
            running = running + piece.astype(float_type)
        return running
    partials = lax.map(forward_tile, (ray_tiles, code_tiles, block_rows))
    ray_colors, pullback = jax.vjp(blend_colors, partials)
    cot_parts, = pullback((grad_tiles * loss_scale).astype(partials.dtype))

    def backward_tile(totals, inputs):
        ray_rows, codes_row, blocks_row, cot_row = inputs
        for slot_index in range(3):
            block_index = blocks_row[slot_index].astype(jnp.int32)
            center = block_centers[:, block_index]

            def local_render(weights, code_block):
                return render(weights, code_block, center, ray_rows[:3], ray_rows[3:], codes_row)
            _, pull_back = jax.vjp(local_render, block_params(block_index), code_table[block_index])
            grad_params, grad_block = pull_back(cot_row)
            pieces = tuple(grad_params) + (grad_block,)
            totals = tuple((running.at[block_index].add(piece_grad.astype(running.dtype)) for running, piece_grad in zip(totals, pieces)))
        return (totals, None)
    start = tuple((jnp.zeros(member.shape, float_type) for member in every_block + (code_table,)))
    totals, _ = lax.scan(backward_tile, start, (ray_tiles, code_tiles, block_rows, cot_parts))
    colors = ray_colors.transpose(1, 0, 2).reshape(3, tile_count * TILE)
    return (colors, totals[0], totals[1], totals[2], totals[3], totals[4], totals[5], totals[6], totals[7])
```

```python
import numpy as np

import jax
import jax.numpy as jnp
from jax import lax
from jax.experimental import pallas as pl
from jax.experimental.pallas import tpu as pltpu
from jax.sharding import PartitionSpec as P

TILE = 128
SAMPLES = 4
SLOTS = 32
LANES = SAMPLES * TILE
HID = 256
CHID = 128
PC = 96
VC = 48
E = 32
RC = VC + E
LO = 256
SPACING = 0.5
LOSS_SCALE = 0.03125
LOG2E = 1.4426950408889634
LN2 = 0.6931471805599453

R_H1 = PC
R_H2 = R_H1 + HID
R_H3 = R_H2 + HID
R_S = R_H3 + HID
R_END = R_S + CHID

G_T1 = 0
G_T2 = 256
G_FD = 512
G_TAB = 656
G_POS = 1680
G_ROWS = 1984


def code_places(levels, half):
    raw = list(range(3))
    sines, cosines = [], []
    for level in range(levels):
        for c in range(3):
            row = (level // half) * 3 + c
            group = 2 * (level % half)
            sines.append(8 * (1 + group) + row)
            cosines.append(8 * (2 + group) + row)
    return raw + sines + cosines


def selection(places, width):
    out = np.zeros((len(places), width), np.float32)
    out[np.arange(len(places)), places] = 1.0
    return out


POS_SELECT = selection(code_places(10, 5), PC)
VIEW_SELECT = selection(code_places(4, 2), VC)


def mm(a, b):
    return lax.dot_general(a, b, (((1,), (0,)), ((), ())), preferred_element_type=jnp.float32)


def mm_nt(a, b):
    return lax.dot_general(a, b, (((1,), (1,)), ((), ())), preferred_element_type=jnp.float32)


def softplus(v):
    return jnp.maximum(v, 0.0) + jnp.log(1.0 + jnp.exp(-jnp.abs(v)))


def row_iota(rows, lanes):
    return lax.broadcasted_iota(jnp.int32, (rows, lanes), 0)


def ray_rows(ray, row):
    o8 = jnp.where(row < 3, ray, jnp.where(row < 6, pltpu.roll(ray, 3, 0), 0.0))
    d8 = jnp.where(row < 3, pltpu.roll(ray, 5, 0), jnp.where(row < 6, ray, 0.0))
    return o8, d8


def center_rows(center_ref, row):
    third = jnp.where(row >= 3, row - 3, row)
    return jnp.where(
        third == 0,
        center_ref[0, 0],
        jnp.where(third == 1, center_ref[1, 0], jnp.where(third == 2, center_ref[2, 0], 0.0)),
    )


def code_groups(values, doublings):
    groups = [values]
    sine, cosine = jnp.sin(values), jnp.cos(values)
    for step in range(doublings):
        groups += [sine, cosine]
        if step + 1 < doublings:
            sine, cosine = 2.0 * sine * cosine, (cosine - sine) * (cosine + sine)
    groups.append(jnp.zeros_like(values))
    return jnp.concatenate(groups, 0).astype(jnp.bfloat16)


def over_samples(x):
    return [x[:, s * TILE : (s + 1) * TILE] for s in range(SAMPLES)]


def composite(small, o8, c8, row):
    density = over_samples(softplus(small))
    rad = over_samples(1.0 / (1.0 + jnp.exp(-small)))
    off = o8 - c8
    off2 = jnp.sum(jnp.where(row < 3, off * off, 0.0), 0, keepdims=True)
    inv = 1.0 / (1.0 + off2)
    depth = jnp.zeros((1, TILE), jnp.float32)
    before = jnp.ones((1, TILE), jnp.float32)
    weights, after = [], []
    for s in range(SAMPLES):
        u = density[s][3:4] * SPACING
        weights.append(before * (1.0 - jnp.exp(-u)))
        depth = depth + u
        before = jnp.exp(-depth)
        after.append(before)
    color = sum(w * r for w, r in zip(weights, rad))
    opacity = sum(weights)
    return rad, weights, after, color, (0.1 + opacity) * inv, inv


def forward_kernel(
    live_ref, center_ref, rays_ref, pos_ref, trunk_ref, density_ref, feature_ref, view_ref,
    code_ref, radiance_ref, table_ref, pos_select_ref, view_select_ref,
    part_ref, saved_ref, raycode_ref, small_ref,
    wp, wfd, wray, wrad, tab, buf, sem,
):
    row = row_iota(8, TILE)
    c8 = center_rows(center_ref, row)
    wp[...] = mm(pos_ref[0], pos_select_ref[...]).astype(jnp.bfloat16)
    wray[:, :VC] = mm(view_ref[0], view_select_ref[...]).astype(jnp.bfloat16)
    wray[:, VC:] = code_ref[0]
    wfd[:CHID, :] = feature_ref[0]
    row16 = row_iota(16, HID)
    wfd[CHID:, :] = jnp.where(row16 == 3, density_ref[...].astype(jnp.float32), 0.0).astype(jnp.bfloat16)
    wrad[...] = jnp.concatenate(
        [radiance_ref[0].astype(jnp.float32), jnp.zeros((5, CHID), jnp.float32)], 0
    ).astype(jnp.bfloat16)
    for h in range(SLOTS):
        tab[h * E : (h + 1) * E, :] = table_ref[0, :, h * LO : (h + 1) * LO]
    pos_scale = jnp.where(row < 3, 1.0, 32.0)
    view_scale = jnp.where(row < 3, 1.0, 4.0)

    def saving(count):
        slot = count % 2
        return pltpu.make_async_copy(buf.at[slot], saved_ref.at[count], sem.at[slot])

    def tile(s, count):
        @pl.when(count >= 2)
        def _():
            saving(count - 2).wait()

        out = buf.at[count % 2]
        ray = rays_ref[s]
        o8, d8 = ray_rows(ray, row)
        points = jnp.concatenate(
            [(o8 + (t + 0.5) * SPACING * d8 - c8) * pos_scale for t in range(SAMPLES)], 1
        )
        out[:PC, :] = code_groups(points, 5)
        ids = ray[6:7].astype(jnp.int32)
        lo, hi = ids & (LO - 1), ids >> 8
        hot = (row_iota(LO, TILE) == lo).astype(jnp.float32).astype(jnp.bfloat16)
        rows = mm(tab[...], hot)
        app = jnp.zeros((E, TILE), jnp.float32)
        for h in range(SLOTS):
            app = app + jnp.where(hi == h, rows[h * E : (h + 1) * E], 0.0)
        raycode_ref[s, :VC, :] = code_groups(d8 * view_scale, 2)
        raycode_ref[s, VC:, :] = app.astype(jnp.bfloat16)
        per_ray = mm(wray[...], raycode_ref[s])
        out[R_H1:R_H2, :] = softplus(mm(wp[...], out[:PC, :])).astype(jnp.bfloat16)
        out[R_H2:R_H3, :] = softplus(mm(trunk_ref[0, 0], out[R_H1:R_H2, :])).astype(jnp.bfloat16)
        out[R_H3:R_S, :] = softplus(mm(trunk_ref[0, 1], out[R_H2:R_H3, :])).astype(jnp.bfloat16)
        both = mm(wfd[...], out[R_H3:R_S, :])
        out[R_S:R_END, :] = softplus(
            both[:CHID] + jnp.concatenate([per_ray] * SAMPLES, 1)
        ).astype(jnp.bfloat16)
        logits = mm(wrad[...], out[R_S:R_END, :])
        small = jnp.where(row_iota(8, LANES) == 3, both[CHID : CHID + 8], logits)
        small_ref[s] = small
        _, _, _, color, share, _ = composite(small, o8, c8, row)
        part_ref[s] = jnp.where(row < 3, color * share, share)[:4]
        saving(count).start()
        return count + 1

    def step(s, count):
        return lax.cond(live_ref[s] > 0, lambda: tile(s, count), lambda: count)

    count = lax.fori_loop(0, SLOTS, step, jnp.int32(0))

    @pl.when(count >= 2)
    def _():
        saving(count - 2).wait()

    @pl.when(count >= 1)
    def _():
        saving(count - 1).wait()


def backward_kernel(
    live_ref, center_ref, rays_ref, cot_ref, saved_ref, raycode_ref, small_ref, trunk_ref,
    density_ref, feature_ref, code_ref, radiance_ref,
    g_ref,
    t1, t2, fdt, codet, radt, buf, slots, sem,
):
    row = row_iota(8, TILE)
    c8 = center_rows(center_ref, row)

    def flip(x):
        return x.astype(jnp.float32).T.astype(jnp.bfloat16)

    t1[...] = flip(trunk_ref[0, 0])
    t2[...] = flip(trunk_ref[0, 1])
    fdt[:, :CHID] = flip(feature_ref[0])
    row16 = row_iota(16, HID)
    fdt[:, CHID:] = jnp.where(row16 == 3, density_ref[...].astype(jnp.float32), 0.0).T.astype(jnp.bfloat16)
    codet[...] = flip(code_ref[0])
    radt[...] = jnp.concatenate(
        [radiance_ref[0].astype(jnp.float32), jnp.zeros((13, CHID), jnp.float32)], 0
    ).T.astype(jnp.bfloat16)
    g_ref[...] = jnp.zeros_like(g_ref)

    def listing(s, count):
        @pl.when(live_ref[s] > 0)
        def _():
            slots[count] = s

        return count + (live_ref[s] > 0).astype(jnp.int32)

    total = lax.fori_loop(0, SLOTS, listing, jnp.int32(0))

    def fetching(j):
        return pltpu.make_async_copy(saved_ref.at[j], buf.at[j % 2], sem.at[j % 2])

    @pl.when(total > 0)
    def _():
        fetching(0).start()

    def tile(j, carry):
        s = slots[j]
        fetching(j).wait()

        @pl.when(j + 1 < total)
        def _():
            fetching(j + 1).start()

        act = buf.at[j % 2]
        ray = rays_ref[s]
        o8, _ = ray_rows(ray, row)
        small = small_ref[s]
        rad, weights, after, color, share, inv = composite(small, o8, c8, row)
        cot = jnp.concatenate([cot_ref[s], jnp.zeros((4, TILE), jnp.float32)], 0)
        d_share = jnp.sum(
            jnp.where(row < 3, cot * color, jnp.where(row == 3, cot, 0.0)), 0, keepdims=True
        )
        d_color = jnp.where(row < 3, cot * share, 0.0)
        d_opacity = d_share * inv
        sig = over_samples(1.0 / (1.0 + jnp.exp(-small)))
        later = jnp.zeros((1, TILE), jnp.float32)
        pieces = [None] * SAMPLES
        for t in reversed(range(SAMPLES)):
            d_w = jnp.sum(d_color * rad[t], 0, keepdims=True) + d_opacity
            d_u = d_w * after[t] - later
            later = later + d_w * weights[t]
            d_logit = d_color * weights[t] * rad[t] * (1.0 - rad[t])
            pieces[t] = jnp.where(
                row < 3, d_logit, jnp.where(row == 3, d_u * SPACING * sig[t], 0.0)
            )
        d_small = jnp.concatenate(pieces, 1)
        d_small = jnp.concatenate([d_small, jnp.zeros_like(d_small)], 0).astype(jnp.bfloat16)

        def through(grad, lo_row, hi_row):
            value = act[lo_row:hi_row, :].astype(jnp.float32)
            return grad * (1.0 - jnp.exp(-value))

        shaded = act[R_S:R_END, :]
        d_feature = through(mm(radt[...], d_small), R_S, R_END)
        g_ref[G_POS + CHID : G_POS + CHID + 16, 128:256] += mm_nt(d_small, shaded)
        d_ray = sum(over_samples(d_feature)).astype(jnp.bfloat16)
        g_ref[G_POS : G_POS + CHID, 128 : 128 + RC] += mm_nt(d_ray, raycode_ref[s])
        d_app = mm(codet[...], d_ray)
        ids = ray[6:7].astype(jnp.int32)
        lo, hi = ids & (LO - 1), ids >> 8
        hot = (row_iota(LO, TILE) == lo).astype(jnp.float32).astype(jnp.bfloat16)
        spread = jnp.concatenate(
            [jnp.where(hi == h, d_app, 0.0).astype(jnp.bfloat16) for h in range(SLOTS)], 0
        )
        g_ref[G_TAB:G_POS, :] += mm_nt(spread, hot)
        both = jnp.concatenate([d_feature.astype(jnp.bfloat16), d_small], 0)
        g_ref[G_FD:G_TAB, :] += mm_nt(both, act[R_H3:R_S, :])
        d_z = through(mm(fdt[...], both), R_H3, R_S).astype(jnp.bfloat16)
        g_ref[G_T2:G_FD, :] += mm_nt(d_z, act[R_H2:R_H3, :])
        d_z = through(mm(t2[...], d_z), R_H2, R_H3).astype(jnp.bfloat16)
        g_ref[G_T1:G_T2, :] += mm_nt(d_z, act[R_H1:R_H2, :])
        d_z = through(mm(t1[...], d_z), R_H1, R_H2).astype(jnp.bfloat16)
        g_ref[G_POS : G_POS + HID, :PC] += mm_nt(d_z, act[:PC, :])
        return carry

    lax.fori_loop(0, total, tile, jnp.int32(0))


def unpack_kernel(
    g_ref, pos_select_ref, view_select_ref,
    pos_ref, trunk_ref, density_ref, feature_ref, view_ref, code_ref, radiance_ref, table_ref,
):
    def pick(a, select):
        return lax.dot_general(
            a, select.astype(jnp.float32), (((1,), (1,)), ((), ())),
            preferred_element_type=jnp.float32, precision=lax.Precision.HIGHEST,
        )

    pos_ref[0] = pick(g_ref[G_POS : G_POS + HID, :PC], pos_select_ref[...])
    trunk_ref[0, 0] = g_ref[G_T1:G_T2, :]
    trunk_ref[0, 1] = g_ref[G_T2:G_FD, :]
    feature_ref[0] = g_ref[G_FD : G_FD + CHID, :]
    density_ref[...] = g_ref[G_FD + CHID + 3 : G_FD + CHID + 4, :]
    view_ref[0] = pick(g_ref[G_POS : G_POS + CHID, 128 : 128 + VC], view_select_ref[...])
    code_ref[0] = g_ref[G_POS : G_POS + CHID, 128 + VC : 128 + RC]
    radiance_ref[0] = g_ref[G_POS + CHID : G_POS + CHID + 3, 128:256]
    for h in range(SLOTS):
        table_ref[0, :, h * LO : (h + 1) * LO] = g_ref[G_TAB + h * E : G_TAB + (h + 1) * E, :]


VMEM = pl.BlockSpec(memory_space=pltpu.VMEM)
SMEM = pl.BlockSpec(memory_space=pltpu.SMEM)
ANY = pl.BlockSpec(memory_space=pl.ANY)


def run_forward(live, center, rays, pos, trunk, density, feature, view, code, radiance, table):
    bf = jnp.bfloat16
    return pl.pallas_call(
        forward_kernel,
        name="forward_tiles",
        out_shape=(
            jax.ShapeDtypeStruct((SLOTS, 4, TILE), jnp.float32),
            jax.ShapeDtypeStruct((SLOTS, R_END, LANES), bf),
            jax.ShapeDtypeStruct((SLOTS, RC, TILE), bf),
            jax.ShapeDtypeStruct((SLOTS, 8, LANES), jnp.float32),
        ),
        in_specs=[SMEM, SMEM] + [VMEM] * 11,
        out_specs=(VMEM, ANY, VMEM, VMEM),
        scratch_shapes=[
            pltpu.VMEM((HID, PC), bf),
            pltpu.VMEM((CHID + 16, HID), bf),
            pltpu.VMEM((CHID, RC), bf),
            pltpu.VMEM((8, CHID), bf),
            pltpu.VMEM((SLOTS * E, LO), bf),
            pltpu.VMEM((2, R_END, LANES), bf),
            pltpu.SemaphoreType.DMA((2,)),
        ],
        compiler_params=pltpu.CompilerParams(vmem_limit_bytes=32 * 1024 * 1024),
        cost_estimate=pl.CostEstimate(flops=10**10, bytes_accessed=3 * 10**7, transcendentals=0),
    )(live, center, rays, pos, trunk, density, feature, view, code, radiance, table,
      jnp.asarray(POS_SELECT, bf), jnp.asarray(VIEW_SELECT, bf))


def run_backward(live, center, rays, cot, saved, raycode, small, trunk, density, feature, code, radiance):
    bf = jnp.bfloat16
    return pl.pallas_call(
        backward_kernel,
        name="backward_tiles",
        out_shape=jax.ShapeDtypeStruct((G_ROWS, 256), jnp.float32),
        in_specs=[SMEM, SMEM, VMEM, VMEM, ANY] + [VMEM] * 7,
        out_specs=VMEM,
        scratch_shapes=[
            pltpu.VMEM((HID, HID), bf),
            pltpu.VMEM((HID, HID), bf),
            pltpu.VMEM((HID, CHID + 16), bf),
            pltpu.VMEM((E, CHID), bf),
            pltpu.VMEM((CHID, 16), bf),
            pltpu.VMEM((2, R_END, LANES), bf),
            pltpu.SMEM((SLOTS,), jnp.int32),
            pltpu.SemaphoreType.DMA((2,)),
        ],
        compiler_params=pltpu.CompilerParams(vmem_limit_bytes=32 * 1024 * 1024),
        cost_estimate=pl.CostEstimate(flops=2 * 10**10, bytes_accessed=3 * 10**7, transcendentals=0),
    )(live, center, rays, cot, saved, raycode, small, trunk, density, feature, code, radiance)


def run_unpack(packed):
    f32 = jnp.float32
    shapes = [(1, 256, 63), (1, 2, 256, 256), (1, 256), (1, 128, 256), (1, 128, 27), (1, 128, 32),
              (1, 3, 128), (1, 32, 8192)]
    return pl.pallas_call(
        unpack_kernel,
        name="unpack_gradients",
        out_shape=tuple(jax.ShapeDtypeStruct(s, f32) for s in shapes),
        in_specs=[VMEM] * 3,
        out_specs=tuple(VMEM for _ in shapes),
        compiler_params=pltpu.CompilerParams(vmem_limit_bytes=32 * 1024 * 1024),
    )(packed, jnp.asarray(POS_SELECT, jnp.bfloat16), jnp.asarray(VIEW_SELECT, jnp.bfloat16))


def local(
    anchors, directions, app_ids, block_ids, color_grad, block_centers, pos_weight, trunk_weight,
    density_weight, feature_weight, view_weight, code_weight, radiance_weight, code_table,
):
    tiles = block_ids.shape[0]
    peers = jnp.arange(SLOTS, dtype=jnp.int32)
    flat_ids = block_ids.reshape(-1)
    matches = (flat_ids[None, :] == peers[:, None]).astype(jnp.int32)
    is_live = jnp.sum(matches, 1)
    source_tile = jnp.sum(matches * jnp.arange(3 * tiles, dtype=jnp.int32)[None, :], 1) // 3
    rows = jnp.concatenate(
        [anchors, directions, app_ids.astype(jnp.float32)[None], jnp.zeros((1, tiles * TILE), jnp.float32)], 0
    )
    ray_tiles = rows.reshape(8, tiles, TILE).transpose(1, 0, 2)
    send = jnp.where(
        jnp.arange(8)[None, :, None] == 7,
        is_live.astype(jnp.float32)[:, None, None],
        ray_tiles[source_tile],
    )
    rays = lax.all_to_all(send, "blk", split_axis=0, concat_axis=0, tiled=True)
    live = (rays[:, 7, 0] > 0.5).astype(jnp.int32)
    part, saved, raycode, small = run_forward(
        live, block_centers, rays, pos_weight, trunk_weight, density_weight, feature_weight,
        view_weight, code_weight, radiance_weight, code_table,
    )
    returned = lax.all_to_all(part, "blk", split_axis=0, concat_axis=0, tiled=True)
    summed = returned[block_ids[:, 0]] + returned[block_ids[:, 1]] + returned[block_ids[:, 2]]
    scaled = color_grad.reshape(3, tiles, TILE).transpose(1, 0, 2) * LOSS_SCALE
    colors = summed[:, :3] / summed[:, 3:4]
    cot_color = scaled / summed[:, 3:4]
    cot = jnp.concatenate([cot_color, -jnp.sum(cot_color * colors, 1, keepdims=True)], 1)
    got_cot = lax.all_to_all(cot[source_tile], "blk", split_axis=0, concat_axis=0, tiled=True)
    packed = run_backward(
        live, block_centers, rays, got_cot, saved, raycode, small, trunk_weight, density_weight,
        feature_weight, code_weight, radiance_weight,
    )
    packed = lax.psum(packed, "rep")
    return (colors.transpose(1, 0, 2).reshape(3, tiles * TILE),) + tuple(run_unpack(packed))


def solution(mesh):
    weights = (P("blk", None, None), P("blk", None, None, None), P("blk", None)) + (
        P("blk", None, None),
    ) * 5
    ray = P(None, ("blk", "rep"))
    return jax.shard_map(
        local,
        mesh=mesh,
        in_specs=(ray, ray, P(("blk", "rep")), P(("blk", "rep"), None), ray, P(None, "blk")) + weights,
        out_specs=(ray,) + weights,
        check_vma=False,
    )
```

```python
import numpy as np

import jax
import jax.numpy as jnp
from jax import lax
from jax.experimental import pallas as pl
from jax.experimental.pallas import tpu as pltpu
from jax.sharding import PartitionSpec as P

TILE = 128
SAMPLES = 4
SLOTS = 32
LANES = SAMPLES * TILE
HID = 256
CHID = 128
PC = 96
VC = 48
E = 32
RC = VC + E
LO = 256
SPACING = 0.5
LOSS_SCALE = 0.03125
LOG2E = 1.4426950408889634
LN2 = 0.6931471805599453

R_H1 = PC
R_H2 = R_H1 + HID
R_H3 = R_H2 + HID
R_S = R_H3 + HID
R_END = R_S + CHID

G_T1 = 0
G_T2 = 256
G_FD = 512
G_TAB = 640
G_POS = 1664
G_RAD = G_POS + 128
G_DEN = G_RAD + 16
G_ROWS = 1920


def code_places(levels, half):
    raw = list(range(3))
    sines, cosines = [], []
    for level in range(levels):
        for c in range(3):
            row = (level // half) * 3 + c
            group = 2 * (level % half)
            sines.append(8 * (1 + group) + row)
            cosines.append(8 * (2 + group) + row)
    return raw + sines + cosines


def selection(places, width):
    out = np.zeros((len(places), width), np.float32)
    out[np.arange(len(places)), places] = 1.0
    return out


POS_SELECT = selection(code_places(10, 5), PC)
VIEW_SELECT = selection(code_places(4, 2), VC)


def mm(a, b):
    return lax.dot_general(a, b, (((1,), (0,)), ((), ())), preferred_element_type=jnp.float32)


def mm_nt(a, b):
    return lax.dot_general(a, b, (((1,), (1,)), ((), ())), preferred_element_type=jnp.float32)


def softplus(v):
    return jnp.maximum(v, 0.0) + jnp.log(1.0 + jnp.exp(-jnp.abs(v)))


def row_iota(rows, lanes):
    return lax.broadcasted_iota(jnp.int32, (rows, lanes), 0)


def ray_rows(ray, row):
    o8 = jnp.where(row < 3, ray, jnp.where(row < 6, pltpu.roll(ray, 3, 0), 0.0))
    d8 = jnp.where(row < 3, pltpu.roll(ray, 5, 0), jnp.where(row < 6, ray, 0.0))
    return o8, d8


def center_rows(center_ref, row):
    third = jnp.where(row >= 3, row - 3, row)
    return jnp.where(
        third == 0,
        center_ref[0, 0],
        jnp.where(third == 1, center_ref[1, 0], jnp.where(third == 2, center_ref[2, 0], 0.0)),
    )


def code_groups(values, doublings):
    groups = [values]
    sine, cosine = jnp.sin(values), jnp.cos(values)
    for step in range(doublings):
        groups += [sine, cosine]
        if step + 1 < doublings:
            sine, cosine = 2.0 * sine * cosine, (cosine - sine) * (cosine + sine)
    groups.append(jnp.zeros_like(values))
    return jnp.concatenate(groups, 0).astype(jnp.bfloat16)


def over_samples(x):
    return [x[:, s * TILE : (s + 1) * TILE] for s in range(SAMPLES)]


def composite(small, o8, c8, row):
    density = over_samples(softplus(small))
    rad = over_samples(1.0 / (1.0 + jnp.exp(-small)))
    off = o8 - c8
    off2 = jnp.sum(jnp.where(row < 3, off * off, 0.0), 0, keepdims=True)
    inv = 1.0 / (1.0 + off2)
    depth = jnp.zeros((1, TILE), jnp.float32)
    before = jnp.ones((1, TILE), jnp.float32)
    weights, after = [], []
    for s in range(SAMPLES):
        u = density[s][3:4] * SPACING
        weights.append(before * (1.0 - jnp.exp(-u)))
        depth = depth + u
        before = jnp.exp(-depth)
        after.append(before)
    color = sum(w * r for w, r in zip(weights, rad))
    opacity = sum(weights)
    return rad, weights, after, color, (0.1 + opacity) * inv, inv


def forward_kernel(
    live_ref, center_ref, rays_ref, pos_ref, trunk_ref, density_ref, feature_ref, view_ref,
    code_ref, radiance_ref, table_ref, pos_select_ref, view_select_ref,
    part_ref, saved_ref, raycode_ref, small_ref,
    wp, wfd, wray, wrad, tab, buf, sem,
):
    row = row_iota(8, TILE)
    c8 = center_rows(center_ref, row)
    wp[...] = mm(pos_ref[0], pos_select_ref[...]).astype(jnp.bfloat16)
    wray[:, :VC] = mm(view_ref[0], view_select_ref[...]).astype(jnp.bfloat16)
    wray[:, VC:] = code_ref[0]
    wfd[:CHID, :] = feature_ref[0]
    row16 = row_iota(16, HID)
    wfd[CHID:, :] = jnp.where(row16 == 3, density_ref[...].astype(jnp.float32), 0.0).astype(jnp.bfloat16)
    wrad[...] = jnp.concatenate(
        [radiance_ref[0].astype(jnp.float32), jnp.zeros((5, CHID), jnp.float32)], 0
    ).astype(jnp.bfloat16)
    for h in range(SLOTS):
        tab[h * E : (h + 1) * E, :] = table_ref[0, :, h * LO : (h + 1) * LO]
    pos_scale = jnp.where(row < 3, 1.0, 32.0)
    view_scale = jnp.where(row < 3, 1.0, 4.0)

    def saving(count):
        slot = count % 2
        return pltpu.make_async_copy(buf.at[slot], saved_ref.at[count], sem.at[slot])

    def tile(s, count):
        @pl.when(count >= 2)
        def _():
            saving(count - 2).wait()

        out = buf.at[count % 2]
        ray = rays_ref[s]
        o8, d8 = ray_rows(ray, row)
        points = jnp.concatenate(
            [(o8 + (t + 0.5) * SPACING * d8 - c8) * pos_scale for t in range(SAMPLES)], 1
        )
        out[:PC, :] = code_groups(points, 5)
        ids = ray[6:7].astype(jnp.int32)
        lo, hi = ids & (LO - 1), ids >> 8
        hot = (row_iota(LO, TILE) == lo).astype(jnp.float32).astype(jnp.bfloat16)
        rows = mm(tab[...], hot)
        app = jnp.zeros((E, TILE), jnp.float32)
        for h in range(SLOTS):
            app = app + jnp.where(hi == h, rows[h * E : (h + 1) * E], 0.0)
        raycode_ref[s, :VC, :] = code_groups(d8 * view_scale, 2)
        raycode_ref[s, VC:, :] = app.astype(jnp.bfloat16)
        per_ray = mm(wray[...], raycode_ref[s])
        out[R_H1:R_H2, :] = softplus(mm(wp[...], out[:PC, :])).astype(jnp.bfloat16)
        out[R_H2:R_H3, :] = softplus(mm(trunk_ref[0, 0], out[R_H1:R_H2, :])).astype(jnp.bfloat16)
        out[R_H3:R_S, :] = softplus(mm(trunk_ref[0, 1], out[R_H2:R_H3, :])).astype(jnp.bfloat16)
        both = mm(wfd[...], out[R_H3:R_S, :])
        out[R_S:R_END, :] = softplus(
            both[:CHID] + jnp.concatenate([per_ray] * SAMPLES, 1)
        ).astype(jnp.bfloat16)
        logits = mm(wrad[...], out[R_S:R_END, :])
        small = jnp.where(row_iota(8, LANES) == 3, both[CHID : CHID + 8], logits)
        small_ref[s] = small
        _, _, _, color, share, _ = composite(small, o8, c8, row)
        part_ref[s] = jnp.where(row < 3, color * share, share)[:4]
        saving(count).start()
        return count + 1

    def step(s, count):
        return lax.cond(live_ref[s] > 0, lambda: tile(s, count), lambda: count)

    count = lax.fori_loop(0, SLOTS, step, jnp.int32(0))

    @pl.when(count >= 2)
    def _():
        saving(count - 2).wait()

    @pl.when(count >= 1)
    def _():
        saving(count - 1).wait()


def backward_kernel(
    live_ref, center_ref, rays_ref, cot_ref, saved_ref, raycode_ref, small_ref, trunk_ref,
    density_ref, feature_ref, code_ref, radiance_ref,
    g_ref,
    t1, t2, fdt, codet, radt, buf, slots, sem,
):
    row = row_iota(8, TILE)
    c8 = center_rows(center_ref, row)

    def flip(x):
        return x.astype(jnp.float32).T.astype(jnp.bfloat16)

    t1[...] = flip(trunk_ref[0, 0])
    t2[...] = flip(trunk_ref[0, 1])
    fdt[:, :CHID] = flip(feature_ref[0])
    row16 = row_iota(16, HID)
    fdt[:, CHID:] = jnp.where(row16 == 3, density_ref[...].astype(jnp.float32), 0.0).T.astype(jnp.bfloat16)
    codet[...] = flip(code_ref[0])
    radt[...] = jnp.concatenate(
        [radiance_ref[0].astype(jnp.float32), jnp.zeros((13, CHID), jnp.float32)], 0
    ).T.astype(jnp.bfloat16)
    g_ref[...] = jnp.zeros_like(g_ref)

    def listing(s, count):
        @pl.when(live_ref[s] > 0)
        def _():
            slots[count] = s

        return count + (live_ref[s] > 0).astype(jnp.int32)

    total = lax.fori_loop(0, SLOTS, listing, jnp.int32(0))

    def fetching(j):
        return pltpu.make_async_copy(saved_ref.at[j], buf.at[j % 2], sem.at[j % 2])

    @pl.when(total > 0)
    def _():
        fetching(0).start()

    def tile(j, carry):
        s = slots[j]
        fetching(j).wait()

        @pl.when(j + 1 < total)
        def _():
            fetching(j + 1).start()

        act = buf.at[j % 2]
        ray = rays_ref[s]
        o8, _ = ray_rows(ray, row)
        small = small_ref[s]
        rad, weights, after, color, share, inv = composite(small, o8, c8, row)
        cot = jnp.concatenate([cot_ref[s], jnp.zeros((4, TILE), jnp.float32)], 0)
        d_share = jnp.sum(
            jnp.where(row < 3, cot * color, jnp.where(row == 3, cot, 0.0)), 0, keepdims=True
        )
        d_color = jnp.where(row < 3, cot * share, 0.0)
        d_opacity = d_share * inv
        sig = over_samples(1.0 / (1.0 + jnp.exp(-small)))
        later = jnp.zeros((1, TILE), jnp.float32)
        pieces = [None] * SAMPLES
        for t in reversed(range(SAMPLES)):
            d_w = jnp.sum(d_color * rad[t], 0, keepdims=True) + d_opacity
            d_u = d_w * after[t] - later
            later = later + d_w * weights[t]
            d_logit = d_color * weights[t] * rad[t] * (1.0 - rad[t])
            pieces[t] = jnp.where(
                row < 3, d_logit, jnp.where(row == 3, d_u * SPACING * sig[t], 0.0)
            )
        d_small = jnp.concatenate(pieces, 1)
        d_small = jnp.concatenate([d_small, jnp.zeros_like(d_small)], 0).astype(jnp.bfloat16)

        def through(grad, lo_row, hi_row):
            value = act[lo_row:hi_row, :].astype(jnp.float32)
            return grad * (1.0 - jnp.exp(-value))

        shaded = act[R_S:R_END, :]
        d_feature = through(mm(radt[...], d_small), R_S, R_END)
        g_ref[G_POS + CHID : G_POS + CHID + 16, 128:256] += mm_nt(d_small, shaded)
        d_ray = sum(over_samples(d_feature)).astype(jnp.bfloat16)
        g_ref[G_POS : G_POS + CHID, 128 : 128 + RC] += mm_nt(d_ray, raycode_ref[s])
        d_app = mm(codet[...], d_ray)
        ids = ray[6:7].astype(jnp.int32)
        lo, hi = ids & (LO - 1), ids >> 8
        hot = (row_iota(LO, TILE) == lo).astype(jnp.float32).astype(jnp.bfloat16)
        spread = jnp.concatenate(
            [jnp.where(hi == h, d_app, 0.0).astype(jnp.bfloat16) for h in range(SLOTS)], 0
        )
        g_ref[G_TAB:G_POS, :] += mm_nt(spread, hot)
        both = jnp.concatenate([d_feature.astype(jnp.bfloat16), d_small], 0)
        d_both = mm_nt(both, act[R_H3:R_S, :])
        g_ref[G_FD:G_TAB, :] += d_both[:CHID]
        g_ref[G_DEN : G_DEN + 16, 128:256] += d_both[CHID:, :128]
        g_ref[G_DEN + 16 : G_DEN + 32, 128:256] += d_both[CHID:, 128:]
        d_z = through(mm(fdt[...], both), R_H3, R_S).astype(jnp.bfloat16)
        g_ref[G_T2:G_FD, :] += mm_nt(d_z, act[R_H2:R_H3, :])
        d_z = through(mm(t2[...], d_z), R_H2, R_H3).astype(jnp.bfloat16)
        g_ref[G_T1:G_T2, :] += mm_nt(d_z, act[R_H1:R_H2, :])
        d_z = through(mm(t1[...], d_z), R_H1, R_H2).astype(jnp.bfloat16)
        g_ref[G_POS : G_POS + HID, :PC] += mm_nt(d_z, act[:PC, :])
        return carry

    lax.fori_loop(0, total, tile, jnp.int32(0))


def unpack_kernel(
    g_ref, pos_select_ref, view_select_ref,
    pos_ref, trunk_ref, density_ref, feature_ref, view_ref, code_ref, radiance_ref, table_ref,
):
    def pick(a, select):
        return lax.dot_general(
            a, select.astype(jnp.float32), (((1,), (1,)), ((), ())),
            preferred_element_type=jnp.float32, precision=lax.Precision.HIGHEST,
        )

    pos_ref[0] = pick(g_ref[G_POS : G_POS + HID, :PC], pos_select_ref[...])
    trunk_ref[0, 0] = g_ref[G_T1:G_T2, :]
    trunk_ref[0, 1] = g_ref[G_T2:G_FD, :]
    feature_ref[0] = g_ref[G_FD : G_FD + CHID, :]
    density_ref[:, :128] = g_ref[G_DEN + 3 : G_DEN + 4, 128:256]
    density_ref[:, 128:] = g_ref[G_DEN + 19 : G_DEN + 20, 128:256]
    view_ref[0] = pick(g_ref[G_POS : G_POS + CHID, 128 : 128 + VC], view_select_ref[...])
    code_ref[0] = g_ref[G_POS : G_POS + CHID, 128 + VC : 128 + RC]
    radiance_ref[0] = g_ref[G_POS + CHID : G_POS + CHID + 3, 128:256]
    for h in range(SLOTS):
        table_ref[0, :, h * LO : (h + 1) * LO] = g_ref[G_TAB + h * E : G_TAB + (h + 1) * E, :]


VMEM = pl.BlockSpec(memory_space=pltpu.VMEM)
SMEM = pl.BlockSpec(memory_space=pltpu.SMEM)
ANY = pl.BlockSpec(memory_space=pl.ANY)


def run_forward(live, center, rays, pos, trunk, density, feature, view, code, radiance, table):
    bf = jnp.bfloat16
    return pl.pallas_call(
        forward_kernel,
        name="forward_tiles",
        out_shape=(
            jax.ShapeDtypeStruct((SLOTS, 4, TILE), jnp.float32),
            jax.ShapeDtypeStruct((SLOTS, R_END, LANES), bf),
            jax.ShapeDtypeStruct((SLOTS, RC, TILE), bf),
            jax.ShapeDtypeStruct((SLOTS, 8, LANES), jnp.float32),
        ),
        in_specs=[SMEM, SMEM] + [VMEM] * 11,
        out_specs=(VMEM, ANY, VMEM, VMEM),
        scratch_shapes=[
            pltpu.VMEM((HID, PC), bf),
            pltpu.VMEM((CHID + 16, HID), bf),
            pltpu.VMEM((CHID, RC), bf),
            pltpu.VMEM((8, CHID), bf),
            pltpu.VMEM((SLOTS * E, LO), bf),
            pltpu.VMEM((2, R_END, LANES), bf),
            pltpu.SemaphoreType.DMA((2,)),
        ],
        compiler_params=pltpu.CompilerParams(vmem_limit_bytes=32 * 1024 * 1024),
        cost_estimate=pl.CostEstimate(flops=10**10, bytes_accessed=3 * 10**7, transcendentals=0),
    )(live, center, rays, pos, trunk, density, feature, view, code, radiance, table,
      jnp.asarray(POS_SELECT, bf), jnp.asarray(VIEW_SELECT, bf))


def run_backward(live, center, rays, cot, saved, raycode, small, trunk, density, feature, code, radiance):
    bf = jnp.bfloat16
    return pl.pallas_call(
        backward_kernel,
        name="backward_tiles",
        out_shape=jax.ShapeDtypeStruct((G_ROWS, 256), jnp.float32),
        in_specs=[SMEM, SMEM, VMEM, VMEM, ANY] + [VMEM] * 7,
        out_specs=VMEM,
        scratch_shapes=[
            pltpu.VMEM((HID, HID), bf),
            pltpu.VMEM((HID, HID), bf),
            pltpu.VMEM((HID, CHID + 16), bf),
            pltpu.VMEM((E, CHID), bf),
            pltpu.VMEM((CHID, 16), bf),
            pltpu.VMEM((2, R_END, LANES), bf),
            pltpu.SMEM((SLOTS,), jnp.int32),
            pltpu.SemaphoreType.DMA((2,)),
        ],
        compiler_params=pltpu.CompilerParams(vmem_limit_bytes=32 * 1024 * 1024),
        cost_estimate=pl.CostEstimate(flops=2 * 10**10, bytes_accessed=3 * 10**7, transcendentals=0),
    )(live, center, rays, cot, saved, raycode, small, trunk, density, feature, code, radiance)


def run_unpack(packed):
    f32 = jnp.float32
    shapes = [(1, 256, 63), (1, 2, 256, 256), (1, 256), (1, 128, 256), (1, 128, 27), (1, 128, 32),
              (1, 3, 128), (1, 32, 8192)]
    return pl.pallas_call(
        unpack_kernel,
        name="unpack_gradients",
        out_shape=tuple(jax.ShapeDtypeStruct(s, f32) for s in shapes),
        in_specs=[VMEM] * 3,
        out_specs=tuple(VMEM for _ in shapes),
        compiler_params=pltpu.CompilerParams(vmem_limit_bytes=32 * 1024 * 1024),
    )(packed, jnp.asarray(POS_SELECT, jnp.bfloat16), jnp.asarray(VIEW_SELECT, jnp.bfloat16))


MESH = pl.DeviceIdType.MESH
GROUP = SLOTS
REPS = 4
CHUNK = G_ROWS // (4 * REPS)


def place():
    return lax.axis_index("blk"), lax.axis_index("rep")


def partner(blk, rep, i):
    return lax.rem(blk + i, GROUP), lax.rem(rep + GROUP * REPS - i, REPS)


def meet(blk, rep):
    barrier = pltpu.get_barrier_semaphore()

    def greet(i, carry):
        pl.semaphore_signal(barrier, inc=1, device_id=partner(blk, rep, i), device_id_type=MESH)
        return carry

    lax.fori_loop(1, GROUP, greet, 0)
    pl.semaphore_wait(barrier, GROUP - 1)


def exchange(blk, rep, src, dst, send_sem, recv_sem):
    def copy(i):
        to_blk, to_rep = partner(blk, rep, i)
        return pltpu.make_async_remote_copy(
            src_ref=src.at[to_blk], dst_ref=dst.at[blk], send_sem=send_sem.at[i],
            recv_sem=recv_sem.at[i], device_id=(to_blk, to_rep), device_id_type=MESH,
        )

    def begin(i, carry):
        copy(i).start()
        return carry

    lax.fori_loop(1, GROUP, begin, 0)
    dst[blk] = src[blk]
    return copy


def finish(copy):
    def end(i, carry):
        copy(i).wait()
        return carry

    lax.fori_loop(1, GROUP, end, 0)


def scatter_kernel(tile_ref, live_ref, tiles_ref, out_ref, send, send_sem, recv_sem):
    blk, rep = place()
    row = row_iota(8, TILE)
    for k in range(GROUP):
        flag = live_ref[k].astype(jnp.float32)
        send[k] = jnp.where(row == 7, flag, tiles_ref[tile_ref[k]])
    meet(blk, rep)
    finish(exchange(blk, rep, send, out_ref, send_sem, recv_sem))


def blend_kernel(
    ids_ref, tile_ref, part_ref, grad_ref, colors_ref, cot_ref,
    back, cots, send, send_sem, recv_sem, send_sem2, recv_sem2,
):
    blk, rep = place()
    meet(blk, rep)
    finish(exchange(blk, rep, part_ref, back, send_sem, recv_sem))
    for t in range(cots.shape[0]):
        summed = back[ids_ref[3 * t]] + back[ids_ref[3 * t + 1]] + back[ids_ref[3 * t + 2]]
        lanes = slice(t * TILE, (t + 1) * TILE)
        colors = summed[:3] / summed[3:4]
        colors_ref[:, lanes] = colors
        cot = grad_ref[:, lanes] * LOSS_SCALE / summed[3:4]
        cots[t] = jnp.concatenate([cot, -jnp.sum(cot * colors, 0, keepdims=True)], 0)
    for k in range(GROUP):
        send[k] = cots[tile_ref[k]]
    finish(exchange(blk, rep, send, cot_ref, send_sem2, recv_sem2))


def total_kernel(g_ref, out_ref, got, held, send_sem, recv_sem):
    blk, rep = place()
    up, down = lax.rem(rep + 1, REPS), lax.rem(rep + REPS - 1, REPS)
    barrier = pltpu.get_barrier_semaphore()
    for other in (up, down):
        pl.semaphore_signal(barrier, inc=1, device_id=(blk, other), device_id_type=MESH)
    pl.semaphore_wait(barrier, 2)
    rings = range(4)

    def chunk(ring, ahead):
        sign = 1 if ring % 2 == 0 else REPS - 1
        which = lax.rem(rep + sign * (ahead + REPS), REPS)
        return pl.ds(pl.multiple_of((ring * REPS + which) * CHUNK, 8), CHUNK)

    def copy(ring, step):
        if step == 0:
            src, dst = g_ref.at[chunk(ring, 0)], got.at[ring, 0]
        elif step < 3:
            src, dst = held.at[ring, step - 1], got.at[ring, step]
        else:
            rows = chunk(ring, 4 - step)
            src, dst = out_ref.at[rows], out_ref.at[rows]
        return pltpu.make_async_remote_copy(
            src_ref=src, dst_ref=dst, send_sem=send_sem.at[ring, step],
            recv_sem=recv_sem.at[ring, step],
            device_id=(blk, up if ring % 2 == 0 else down), device_id_type=MESH,
        )

    for ring in rings:
        copy(ring, 0).start()
    for step in range(6):
        for ring in rings:
            copy(ring, step).wait_recv()
            if step < 2:
                held[ring, step] = got[ring, step] + g_ref[chunk(ring, -step - 1), :]
            elif step == 2:
                out_ref[chunk(ring, 1), :] = got[ring, 2] + g_ref[chunk(ring, 1), :]
            if step < 5:
                copy(ring, step + 1).start()
    for step in range(6):
        for ring in rings:
            copy(ring, step).wait_send()


def communicate(kernel, name, number, args, specs, shapes, scratch):
    return pl.pallas_call(
        kernel,
        name=name,
        out_shape=shapes,
        in_specs=specs,
        out_specs=jax.tree.map(lambda _: VMEM, shapes),
        scratch_shapes=scratch,
        compiler_params=pltpu.CompilerParams(
            collective_id=number, has_side_effects=True, vmem_limit_bytes=16 * 1024 * 1024
        ),
    )(*args)


def run_scatter(tile_of, live, tiles):
    return communicate(
        scatter_kernel, "scatter_rays", 0, (tile_of, live, tiles), [SMEM, SMEM, VMEM],
        jax.ShapeDtypeStruct((GROUP, 8, TILE), jnp.float32),
        [pltpu.VMEM((GROUP, 8, TILE), jnp.float32)] + [pltpu.SemaphoreType.DMA((GROUP,))] * 2,
    )


def run_blend(ids, tile_of, part, grad):
    tiles = grad.shape[1] // TILE
    small = (GROUP, 4, TILE)
    return communicate(
        blend_kernel, "blend_colors", 1, (ids, tile_of, part, grad), [SMEM, SMEM, VMEM, VMEM],
        (jax.ShapeDtypeStruct(grad.shape, jnp.float32), jax.ShapeDtypeStruct(small, jnp.float32)),
        [pltpu.VMEM(small, jnp.float32), pltpu.VMEM((tiles, 4, TILE), jnp.float32),
         pltpu.VMEM(small, jnp.float32)] + [pltpu.SemaphoreType.DMA((GROUP,))] * 4,
    )


def run_total(packed):
    return communicate(
        total_kernel, "total_gradients", 2, (packed,), [VMEM],
        jax.ShapeDtypeStruct((G_ROWS, 256), jnp.float32),
        [pltpu.VMEM((4, 3, CHUNK, 256), jnp.float32), pltpu.VMEM((4, 2, CHUNK, 256), jnp.float32)]
        + [pltpu.SemaphoreType.DMA((4, 6))] * 2,
    )


def local(
    anchors, directions, app_ids, block_ids, color_grad, block_centers, pos_weight, trunk_weight,
    density_weight, feature_weight, view_weight, code_weight, radiance_weight, code_table,
):
    tiles = block_ids.shape[0]
    peers = jnp.arange(SLOTS, dtype=jnp.int32)
    flat_ids = block_ids.reshape(-1)
    matches = (flat_ids[None, :] == peers[:, None]).astype(jnp.int32)
    is_live = jnp.sum(matches, 1)
    source_tile = jnp.sum(matches * jnp.arange(3 * tiles, dtype=jnp.int32)[None, :], 1) // 3
    rows = jnp.concatenate(
        [anchors, directions, app_ids.astype(jnp.float32)[None], jnp.zeros((1, tiles * TILE), jnp.float32)], 0
    )
    ray_tiles = rows.reshape(8, tiles, TILE).transpose(1, 0, 2)
    rays = run_scatter(source_tile, is_live, ray_tiles)
    live = (rays[:, 7, 0] > 0.5).astype(jnp.int32)
    part, saved, raycode, small = run_forward(
        live, block_centers, rays, pos_weight, trunk_weight, density_weight, feature_weight,
        view_weight, code_weight, radiance_weight, code_table,
    )
    colors, cot = run_blend(flat_ids, source_tile, part, color_grad)
    packed = run_backward(
        live, block_centers, rays, cot, saved, raycode, small, trunk_weight, density_weight,
        feature_weight, code_weight, radiance_weight,
    )
    return (colors,) + tuple(run_unpack(run_total(packed)))


def solution(mesh):
    weights = (P("blk", None, None), P("blk", None, None, None), P("blk", None)) + (
        P("blk", None, None),
    ) * 5
    ray = P(None, ("blk", "rep"))
    return jax.shard_map(
        local,
        mesh=mesh,
        in_specs=(ray, ray, P(("blk", "rep")), P(("blk", "rep"), None), ray, P(None, "blk")) + weights,
        out_specs=(ray,) + weights,
        check_vma=False,
    )
```

```python
import numpy as np

import jax
import jax.numpy as jnp
from jax import lax
from jax.experimental import pallas as pl
from jax.experimental.pallas import tpu as pltpu
from jax.sharding import PartitionSpec as P

TILE = 128
SAMPLES = 4
SLOTS = 32
LANES = SAMPLES * TILE
HID = 256
CHID = 128
PC = 96
VC = 48
E = 32
RC = VC + E
LO = 256
SPACING = 0.5
LOSS_SCALE = 0.03125
DEEP = 3
PARTS_F = 4
PARTS_B = 4

R_H1 = PC
R_H2 = R_H1 + HID
R_H3 = R_H2 + HID
R_S = R_H3 + HID
R_END = R_S + CHID

G_T1 = 0
G_T2 = 256
G_FD = 512
G_TAB = 640
G_POS = 1664
G_RAD = G_POS + 128
G_DEN = G_RAD + 16
G_ROWS = 1920


def code_places(levels, half):
    raw = list(range(3))
    sines, cosines = [], []
    for level in range(levels):
        for c in range(3):
            row = (level // half) * 3 + c
            group = 2 * (level % half)
            sines.append(8 * (1 + group) + row)
            cosines.append(8 * (2 + group) + row)
    return raw + sines + cosines


def selection(places, width):
    out = np.zeros((len(places), width), np.float32)
    out[np.arange(len(places)), places] = 1.0
    return out


POS_SELECT = selection(code_places(10, 5), PC)
VIEW_SELECT = selection(code_places(4, 2), VC)


def mm(a, b):
    return lax.dot_general(a, b, (((1,), (0,)), ((), ())), preferred_element_type=jnp.float32)


def mm_nt(a, b):
    return lax.dot_general(a, b, (((1,), (1,)), ((), ())), preferred_element_type=jnp.float32)


def mm_tn(a, b):
    return lax.dot_general(a, b, (((0,), (0,)), ((), ())), preferred_element_type=jnp.float32)


def softplus(v):
    return jnp.maximum(v, 0.0) + jnp.log(1.0 + jnp.exp(-jnp.abs(v)))


def row_iota(rows, lanes):
    return lax.broadcasted_iota(jnp.int32, (rows, lanes), 0)


def ray_rows(ray, row):
    o8 = jnp.where(row < 3, ray, jnp.where(row < 6, pltpu.roll(ray, 3, 0), 0.0))
    d8 = jnp.where(row < 3, pltpu.roll(ray, 5, 0), jnp.where(row < 6, ray, 0.0))
    return o8, d8


def center_rows(center_ref, row):
    third = jnp.where(row >= 3, row - 3, row)
    return jnp.where(
        third == 0,
        center_ref[0, 0],
        jnp.where(third == 1, center_ref[0, 1], jnp.where(third == 2, center_ref[0, 2], 0.0)),
    )


def code_groups(values, doublings):
    groups = [values]
    sine, cosine = jnp.sin(values), jnp.cos(values)
    for step in range(doublings):
        groups += [sine, cosine]
        if step + 1 < doublings:
            sine, cosine = 2.0 * sine * cosine, (cosine - sine) * (cosine + sine)
    groups.append(jnp.zeros_like(values))
    return jnp.concatenate(groups, 0).astype(jnp.bfloat16)


def halves(x):
    return x[:, :TILE], x[:, TILE:]


def over_samples(x):
    return [
        jnp.concatenate([x[:, s * TILE : (s + 1) * TILE], x[:, LANES + s * TILE : LANES + (s + 1) * TILE]], 1)
        for s in range(SAMPLES)
    ]


def by_samples(pieces):
    return jnp.concatenate([halves(p)[h] for h in range(2) for p in pieces], 1)


def composite(small, o8, c8, row):
    density = over_samples(softplus(small))
    rad = over_samples(1.0 / (1.0 + jnp.exp(-small)))
    off = o8 - c8
    off2 = jnp.sum(jnp.where(row < 3, off * off, 0.0), 0, keepdims=True)
    inv = 1.0 / (1.0 + off2)
    depth = jnp.zeros((1, 2 * TILE), jnp.float32)
    before = jnp.ones((1, 2 * TILE), jnp.float32)
    weights, after = [], []
    for s in range(SAMPLES):
        u = density[s][3:4] * SPACING
        weights.append(before * (1.0 - jnp.exp(-u)))
        depth = depth + u
        before = jnp.exp(-depth)
        after.append(before)
    color = sum(w * r for w, r in zip(weights, rad))
    opacity = sum(weights)
    return rad, weights, after, color, (0.1 + opacity) * inv, inv


def list_live(live_ref, slots):
    def listing(s, count):
        @pl.when(live_ref[s] > 0)
        def _():
            slots[count] = s

        return count + (live_ref[s] > 0).astype(jnp.int32)

    total = lax.fori_loop(0, SLOTS, listing, jnp.int32(0))

    @pl.when(total % 2 == 1)
    def _():
        slots[total] = slots[total - 1]

    return total, (total + 1) // 2


def pair_copies(buf, saved_ref, sem, j, out):
    slot = lax.rem(j, DEEP)
    copies = []
    for n, (lo, hi) in enumerate(((0, 256), (256, 512), (512, 752), (752, R_END))):
        near, far = buf.at[slot, lo:hi], saved_ref.at[j, lo:hi]
        src, dst = (near, far) if out else (far, near)
        copies.append(pltpu.make_async_copy(src, dst, sem.at[slot, n]))
    return copies


def hot_lanes(ids):
    lo, hi = ids & (LO - 1), ids >> 8
    return (row_iota(LO, 2 * TILE) == lo).astype(jnp.float32).astype(jnp.bfloat16), hi


def lane_parts(parts):
    width = 2 * LANES // parts
    return [slice(p * width, (p + 1) * width) for p in range(parts)]


def forward_kernel(
    live_ref, center_ref, rays_ref, pos_ref, trunk_ref, density_ref, feature_ref, view_ref,
    code_ref, radiance_ref, table_ref, pos_select_ref, view_select_ref,
    part_ref, saved_ref, raycode_ref, small_ref,
    wp, wfd, wray, wrad, tab, buf, slots, sem,
):
    row = row_iota(8, 2 * TILE)
    c8 = center_rows(center_ref, row)
    wp[...] = mm_tn(pos_select_ref[...], pos_ref[0]).T.astype(jnp.bfloat16)
    wray[...] = jnp.concatenate(
        [mm_tn(view_select_ref[...], view_ref[0]), code_ref[0].astype(jnp.float32)], 0
    ).T.astype(jnp.bfloat16)
    wfd[:CHID, :] = feature_ref[0]
    row16 = row_iota(16, HID)
    wfd[CHID:, :] = jnp.where(row16 == 3, density_ref[...].astype(jnp.float32), 0.0).astype(jnp.bfloat16)
    wrad[...] = jnp.concatenate(
        [radiance_ref[0].astype(jnp.float32), jnp.zeros((5, CHID), jnp.float32)], 0
    ).astype(jnp.bfloat16)
    for h in range(SLOTS):
        tab[h * E : (h + 1) * E, :] = table_ref[0, :, h * LO : (h + 1) * LO]
    pos_scale = jnp.where(row < 3, 1.0, 32.0)
    view_scale = jnp.where(row < 3, 1.0, 4.0)
    total, pairs = list_live(live_ref, slots)

    def pair(j, carry):
        @pl.when(j >= DEEP)
        def _():
            for copy in pair_copies(buf, saved_ref, sem, j - DEEP, True):
                copy.wait()

        out = buf.at[lax.rem(j, DEEP)]
        s0, s1 = slots[2 * j], slots[2 * j + 1]
        ray = jnp.concatenate([rays_ref[s0], rays_ref[s1]], 1)
        o8, d8 = ray_rows(ray, row)
        points = by_samples(
            [(o8 + (t + 0.5) * SPACING * d8 - c8) * pos_scale for t in range(SAMPLES)]
        )
        out[:PC, :] = code_groups(points, 5)
        hot, hi = hot_lanes(ray[6:7].astype(jnp.int32))
        rows = mm(tab[...], hot)
        app = jnp.zeros((E, 2 * TILE), jnp.float32)
        for h in range(SLOTS):
            app = app + jnp.where(hi == h, rows[h * E : (h + 1) * E], 0.0)
        raycode = jnp.concatenate([code_groups(d8 * view_scale, 2), app.astype(jnp.bfloat16)], 0)
        raycode_ref[j] = raycode
        per_ray = mm(wray[...], raycode)
        lanes = lane_parts(PARTS_F)
        for w, lo, mid, hi_row in (
            (wp, 0, R_H1, R_H2), (trunk_ref.at[0, 0], R_H1, R_H2, R_H3), (trunk_ref.at[0, 1], R_H2, R_H3, R_S)
        ):
            for part in lanes:
                out[mid:hi_row, part] = softplus(mm(w[...], out[lo:mid, part])).astype(jnp.bfloat16)
        ray_lanes = by_samples([per_ray] * SAMPLES)
        small = []
        for part in lanes:
            both = mm(wfd[...], out[R_H3:R_S, part])
            shaded = softplus(both[:CHID] + ray_lanes[:, part]).astype(jnp.bfloat16)
            out[R_S:R_END, part] = shaded
            logits = mm(wrad[...], shaded)
            small.append(jnp.where(row_iota(8, logits.shape[1]) == 3, both[CHID : CHID + 8], logits))
        small = jnp.concatenate(small, 1)
        small_ref[j] = small
        _, _, _, color, share, _ = composite(small, o8, c8, row)
        first, second = halves(jnp.where(row < 3, color * share, share)[:4])
        part_ref[s0] = first
        part_ref[s1] = second
        for copy in pair_copies(buf, saved_ref, sem, j, True):
            copy.start()
        return carry

    lax.fori_loop(0, pairs, pair, jnp.int32(0))

    def drain(j, carry):
        for copy in pair_copies(buf, saved_ref, sem, j, True):
            copy.wait()
        return carry

    lax.fori_loop(jnp.maximum(pairs - DEEP, 0), pairs, drain, jnp.int32(0))


def backward_kernel(
    live_ref, center_ref, rays_ref, cot_ref, saved_ref, raycode_ref, small_ref, trunk_ref,
    density_ref, feature_ref, code_ref, radiance_ref,
    g_ref,
    t1, t2, fdt, radt, dz0, dz1, dz2, dz3, buf, slots, sem,
):
    total, pairs = list_live(live_ref, slots)

    def fetch(j, carry):
        for copy in pair_copies(buf, saved_ref, sem, j, False):
            copy.start()
        return carry

    lax.fori_loop(0, jnp.minimum(pairs, DEEP - 1), fetch, jnp.int32(0))
    row = row_iota(8, 2 * TILE)
    lane = lax.broadcasted_iota(jnp.int32, (1, 2 * TILE), 1)
    c8 = center_rows(center_ref, row)

    def flip(x):
        return x.astype(jnp.float32).T.astype(jnp.bfloat16)

    t1[...] = flip(trunk_ref[0, 0])
    t2[...] = flip(trunk_ref[0, 1])
    fdt[:, :CHID] = flip(feature_ref[0])
    row16 = row_iota(16, HID)
    fdt[:, CHID:] = jnp.where(row16 == 3, density_ref[...].astype(jnp.float32), 0.0).T.astype(jnp.bfloat16)
    radt[...] = jnp.concatenate(
        [radiance_ref[0].astype(jnp.float32), jnp.zeros((13, CHID), jnp.float32)], 0
    ).T.astype(jnp.bfloat16)
    g_ref[...] = jnp.zeros_like(g_ref)

    def pair(j, carry):
        for copy in pair_copies(buf, saved_ref, sem, j, False):
            copy.wait()

        @pl.when(j + DEEP - 1 < pairs)
        def _():
            fetch(j + DEEP - 1, carry)

        act = buf.at[lax.rem(j, DEEP)]
        s0, s1 = slots[2 * j], slots[2 * j + 1]
        ray = jnp.concatenate([rays_ref[s0], rays_ref[s1]], 1)
        o8, _ = ray_rows(ray, row)
        small = small_ref[j]
        rad, weights, after, color, share, inv = composite(small, o8, c8, row)
        cot = jnp.concatenate([cot_ref[s0], cot_ref[s1]], 1)
        cot = jnp.where((lane < TILE) | (2 * j + 1 < total), cot, 0.0)
        cot = jnp.concatenate([cot, jnp.zeros_like(cot)], 0)
        d_share = jnp.sum(
            jnp.where(row < 3, cot * color, jnp.where(row == 3, cot, 0.0)), 0, keepdims=True
        )
        d_color = jnp.where(row < 3, cot * share, 0.0)
        d_opacity = d_share * inv
        sig = rad
        later = jnp.zeros((1, 2 * TILE), jnp.float32)
        pieces = [None] * SAMPLES
        for t in reversed(range(SAMPLES)):
            d_w = jnp.sum(d_color * rad[t], 0, keepdims=True) + d_opacity
            d_u = d_w * after[t] - later
            later = later + d_w * weights[t]
            d_logit = d_color * weights[t] * rad[t] * (1.0 - rad[t])
            pieces[t] = jnp.where(
                row < 3, d_logit, jnp.where(row == 3, d_u * SPACING * sig[t], 0.0)
            )
        d_small = by_samples(pieces)
        dz3[CHID:, :] = jnp.concatenate([d_small, jnp.zeros_like(d_small)], 0).astype(jnp.bfloat16)

        def through(grad, lo_row, hi_row, part):
            value = act[lo_row:hi_row, part].astype(jnp.float32)
            return grad * (1.0 - jnp.exp(-value))

        lanes = lane_parts(PARTS_B)
        d_feature = []
        for part in lanes:
            piece = through(mm(radt[...], dz3[CHID:, part]), R_S, R_END, part)
            dz3[:CHID, part] = piece.astype(jnp.bfloat16)
            d_feature.append(piece)
        d_ray = sum(over_samples(jnp.concatenate(d_feature, 1))).astype(jnp.bfloat16)
        for wt, src, dst, lo, hi in (
            (fdt, dz3, dz2, R_H3, R_S), (t2, dz2, dz1, R_H2, R_H3), (t1, dz1, dz0, R_H1, R_H2)
        ):
            for part in lanes:
                dst[:, part] = through(mm(wt[...], src[:, part]), lo, hi, part).astype(jnp.bfloat16)
            if src is dz3:
                d_app = mm(code_ref[0], d_ray)
                hot, high = hot_lanes(ray[6:7].astype(jnp.int32))
                spread = jnp.concatenate(
                    [jnp.where(high == h, d_app, 0.0).astype(jnp.bfloat16) for h in range(SLOTS)], 0
                )
                g_ref[G_POS : G_POS + CHID, 128 : 128 + RC] += mm_nt(d_ray, raycode_ref[j])
                g_ref[G_RAD:G_DEN, 128:256] += mm_nt(dz3[CHID:, :], act[R_S:R_END, :])
                d_both = mm_nt(dz3[...], act[R_H3:R_S, :])
                g_ref[G_FD:G_TAB, :] += d_both[:CHID]
                g_ref[G_DEN : G_DEN + 16, 128:256] += d_both[CHID:, :128]
                g_ref[G_DEN + 16 : G_DEN + 32, 128:256] += d_both[CHID:, 128:]
                g_ref[G_TAB:G_POS, :] += mm_nt(spread, hot)
            elif src is dz2:
                g_ref[G_T2:G_FD, :] += mm_nt(dz2[...], act[R_H2:R_H3, :])
            else:
                g_ref[G_T1:G_T2, :] += mm_nt(dz1[...], act[R_H1:R_H2, :])
        g_ref[G_POS : G_POS + HID, :PC] += mm_nt(dz0[...], act[:PC, :])
        return carry

    lax.fori_loop(0, pairs, pair, jnp.int32(0))


def unpack_kernel(
    g_ref, got_colors_ref, pos_select_ref, view_select_ref,
    colors_ref, pos_ref, trunk_ref, density_ref, feature_ref, view_ref, code_ref, radiance_ref, table_ref,
):
    colors_ref[...] = got_colors_ref[...]

    def pick(a, select):
        return lax.dot_general(
            select.astype(jnp.float32), a, (((1,), (1,)), ((), ())),
            preferred_element_type=jnp.float32, precision=lax.Precision.HIGHEST,
        )

    pos = pick(g_ref[G_POS : G_POS + HID, :PC], pos_select_ref[...])
    for n in range(pos.shape[0]):
        pos_ref[n] = pos[n : n + 1]
    trunk_ref[0, 0] = g_ref[G_T1:G_T2, :]
    trunk_ref[0, 1] = g_ref[G_T2:G_FD, :]
    feature_ref[0] = g_ref[G_FD : G_FD + CHID, :]
    density_ref[:, :128] = g_ref[G_DEN + 3 : G_DEN + 4, 128:256]
    density_ref[:, 128:] = g_ref[G_DEN + 19 : G_DEN + 20, 128:256]
    view = pick(g_ref[G_POS : G_POS + CHID, 128 : 128 + VC], view_select_ref[...])
    for n in range(view.shape[0]):
        view_ref[n] = view[n : n + 1]
    code_ref[0] = g_ref[G_POS : G_POS + CHID, 128:256].T[VC:RC]
    for n in range(3):
        radiance_ref[n] = g_ref[G_RAD + n : G_RAD + n + 1, 128:256]
    for h in range(SLOTS):
        table_ref[0, :, h * LO : (h + 1) * LO] = g_ref[G_TAB + h * E : G_TAB + (h + 1) * E, :]


VMEM = pl.BlockSpec(memory_space=pltpu.VMEM)
SMEM = pl.BlockSpec(memory_space=pltpu.SMEM)
ANY = pl.BlockSpec(memory_space=pl.ANY)


def run_forward(live, center, rays, pos, trunk, density, feature, view, code, radiance, table):
    bf = jnp.bfloat16
    return pl.pallas_call(
        forward_kernel,
        name="forward_tiles",
        out_shape=(
            jax.ShapeDtypeStruct((SLOTS, 4, TILE), jnp.float32),
            jax.ShapeDtypeStruct((SLOTS // 2, R_END, 2 * LANES), bf),
            jax.ShapeDtypeStruct((SLOTS // 2, RC, 2 * TILE), bf),
            jax.ShapeDtypeStruct((SLOTS // 2, 8, 2 * LANES), jnp.float32),
        ),
        in_specs=[SMEM, SMEM] + [VMEM] * 11,
        out_specs=(VMEM, ANY, VMEM, VMEM),
        scratch_shapes=[
            pltpu.VMEM((HID, PC), bf),
            pltpu.VMEM((CHID + 16, HID), bf),
            pltpu.VMEM((CHID, RC), bf),
            pltpu.VMEM((8, CHID), bf),
            pltpu.VMEM((SLOTS * E, LO), bf),
            pltpu.VMEM((DEEP, R_END, 2 * LANES), bf),
            pltpu.SMEM((SLOTS,), jnp.int32),
            pltpu.SemaphoreType.DMA((DEEP, 4)),
        ],
        compiler_params=pltpu.CompilerParams(vmem_limit_bytes=40 * 1024 * 1024),
        cost_estimate=pl.CostEstimate(flops=10**10, bytes_accessed=3 * 10**7, transcendentals=0),
    )(live, center, rays, pos, trunk, density, feature, view, code, radiance, table,
      jnp.asarray(POS_SELECT, bf), jnp.asarray(VIEW_SELECT, bf))


def run_backward(live, center, rays, cot, saved, raycode, small, trunk, density, feature, code, radiance):
    bf = jnp.bfloat16
    return pl.pallas_call(
        backward_kernel,
        name="backward_tiles",
        out_shape=jax.ShapeDtypeStruct((G_ROWS, 256), jnp.float32),
        in_specs=[SMEM, SMEM, VMEM, VMEM, ANY] + [VMEM] * 7,
        out_specs=VMEM,
        scratch_shapes=[
            pltpu.VMEM((HID, HID), bf),
            pltpu.VMEM((HID, HID), bf),
            pltpu.VMEM((HID, CHID + 16), bf),
            pltpu.VMEM((CHID, 16), bf),
            pltpu.VMEM((HID, 2 * LANES), bf),
            pltpu.VMEM((HID, 2 * LANES), bf),
            pltpu.VMEM((HID, 2 * LANES), bf),
            pltpu.VMEM((CHID + 16, 2 * LANES), bf),
            pltpu.VMEM((DEEP, R_END, 2 * LANES), bf),
            pltpu.SMEM((SLOTS,), jnp.int32),
            pltpu.SemaphoreType.DMA((DEEP, 4)),
        ],
        compiler_params=pltpu.CompilerParams(vmem_limit_bytes=40 * 1024 * 1024),
        cost_estimate=pl.CostEstimate(flops=2 * 10**10, bytes_accessed=3 * 10**7, transcendentals=0),
    )(live, center, rays, cot, saved, raycode, small, trunk, density, feature, code, radiance)


def run_unpack(packed, colors):
    f32 = jnp.float32
    shapes = [colors.shape, (63, 1, 256), (1, 2, 256, 256), (1, 256), (1, 128, 256), (27, 1, 128),
              (1, 32, 128), (3, 1, 128), (1, 32, 8192)]
    outs = pl.pallas_call(
        unpack_kernel,
        name="unpack_gradients",
        out_shape=tuple(jax.ShapeDtypeStruct(s, f32) for s in shapes),
        in_specs=[VMEM] * 4,
        out_specs=tuple(VMEM for _ in shapes),
        compiler_params=pltpu.CompilerParams(vmem_limit_bytes=32 * 1024 * 1024),
    )(packed, colors, jnp.asarray(POS_SELECT, jnp.bfloat16), jnp.asarray(VIEW_SELECT, jnp.bfloat16))
    colors, pos, trunk, density, feature, view, code, radiance, table = outs
    return (
        colors, pos.transpose(1, 2, 0), trunk, density, feature, view.transpose(1, 2, 0),
        code.transpose(0, 2, 1), radiance.transpose(1, 0, 2), table,
    )


MESH = pl.DeviceIdType.MESH
GROUP = SLOTS
REPS = 4
CHUNK = G_ROWS // (4 * REPS)


def place():
    return lax.axis_index("blk"), lax.axis_index("rep")


def partner(blk, rep, i):
    return lax.rem(blk + i, GROUP), lax.rem(rep + GROUP * REPS - i, REPS)


def meet(blk, rep):
    barrier = pltpu.get_barrier_semaphore()

    def greet(i, carry):
        pl.semaphore_signal(barrier, inc=1, device_id=partner(blk, rep, i), device_id_type=MESH)
        return carry

    lax.fori_loop(1, GROUP, greet, 0)
    pl.semaphore_wait(barrier, GROUP - 1)


def exchange(blk, rep, src, dst, send_sem, recv_sem):
    def copy(i):
        to_blk, to_rep = partner(blk, rep, i)
        return pltpu.make_async_remote_copy(
            src_ref=src.at[to_blk], dst_ref=dst.at[blk], send_sem=send_sem.at[i],
            recv_sem=recv_sem.at[i], device_id=(to_blk, to_rep), device_id_type=MESH,
        )

    def begin(i, carry):
        copy(i).start()
        return carry

    lax.fori_loop(1, GROUP, begin, 0)
    dst[blk] = src[blk]
    return copy


def finish(copy):
    def end(i, carry):
        copy(i).wait()
        return carry

    lax.fori_loop(1, GROUP, end, 0)


def scatter_kernel(
    tile_ref, live_ref, anchors_ref, directions_ref, codes_ref, out_ref, tiles, send, send_sem, recv_sem
):
    blk, rep = place()
    row = row_iota(8, TILE)
    for t in range(tiles.shape[0]):
        lanes = slice(t * TILE, (t + 1) * TILE)
        tiles[t, 0:3] = anchors_ref[:, lanes]
        tiles[t, 3:6] = directions_ref[:, lanes]
        tiles[t, 6:7] = codes_ref[t : t + 1, :].astype(jnp.float32)
        tiles[t, 7:8] = jnp.zeros((1, TILE), jnp.float32)
    for k in range(GROUP):
        flag = live_ref[k].astype(jnp.float32)
        send[k] = jnp.where(row == 7, flag, tiles[tile_ref[k]])
    meet(blk, rep)
    finish(exchange(blk, rep, send, out_ref, send_sem, recv_sem))


def blend_kernel(
    ids_ref, tile_ref, part_ref, grad_ref, colors_ref, cot_ref,
    back, cots, send, send_sem, recv_sem, send_sem2, recv_sem2,
):
    blk, rep = place()
    meet(blk, rep)
    finish(exchange(blk, rep, part_ref, back, send_sem, recv_sem))
    for t in range(cots.shape[0]):
        summed = back[ids_ref[0, t]] + back[ids_ref[1, t]] + back[ids_ref[2, t]]
        lanes = slice(t * TILE, (t + 1) * TILE)
        colors = summed[:3] / summed[3:4]
        colors_ref[:, lanes] = colors
        cot = grad_ref[:, lanes] * LOSS_SCALE / summed[3:4]
        cots[t] = jnp.concatenate([cot, -jnp.sum(cot * colors, 0, keepdims=True)], 0)
    for k in range(GROUP):
        send[k] = cots[tile_ref[k]]
    finish(exchange(blk, rep, send, cot_ref, send_sem2, recv_sem2))


def total_kernel(g_ref, out_ref, got, held, send_sem, recv_sem):
    blk, rep = place()
    up, down = lax.rem(rep + 1, REPS), lax.rem(rep + REPS - 1, REPS)
    barrier = pltpu.get_barrier_semaphore()
    for other in (up, down):
        pl.semaphore_signal(barrier, inc=1, device_id=(blk, other), device_id_type=MESH)
    pl.semaphore_wait(barrier, 2)
    rings = range(4)

    def chunk(ring, ahead):
        sign = 1 if ring % 2 == 0 else REPS - 1
        which = lax.rem(rep + sign * (ahead + REPS), REPS)
        return pl.ds(pl.multiple_of((ring * REPS + which) * CHUNK, 8), CHUNK)

    def copy(ring, step):
        if step == 0:
            src, dst = g_ref.at[chunk(ring, 0)], got.at[ring, 0]
        elif step < 3:
            src, dst = held.at[ring, step - 1], got.at[ring, step]
        else:
            rows = chunk(ring, 4 - step)
            src, dst = out_ref.at[rows], out_ref.at[rows]
        return pltpu.make_async_remote_copy(
            src_ref=src, dst_ref=dst, send_sem=send_sem.at[ring, step],
            recv_sem=recv_sem.at[ring, step],
            device_id=(blk, up if ring % 2 == 0 else down), device_id_type=MESH,
        )

    for ring in rings:
        copy(ring, 0).start()
    for step in range(6):
        for ring in rings:
            copy(ring, step).wait_recv()
            if step < 2:
                held[ring, step] = got[ring, step] + g_ref[chunk(ring, -step - 1), :]
            elif step == 2:
                out_ref[chunk(ring, 1), :] = got[ring, 2] + g_ref[chunk(ring, 1), :]
            if step < 5:
                copy(ring, step + 1).start()
    for step in range(6):
        for ring in rings:
            copy(ring, step).wait_send()


def communicate(kernel, name, number, args, specs, shapes, scratch):
    return pl.pallas_call(
        kernel,
        name=name,
        out_shape=shapes,
        in_specs=specs,
        out_specs=jax.tree.map(lambda _: VMEM, shapes),
        scratch_shapes=scratch,
        compiler_params=pltpu.CompilerParams(
            collective_id=number, has_side_effects=True, vmem_limit_bytes=16 * 1024 * 1024
        ),
        cost_estimate=pl.CostEstimate(flops=10**10, bytes_accessed=10**6, transcendentals=0),
    )(*args)


def run_scatter(tile_of, live, anchors, directions, codes):
    return communicate(
        scatter_kernel, "scatter_rays", 0, (tile_of, live, anchors, directions, codes),
        [SMEM, SMEM, VMEM, VMEM, VMEM],
        jax.ShapeDtypeStruct((GROUP, 8, TILE), jnp.float32),
        [pltpu.VMEM((codes.shape[0], 8, TILE), jnp.float32), pltpu.VMEM((GROUP, 8, TILE), jnp.float32)] + [pltpu.SemaphoreType.DMA((GROUP,))] * 2,
    )


def run_blend(ids, tile_of, part, grad):
    tiles = grad.shape[1] // TILE
    small = (GROUP, 4, TILE)
    return communicate(
        blend_kernel, "blend_colors", 1, (ids, tile_of, part, grad), [SMEM, SMEM, VMEM, VMEM],
        (jax.ShapeDtypeStruct(grad.shape, jnp.float32), jax.ShapeDtypeStruct(small, jnp.float32)),
        [pltpu.VMEM(small, jnp.float32), pltpu.VMEM((tiles, 4, TILE), jnp.float32),
         pltpu.VMEM(small, jnp.float32)] + [pltpu.SemaphoreType.DMA((GROUP,))] * 4,
    )


def run_total(packed):
    return communicate(
        total_kernel, "total_gradients", 2, (packed,), [VMEM],
        jax.ShapeDtypeStruct((G_ROWS, 256), jnp.float32),
        [pltpu.VMEM((4, 3, CHUNK, 256), jnp.float32), pltpu.VMEM((4, 2, CHUNK, 256), jnp.float32)]
        + [pltpu.SemaphoreType.DMA((4, 6))] * 2,
    )


def local(
    anchors, directions, app_ids, block_ids, color_grad, block_centers, pos_weight, trunk_weight,
    density_weight, feature_weight, view_weight, code_weight, radiance_weight, code_table,
):
    tiles = block_ids.shape[0]
    ids = block_ids.T
    peers = jnp.arange(SLOTS, dtype=jnp.int32)
    matches = (ids[:, :, None] == peers[None, None, :]).astype(jnp.int32)
    is_live = jnp.sum(matches, (0, 1))
    source_tile = jnp.sum(matches * jnp.arange(tiles, dtype=jnp.int32)[None, :, None], (0, 1))
    rays = run_scatter(source_tile, is_live, anchors, directions, app_ids.reshape(tiles, TILE))
    live = (rays[:, 7, 0] > 0.5).astype(jnp.int32)
    center = block_centers.T
    code = code_weight.transpose(0, 2, 1)
    part, saved, raycode, small = run_forward(
        live, center, rays, pos_weight.transpose(0, 2, 1), trunk_weight, density_weight, feature_weight,
        view_weight.transpose(0, 2, 1), code, radiance_weight, code_table,
    )
    colors, cot = run_blend(ids, source_tile, part, color_grad)
    packed = run_backward(
        live, center, rays, cot, saved, raycode, small, trunk_weight, density_weight,
        feature_weight, code, radiance_weight,
    )
    return run_unpack(run_total(packed), colors)


def solution(mesh):
    weights = (P("blk", None, None), P("blk", None, None, None), P("blk", None)) + (
        P("blk", None, None),
    ) * 5
    ray = P(None, ("blk", "rep"))
    return jax.shard_map(
        local,
        mesh=mesh,
        in_specs=(ray, ray, P(("blk", "rep")), P(("blk", "rep"), None), ray, P(None, "blk")) + weights,
        out_specs=(ray,) + weights,
        check_vma=False,
    )
```

```python
import numpy as np

import jax
import jax.numpy as jnp
from jax import lax
from jax.experimental import pallas as pl
from jax.experimental.pallas import tpu as pltpu
from jax.sharding import PartitionSpec as P

TILE = 128
SAMPLES = 4
SLOTS = 32
LANES = SAMPLES * TILE
HID = 256
CHID = 128
PC = 96
VC = 48
E = 32
RC = VC + E
LO = 256
SPACING = 0.5
LOSS_SCALE = 0.03125
DEEP = 3
PARTS_F = 4
PARTS_B = 4

R_H1 = PC
R_H2 = R_H1 + HID
R_H3 = R_H2 + HID
R_S = R_H3 + HID
R_END = R_S + CHID

G_T1 = 0
G_T2 = 256
G_FEAT = 512
G_TAB = 640
G_POS = 1664
G_VIEW = 1728
G_CODE = 1760
G_RAD = 1728
G_DEN = 1744
G_ROWS = 1792


def code_places(levels, half):
    raw = list(range(3))
    sines, cosines = [], []
    for level in range(levels):
        for c in range(3):
            row = (level // half) * 3 + c
            group = 2 * (level % half)
            sines.append(8 * (1 + group) + row)
            cosines.append(8 * (2 + group) + row)
    return raw + sines + cosines


def selection(places, width):
    out = np.zeros((len(places), width), np.float32)
    out[np.arange(len(places)), places] = 1.0
    return out


POS_SELECT = selection(code_places(10, 5), PC)
VIEW_SELECT = selection(code_places(4, 2), VC)


def mm(a, b):
    return lax.dot_general(a, b, (((1,), (0,)), ((), ())), preferred_element_type=jnp.float32)


def mm_nt(a, b):
    return lax.dot_general(a, b, (((1,), (1,)), ((), ())), preferred_element_type=jnp.float32)


def mm_tn(a, b):
    return lax.dot_general(a, b, (((0,), (0,)), ((), ())), preferred_element_type=jnp.float32)


def softplus(v):
    return jnp.maximum(v, jnp.log(1.0 + jnp.exp(jnp.minimum(v, 80.0))))


def row_iota(rows, lanes):
    return lax.broadcasted_iota(jnp.int32, (rows, lanes), 0)


def ray_rows(ray, row):
    o8 = jnp.where(row < 3, ray, jnp.where(row < 6, pltpu.roll(ray, 3, 0), 0.0))
    d8 = jnp.where(row < 3, pltpu.roll(ray, 5, 0), jnp.where(row < 6, ray, 0.0))
    return o8, d8


def center_rows(center_ref, row):
    third = jnp.where(row >= 3, row - 3, row)
    return jnp.where(
        third == 0,
        center_ref[0, 0],
        jnp.where(third == 1, center_ref[0, 1], jnp.where(third == 2, center_ref[0, 2], 0.0)),
    )


def code_groups(values, doublings):
    groups = [values]
    sine, cosine = jnp.sin(values), jnp.cos(values)
    for step in range(doublings):
        groups += [sine, cosine]
        if step + 1 < doublings:
            sine, cosine = 2.0 * sine * cosine, (cosine - sine) * (cosine + sine)
    groups.append(jnp.zeros_like(values))
    return jnp.concatenate(groups, 0).astype(jnp.bfloat16)


def halves(x):
    return x[:, :TILE], x[:, TILE:]


def over_samples(x):
    return [
        jnp.concatenate([x[:, s * TILE : (s + 1) * TILE], x[:, LANES + s * TILE : LANES + (s + 1) * TILE]], 1)
        for s in range(SAMPLES)
    ]


def by_samples(pieces):
    return jnp.concatenate([halves(p)[h] for h in range(2) for p in pieces], 1)


def composite(small, o8, c8, row):
    density = over_samples(softplus(small))
    rad = over_samples(1.0 / (1.0 + jnp.exp(-small)))
    off = o8 - c8
    off2 = jnp.sum(jnp.where(row < 3, off * off, 0.0), 0, keepdims=True)
    inv = 1.0 / (1.0 + off2)
    depth = jnp.zeros((1, 2 * TILE), jnp.float32)
    before = jnp.ones((1, 2 * TILE), jnp.float32)
    weights, after = [], []
    for s in range(SAMPLES):
        u = density[s][3:4] * SPACING
        weights.append(before * (1.0 - jnp.exp(-u)))
        depth = depth + u
        before = jnp.exp(-depth)
        after.append(before)
    color = sum(w * r for w, r in zip(weights, rad))
    opacity = sum(weights)
    return rad, weights, after, color, (0.1 + opacity) * inv, inv


def list_live(live_ref, slots):
    def listing(s, count):
        @pl.when(live_ref[s] > 0)
        def _():
            slots[count] = s

        return count + (live_ref[s] > 0).astype(jnp.int32)

    total = lax.fori_loop(0, SLOTS, listing, jnp.int32(0))

    @pl.when(total % 2 == 1)
    def _():
        slots[total] = slots[total - 1]

    return total, (total + 1) // 2


def pair_copies(buf, saved_ref, sem, j, out):
    slot = lax.rem(j, DEEP)
    copies = []
    for n, (lo, hi) in enumerate(((0, 256), (256, 512), (512, 752), (752, R_END))):
        near, far = buf.at[slot, lo:hi], saved_ref.at[j, lo:hi]
        src, dst = (near, far) if out else (far, near)
        copies.append(pltpu.make_async_copy(src, dst, sem.at[slot, n]))
    return copies


def hot_lanes(ids):
    lo, hi = ids & (LO - 1), ids >> 8
    return (row_iota(LO, 2 * TILE) == lo).astype(jnp.float32).astype(jnp.bfloat16), hi


def lane_parts(parts):
    width = 2 * LANES // parts
    return [slice(p * width, (p + 1) * width) for p in range(parts)]


def forward_kernel(
    live_ref, center_ref, rays_ref, pos_ref, trunk_ref, density_ref, feature_ref, view_ref,
    code_ref, radiance_ref, table_ref, pos_select_ref, view_select_ref,
    part_ref, saved_ref, raycode_ref, small_ref,
    wp, wfd, wray, wrad, tab, buf, slots, sem,
):
    row = row_iota(8, 2 * TILE)
    c8 = center_rows(center_ref, row)
    wp[...] = mm_tn(pos_select_ref[...], pos_ref[0]).T.astype(jnp.bfloat16)
    wray[...] = jnp.concatenate(
        [mm_tn(view_select_ref[...], view_ref[0]), code_ref[0].astype(jnp.float32)], 0
    ).T.astype(jnp.bfloat16)
    wfd[:CHID, :] = feature_ref[0]
    row16 = row_iota(16, HID)
    wfd[CHID:, :] = jnp.where(row16 == 3, density_ref[...].astype(jnp.float32), 0.0).astype(jnp.bfloat16)
    wrad[...] = jnp.concatenate(
        [radiance_ref[0].astype(jnp.float32), jnp.zeros((5, CHID), jnp.float32)], 0
    ).astype(jnp.bfloat16)
    for h in range(SLOTS):
        tab[h * E : (h + 1) * E, :] = table_ref[0, :, h * LO : (h + 1) * LO]
    pos_scale = jnp.where(row < 3, 1.0, 32.0)
    view_scale = jnp.where(row < 3, 1.0, 4.0)
    total, pairs = list_live(live_ref, slots)

    def finish_pair(j):
        s0, s1 = slots[2 * j], slots[2 * j + 1]
        o8, _ = ray_rows(jnp.concatenate([rays_ref[s0], rays_ref[s1]], 1), row)
        _, _, _, color, share, _ = composite(small_ref[j], o8, c8, row)
        first, second = halves(jnp.where(row < 3, color * share, share)[:4])
        part_ref[s0] = first
        part_ref[s1] = second

    def pair(j, carry):
        @pl.when(j >= DEEP)
        def _():
            for copy in pair_copies(buf, saved_ref, sem, j - DEEP, True):
                copy.wait()

        out = buf.at[lax.rem(j, DEEP)]
        s0, s1 = slots[2 * j], slots[2 * j + 1]
        ray = jnp.concatenate([rays_ref[s0], rays_ref[s1]], 1)
        o8, d8 = ray_rows(ray, row)
        points = by_samples(
            [(o8 + (t + 0.5) * SPACING * d8 - c8) * pos_scale for t in range(SAMPLES)]
        )
        out[:PC, :] = code_groups(points, 5)
        hot, hi = hot_lanes(ray[6:7].astype(jnp.int32))
        rows = mm(tab[...], hot)
        app = jnp.zeros((E, 2 * TILE), jnp.float32)
        for h in range(SLOTS):
            app = app + jnp.where(hi == h, rows[h * E : (h + 1) * E], 0.0)
        raycode = jnp.concatenate([code_groups(d8 * view_scale, 2), app.astype(jnp.bfloat16)], 0)
        raycode_ref[j] = raycode
        per_ray = mm(wray[...], raycode)
        finish_pair(jnp.maximum(j - 1, 0))
        lanes = lane_parts(PARTS_F)
        for w, lo, mid, hi_row in (
            (wp, 0, R_H1, R_H2), (trunk_ref.at[0, 0], R_H1, R_H2, R_H3), (trunk_ref.at[0, 1], R_H2, R_H3, R_S)
        ):
            for part in lanes:
                out[mid:hi_row, part] = softplus(mm(w[...], out[lo:mid, part])).astype(jnp.bfloat16)
        ray_lanes = by_samples([per_ray] * SAMPLES)
        small = []
        for part in lanes:
            both = mm(wfd[...], out[R_H3:R_S, part])
            shaded = softplus(both[:CHID] + ray_lanes[:, part]).astype(jnp.bfloat16)
            out[R_S:R_END, part] = shaded
            logits = mm(wrad[...], shaded)
            small.append(jnp.where(row_iota(8, logits.shape[1]) == 3, both[CHID : CHID + 8], logits))
        small = jnp.concatenate(small, 1)
        small_ref[j] = small
        for copy in pair_copies(buf, saved_ref, sem, j, True):
            copy.start()
        return carry

    small_ref[0] = jnp.zeros_like(small_ref[0])
    lax.fori_loop(0, pairs, pair, jnp.int32(0))

    @pl.when(pairs > 0)
    def _():
        finish_pair(pairs - 1)

    def drain(j, carry):
        for copy in pair_copies(buf, saved_ref, sem, j, True):
            copy.wait()
        return carry

    lax.fori_loop(jnp.maximum(pairs - DEEP, 0), pairs, drain, jnp.int32(0))


def backward_kernel(
    live_ref, center_ref, rays_ref, cot_ref, saved_ref, raycode_ref, small_ref, trunk_ref,
    density_ref, feature_ref, code_ref, radiance_ref, pos_select_ref, view_select_ref,
    g_ref,
    t1, t2, fdt, radt, dz0, dz1, dz2, dz3, d_logits, g_pos, g_ray, buf, slots, sem,
):
    total, pairs = list_live(live_ref, slots)

    def fetch(j, carry):
        for copy in pair_copies(buf, saved_ref, sem, j, False):
            copy.start()
        return carry

    lax.fori_loop(0, jnp.minimum(pairs, DEEP - 1), fetch, jnp.int32(0))
    row = row_iota(8, 2 * TILE)
    lane = lax.broadcasted_iota(jnp.int32, (1, 2 * TILE), 1)
    c8 = center_rows(center_ref, row)

    def flip(x):
        return x.astype(jnp.float32).T.astype(jnp.bfloat16)

    t1[...] = flip(trunk_ref[0, 0])
    t2[...] = flip(trunk_ref[0, 1])
    fdt[:, :CHID] = flip(feature_ref[0])
    row16 = row_iota(16, HID)
    fdt[:, CHID:] = jnp.where(row16 == 3, density_ref[...].astype(jnp.float32), 0.0).T.astype(jnp.bfloat16)
    radt[...] = jnp.concatenate(
        [radiance_ref[0].astype(jnp.float32), jnp.zeros((13, CHID), jnp.float32)], 0
    ).T.astype(jnp.bfloat16)
    g_ref[...] = jnp.zeros_like(g_ref)
    g_pos[...] = jnp.zeros_like(g_pos)
    g_ray[...] = jnp.zeros_like(g_ray)

    def start_pair(j):
        s0, s1 = slots[2 * j], slots[2 * j + 1]
        ray = jnp.concatenate([rays_ref[s0], rays_ref[s1]], 1)
        o8, _ = ray_rows(ray, row)
        small = small_ref[j]
        rad, weights, after, color, share, inv = composite(small, o8, c8, row)
        cot = jnp.concatenate([cot_ref[s0], cot_ref[s1]], 1)
        cot = jnp.where((lane < TILE) | (2 * j + 1 < total), cot, 0.0)
        cot = jnp.concatenate([cot, jnp.zeros_like(cot)], 0)
        d_share = jnp.sum(
            jnp.where(row < 3, cot * color, jnp.where(row == 3, cot, 0.0)), 0, keepdims=True
        )
        d_color = jnp.where(row < 3, cot * share, 0.0)
        d_opacity = d_share * inv
        sig = rad
        later = jnp.zeros((1, 2 * TILE), jnp.float32)
        pieces = [None] * SAMPLES
        for t in reversed(range(SAMPLES)):
            d_w = jnp.sum(d_color * rad[t], 0, keepdims=True) + d_opacity
            d_u = d_w * after[t] - later
            later = later + d_w * weights[t]
            d_logit = d_color * weights[t] * rad[t] * (1.0 - rad[t])
            pieces[t] = jnp.where(
                row < 3, d_logit, jnp.where(row == 3, d_u * SPACING * sig[t], 0.0)
            )
        d_small = by_samples(pieces)
        d_logits[...] = jnp.concatenate([d_small, jnp.zeros_like(d_small)], 0).astype(jnp.bfloat16)

    @pl.when(pairs > 0)
    def _():
        start_pair(0)

    def pair(j, carry):
        for copy in pair_copies(buf, saved_ref, sem, j, False):
            copy.wait()

        @pl.when(j + DEEP - 1 < pairs)
        def _():
            fetch(j + DEEP - 1, carry)

        act = buf.at[lax.rem(j, DEEP)]
        ray = jnp.concatenate([rays_ref[slots[2 * j]], rays_ref[slots[2 * j + 1]]], 1)
        dz3[CHID:, :] = d_logits[...]

        def through(grad, lo_row, hi_row, part):
            value = act[lo_row:hi_row, part].astype(jnp.float32)
            return grad * (1.0 - jnp.exp(-value))

        lanes = lane_parts(PARTS_B)
        d_feature = []
        for part in lanes:
            piece = through(mm(radt[...], dz3[CHID:, part]), R_S, R_END, part)
            dz3[:CHID, part] = piece.astype(jnp.bfloat16)
            d_feature.append(piece)
        d_ray = sum(over_samples(jnp.concatenate(d_feature, 1))).astype(jnp.bfloat16)
        start_pair(jnp.minimum(j + 1, pairs - 1))
        for wt, src, dst, lo, hi in (
            (fdt, dz3, dz2, R_H3, R_S), (t2, dz2, dz1, R_H2, R_H3), (t1, dz1, dz0, R_H1, R_H2)
        ):
            for part in lanes:
                dst[:, part] = through(mm(wt[...], src[:, part]), lo, hi, part).astype(jnp.bfloat16)
            if src is dz3:
                d_app = mm(code_ref[0], d_ray)
                hot, high = hot_lanes(ray[6:7].astype(jnp.int32))
                spread = jnp.concatenate(
                    [jnp.where(high == h, d_app, 0.0).astype(jnp.bfloat16) for h in range(SLOTS)], 0
                )
                g_ray[...] += mm_nt(d_ray, raycode_ref[j])
                g_ref[G_RAD:G_DEN, 128:256] += mm_nt(dz3[CHID:, :], act[R_S:R_END, :])
                d_both = mm_nt(dz3[...], act[R_H3:R_S, :])
                g_ref[G_FEAT:G_TAB, :] += d_both[:CHID]
                g_ref[G_DEN : G_DEN + 16, 128:256] += d_both[CHID:, :128]
                g_ref[G_DEN + 16 : G_DEN + 32, 128:256] += d_both[CHID:, 128:]
                g_ref[G_TAB:G_POS, :] += mm_nt(spread, hot)
            elif src is dz2:
                g_ref[G_T2:G_FEAT, :] += mm_nt(dz2[...], act[R_H2:R_H3, :])
            else:
                g_ref[G_T1:G_T2, :] += mm_nt(dz1[...], act[R_H1:R_H2, :])
        g_pos[...] += mm_nt(dz0[...], act[:PC, :])
        return carry

    lax.fori_loop(0, pairs, pair, jnp.int32(0))

    def pick(a, select):
        return lax.dot_general(
            select.astype(jnp.float32), a, (((1,), (1,)), ((), ())),
            preferred_element_type=jnp.float32, precision=lax.Precision.HIGHEST,
        )

    g_ref[G_POS : G_POS + 63, :] = pick(g_pos[...], pos_select_ref[...])
    g_ref[G_VIEW : G_VIEW + 27, :128] = pick(g_ray[:, :VC], view_select_ref[...])
    g_ref[G_CODE : G_CODE + E, :128] = g_ray[...].T[VC:]


def unpack_kernel(
    g_ref, got_colors_ref,
    colors_ref, pos_ref, trunk_ref, density_ref, feature_ref, view_ref, code_ref, radiance_ref, table_ref,
):
    colors_ref[...] = got_colors_ref[...]
    for n in range(63):
        pos_ref[n] = g_ref[G_POS + n : G_POS + n + 1, :]
    trunk_ref[0, 0] = g_ref[G_T1:G_T2, :]
    trunk_ref[0, 1] = g_ref[G_T2:G_FEAT, :]
    feature_ref[0] = g_ref[G_FEAT:G_TAB, :]
    density_ref[:, :128] = g_ref[G_DEN + 3 : G_DEN + 4, 128:256]
    density_ref[:, 128:] = g_ref[G_DEN + 19 : G_DEN + 20, 128:256]
    for n in range(27):
        view_ref[n] = g_ref[G_VIEW + n : G_VIEW + n + 1, :128]
    code_ref[0] = g_ref[G_CODE : G_CODE + E, :128]
    for n in range(3):
        radiance_ref[n] = g_ref[G_RAD + n : G_RAD + n + 1, 128:256]
    for h in range(SLOTS):
        table_ref[0, :, h * LO : (h + 1) * LO] = g_ref[G_TAB + h * E : G_TAB + (h + 1) * E, :]


VMEM = pl.BlockSpec(memory_space=pltpu.VMEM)
SMEM = pl.BlockSpec(memory_space=pltpu.SMEM)
ANY = pl.BlockSpec(memory_space=pl.ANY)


def run_forward(live, center, rays, pos, trunk, density, feature, view, code, radiance, table):
    bf = jnp.bfloat16
    return pl.pallas_call(
        forward_kernel,
        name="forward_tiles",
        out_shape=(
            jax.ShapeDtypeStruct((SLOTS, 4, TILE), jnp.float32),
            jax.ShapeDtypeStruct((SLOTS // 2, R_END, 2 * LANES), bf),
            jax.ShapeDtypeStruct((SLOTS // 2, RC, 2 * TILE), bf),
            jax.ShapeDtypeStruct((SLOTS // 2, 8, 2 * LANES), jnp.float32),
        ),
        in_specs=[SMEM, SMEM] + [VMEM] * 11,
        out_specs=(VMEM, ANY, VMEM, VMEM),
        scratch_shapes=[
            pltpu.VMEM((HID, PC), bf),
            pltpu.VMEM((CHID + 16, HID), bf),
            pltpu.VMEM((CHID, RC), bf),
            pltpu.VMEM((8, CHID), bf),
            pltpu.VMEM((SLOTS * E, LO), bf),
            pltpu.VMEM((DEEP, R_END, 2 * LANES), bf),
            pltpu.SMEM((SLOTS,), jnp.int32),
            pltpu.SemaphoreType.DMA((DEEP, 4)),
        ],
        compiler_params=pltpu.CompilerParams(vmem_limit_bytes=40 * 1024 * 1024),
        cost_estimate=pl.CostEstimate(flops=10**10, bytes_accessed=3 * 10**7, transcendentals=0),
    )(live, center, rays, pos, trunk, density, feature, view, code, radiance, table,
      jnp.asarray(POS_SELECT, bf), jnp.asarray(VIEW_SELECT, bf))


def run_backward(live, center, rays, cot, saved, raycode, small, trunk, density, feature, code, radiance):
    bf = jnp.bfloat16
    return pl.pallas_call(
        backward_kernel,
        name="backward_tiles",
        out_shape=jax.ShapeDtypeStruct((G_ROWS, 256), jnp.float32),
        in_specs=[SMEM, SMEM, VMEM, VMEM, ANY] + [VMEM] * 9,
        out_specs=VMEM,
        scratch_shapes=[
            pltpu.VMEM((HID, HID), bf),
            pltpu.VMEM((HID, HID), bf),
            pltpu.VMEM((HID, CHID + 16), bf),
            pltpu.VMEM((CHID, 16), bf),
            pltpu.VMEM((HID, 2 * LANES), bf),
            pltpu.VMEM((HID, 2 * LANES), bf),
            pltpu.VMEM((HID, 2 * LANES), bf),
            pltpu.VMEM((CHID + 16, 2 * LANES), bf),
            pltpu.VMEM((16, 2 * LANES), bf),
            pltpu.VMEM((HID, PC), jnp.float32),
            pltpu.VMEM((CHID, RC), jnp.float32),
            pltpu.VMEM((DEEP, R_END, 2 * LANES), bf),
            pltpu.SMEM((SLOTS,), jnp.int32),
            pltpu.SemaphoreType.DMA((DEEP, 4)),
        ],
        compiler_params=pltpu.CompilerParams(vmem_limit_bytes=40 * 1024 * 1024),
        cost_estimate=pl.CostEstimate(flops=2 * 10**10, bytes_accessed=3 * 10**7, transcendentals=0),
    )(live, center, rays, cot, saved, raycode, small, trunk, density, feature, code, radiance,
      jnp.asarray(POS_SELECT, bf), jnp.asarray(VIEW_SELECT, bf))


def run_unpack(packed, colors):
    f32 = jnp.float32
    shapes = [colors.shape, (63, 1, 256), (1, 2, 256, 256), (1, 256), (1, 128, 256), (27, 1, 128),
              (1, 32, 128), (3, 1, 128), (1, 32, 8192)]
    outs = pl.pallas_call(
        unpack_kernel,
        name="unpack_gradients",
        out_shape=tuple(jax.ShapeDtypeStruct(s, f32) for s in shapes),
        in_specs=[VMEM] * 2,
        out_specs=tuple(VMEM for _ in shapes),
        compiler_params=pltpu.CompilerParams(vmem_limit_bytes=32 * 1024 * 1024),
    )(packed, colors)
    colors, pos, trunk, density, feature, view, code, radiance, table = outs
    return (
        colors, pos.transpose(1, 2, 0), trunk, density, feature, view.transpose(1, 2, 0),
        code.transpose(0, 2, 1), radiance.transpose(1, 0, 2), table,
    )


MESH = pl.DeviceIdType.MESH
GROUP = SLOTS
REPS = 4
CHUNK = G_ROWS // (4 * REPS)


def place():
    return lax.axis_index("blk"), lax.axis_index("rep")


def partner(blk, rep, i):
    return lax.rem(blk + i, GROUP), lax.rem(rep + GROUP * REPS - i, REPS)


def meet(blk, rep):
    barrier = pltpu.get_barrier_semaphore()
    for i in range(1, GROUP):
        pl.semaphore_signal(barrier, inc=1, device_id=partner(blk, rep, i), device_id_type=MESH)
    pl.semaphore_wait(barrier, GROUP - 1)


def exchange(blk, rep, src, dst, send_sem, recv_sem):
    for i in range(1, GROUP):
        to_blk, to_rep = partner(blk, rep, i)
        pltpu.make_async_remote_copy(
            src_ref=src.at[to_blk], dst_ref=dst.at[blk], send_sem=send_sem,
            recv_sem=recv_sem, device_id=(to_blk, to_rep), device_id_type=MESH,
        ).start()
    dst[blk] = src[blk]
    most = pl.ds(0, GROUP - 1)
    return pltpu.make_async_remote_copy(
        src_ref=src.at[most], dst_ref=dst.at[most], send_sem=send_sem, recv_sem=recv_sem,
        device_id=partner(blk, rep, 1), device_id_type=MESH,
    )


def finish(everything):
    everything.wait_recv()
    everything.wait_send()


def scatter_kernel(
    tile_ref, live_ref, anchors_ref, directions_ref, codes_ref, out_ref, tiles, send, send_sem, recv_sem
):
    blk, rep = place()
    row = row_iota(8, TILE)
    for t in range(tiles.shape[0]):
        lanes = slice(t * TILE, (t + 1) * TILE)
        tiles[t, 0:3] = anchors_ref[:, lanes]
        tiles[t, 3:6] = directions_ref[:, lanes]
        tiles[t, 6:7] = codes_ref[t : t + 1, :].astype(jnp.float32)
        tiles[t, 7:8] = jnp.zeros((1, TILE), jnp.float32)
    for k in range(GROUP):
        flag = live_ref[k].astype(jnp.float32)
        send[k] = jnp.where(row == 7, flag, tiles[tile_ref[k]])
    meet(blk, rep)
    finish(exchange(blk, rep, send, out_ref, send_sem, recv_sem))


def blend_kernel(
    ids_ref, tile_ref, part_ref, grad_ref, colors_ref, cot_ref,
    back, cots, send, send_sem, recv_sem, send_sem2, recv_sem2,
):
    blk, rep = place()
    meet(blk, rep)
    finish(exchange(blk, rep, part_ref, back, send_sem, recv_sem))
    for t in range(cots.shape[0]):
        summed = back[ids_ref[0, t]] + back[ids_ref[1, t]] + back[ids_ref[2, t]]
        lanes = slice(t * TILE, (t + 1) * TILE)
        colors = summed[:3] / summed[3:4]
        colors_ref[:, lanes] = colors
        cot = grad_ref[:, lanes] * LOSS_SCALE / summed[3:4]
        cots[t] = jnp.concatenate([cot, -jnp.sum(cot * colors, 0, keepdims=True)], 0)
    for k in range(GROUP):
        send[k] = cots[tile_ref[k]]
    finish(exchange(blk, rep, send, cot_ref, send_sem2, recv_sem2))


def total_kernel(g_ref, out_ref, got, held, send_sem, recv_sem):
    blk, rep = place()
    up, down = lax.rem(rep + 1, REPS), lax.rem(rep + REPS - 1, REPS)
    barrier = pltpu.get_barrier_semaphore()
    for other in (up, down):
        pl.semaphore_signal(barrier, inc=1, device_id=(blk, other), device_id_type=MESH)
    pl.semaphore_wait(barrier, 2)
    rings = range(4)

    def chunk(ring, ahead):
        sign = 1 if ring % 2 == 0 else REPS - 1
        which = lax.rem(rep + sign * (ahead + REPS), REPS)
        return pl.ds(pl.multiple_of((ring * REPS + which) * CHUNK, 8), CHUNK)

    def copy(ring, step):
        if step == 0:
            src, dst = g_ref.at[chunk(ring, 0)], got.at[ring, 0]
        elif step < 3:
            src, dst = held.at[ring, step - 1], got.at[ring, step]
        else:
            rows = chunk(ring, 4 - step)
            src, dst = out_ref.at[rows], out_ref.at[rows]
        return pltpu.make_async_remote_copy(
            src_ref=src, dst_ref=dst, send_sem=send_sem.at[ring, step],
            recv_sem=recv_sem.at[ring, step],
            device_id=(blk, up if ring % 2 == 0 else down), device_id_type=MESH,
        )

    for ring in rings:
        copy(ring, 0).start()
    for step in range(6):
        for ring in rings:
            copy(ring, step).wait_recv()
            if step < 2:
                held[ring, step] = got[ring, step] + g_ref[chunk(ring, -step - 1), :]
            elif step == 2:
                out_ref[chunk(ring, 1), :] = got[ring, 2] + g_ref[chunk(ring, 1), :]
            if step < 5:
                copy(ring, step + 1).start()
    for step in range(6):
        for ring in rings:
            copy(ring, step).wait_send()


def communicate(kernel, name, number, args, specs, shapes, scratch):
    return pl.pallas_call(
        kernel,
        name=name,
        out_shape=shapes,
        in_specs=specs,
        out_specs=jax.tree.map(lambda _: VMEM, shapes),
        scratch_shapes=scratch,
        compiler_params=pltpu.CompilerParams(
            collective_id=number, has_side_effects=True, vmem_limit_bytes=16 * 1024 * 1024
        ),
        cost_estimate=pl.CostEstimate(flops=10**10, bytes_accessed=10**6, transcendentals=0),
    )(*args)


def run_scatter(tile_of, live, anchors, directions, codes):
    return communicate(
        scatter_kernel, "scatter_rays", 0, (tile_of, live, anchors, directions, codes),
        [SMEM, SMEM, VMEM, VMEM, VMEM],
        jax.ShapeDtypeStruct((GROUP, 8, TILE), jnp.float32),
        [pltpu.VMEM((codes.shape[0], 8, TILE), jnp.float32), pltpu.VMEM((GROUP, 8, TILE), jnp.float32)] + [pltpu.SemaphoreType.DMA] * 2,
    )


def run_blend(ids, tile_of, part, grad):
    tiles = grad.shape[1] // TILE
    small = (GROUP, 4, TILE)
    return communicate(
        blend_kernel, "blend_colors", 1, (ids, tile_of, part, grad), [SMEM, SMEM, VMEM, VMEM],
        (jax.ShapeDtypeStruct(grad.shape, jnp.float32), jax.ShapeDtypeStruct(small, jnp.float32)),
        [pltpu.VMEM(small, jnp.float32), pltpu.VMEM((tiles, 4, TILE), jnp.float32),
         pltpu.VMEM(small, jnp.float32)] + [pltpu.SemaphoreType.DMA] * 4,
    )


def run_total(packed):
    return communicate(
        total_kernel, "total_gradients", 2, (packed,), [VMEM],
        jax.ShapeDtypeStruct((G_ROWS, 256), jnp.float32),
        [pltpu.VMEM((4, 3, CHUNK, 256), jnp.float32), pltpu.VMEM((4, 2, CHUNK, 256), jnp.float32)]
        + [pltpu.SemaphoreType.DMA((4, 6))] * 2,
    )


def local(
    anchors, directions, app_ids, block_ids, color_grad, block_centers, pos_weight, trunk_weight,
    density_weight, feature_weight, view_weight, code_weight, radiance_weight, code_table,
):
    tiles = block_ids.shape[0]
    ids = block_ids.T
    peers = jnp.arange(SLOTS, dtype=jnp.int32)
    matches = (ids[:, :, None] == peers[None, None, :]).astype(jnp.int32)
    is_live = jnp.sum(matches, (0, 1))
    source_tile = jnp.sum(matches * jnp.arange(tiles, dtype=jnp.int32)[None, :, None], (0, 1))
    rays = run_scatter(source_tile, is_live, anchors, directions, app_ids.reshape(tiles, TILE))
    live = (rays[:, 7, 0] > 0.5).astype(jnp.int32)
    center = block_centers.T
    code = code_weight.transpose(0, 2, 1)
    part, saved, raycode, small = run_forward(
        live, center, rays, pos_weight.transpose(0, 2, 1), trunk_weight, density_weight, feature_weight,
        view_weight.transpose(0, 2, 1), code, radiance_weight, code_table,
    )
    colors, cot = run_blend(ids, source_tile, part, color_grad)
    packed = run_backward(
        live, center, rays, cot, saved, raycode, small, trunk_weight, density_weight,
        feature_weight, code, radiance_weight,
    )
    return run_unpack(run_total(packed), colors)


def solution(mesh):
    weights = (P("blk", None, None), P("blk", None, None, None), P("blk", None)) + (
        P("blk", None, None),
    ) * 5
    ray = P(None, ("blk", "rep"))
    return jax.shard_map(
        local,
        mesh=mesh,
        in_specs=(ray, ray, P(("blk", "rep")), P(("blk", "rep"), None), ray, P(None, "blk")) + weights,
        out_specs=(ray,) + weights,
        check_vma=False,
    )
```

```python
import numpy as np

import jax
import jax.numpy as jnp
from jax import lax
from jax.experimental import pallas as pl
from jax.experimental.pallas import tpu as pltpu
from jax.sharding import PartitionSpec as P

TILE = 128
SAMPLES = 4
SLOTS = 32
LANES = SAMPLES * TILE
HID = 256
CHID = 128
PC = 96
VC = 48
E = 32
RC = VC + E
LO = 256
SPACING = 0.5
LOSS_SCALE = 0.03125
DEEP = 3
PARTS_F = 4
PARTS_B = 4

R_H1 = PC
R_H2 = R_H1 + HID
R_H3 = R_H2 + HID
R_S = R_H3 + HID
R_END = R_S + CHID
GATHER_AFTER = R_H2

G_T1 = 0
G_T2 = 256
G_FEAT = 512
G_TAB = 640
G_POS = 1664
G_VIEW = 1728
G_CODE = 1760
G_RAD = 1728
G_DEN = 1744
G_ROWS = 1792


def code_places(levels, half):
    raw = list(range(3))
    sines, cosines = [], []
    for level in range(levels):
        for c in range(3):
            row = (level // half) * 3 + c
            group = 2 * (level % half)
            sines.append(8 * (1 + group) + row)
            cosines.append(8 * (2 + group) + row)
    return raw + sines + cosines


def selection(places, width):
    out = np.zeros((len(places), width), np.float32)
    out[np.arange(len(places)), places] = 1.0
    return out


POS_SELECT = selection(code_places(10, 5), PC)
VIEW_SELECT = selection(code_places(4, 2), VC)


def mm(a, b):
    return lax.dot_general(a, b, (((1,), (0,)), ((), ())), preferred_element_type=jnp.float32)


def mm_nt(a, b):
    return lax.dot_general(a, b, (((1,), (1,)), ((), ())), preferred_element_type=jnp.float32)


def mm_tn(a, b):
    return lax.dot_general(a, b, (((0,), (0,)), ((), ())), preferred_element_type=jnp.float32)


def softplus(v):
    return jnp.maximum(v, jnp.log(1.0 + jnp.exp(jnp.minimum(v, 80.0))))


def row_iota(rows, lanes):
    return lax.broadcasted_iota(jnp.int32, (rows, lanes), 0)


def ray_rows(ray, row):
    o8 = jnp.where(row < 3, ray, jnp.where(row < 6, pltpu.roll(ray, 3, 0), 0.0))
    d8 = jnp.where(row < 3, pltpu.roll(ray, 5, 0), jnp.where(row < 6, ray, 0.0))
    return o8, d8


def center_rows(center_ref, row):
    third = jnp.where(row >= 3, row - 3, row)
    return jnp.where(
        third == 0,
        center_ref[0, 0],
        jnp.where(third == 1, center_ref[0, 1], jnp.where(third == 2, center_ref[0, 2], 0.0)),
    )


def sine_cosine(x):
    turns = jnp.round(x * 0.6366197723675814)
    r = x - turns * 1.5703125
    r = r - turns * 4.837512969970703e-4
    r = r - turns * 7.549789948768648e-8
    q = turns.astype(jnp.int32)
    z = r * r
    sine = r + r * z * (-1.6666654611e-1 + z * (8.3321608736e-3 - z * 1.9515295891e-4))
    cosine = 1.0 - 0.5 * z + z * z * (
        4.166664568298827e-2 + z * (-1.388731625493765e-3 + z * 2.443315711809948e-5)
    )
    odd = (q & 1) == 1
    first = jnp.where(odd, cosine, sine)
    second = jnp.where(odd, sine, cosine)
    return (
        jnp.where((q & 2) == 2, -first, first),
        jnp.where(((q + 1) & 2) == 2, -second, second),
    )


def code_groups(values, doublings):
    groups = [values]
    sine, cosine = sine_cosine(values)
    for step in range(doublings):
        groups += [sine, cosine]
        if step + 1 < doublings:
            sine, cosine = 2.0 * sine * cosine, (cosine - sine) * (cosine + sine)
    groups.append(jnp.zeros_like(values))
    return jnp.concatenate(groups, 0).astype(jnp.bfloat16)


def halves(x):
    return x[:, :TILE], x[:, TILE:]


def over_samples(x):
    return [
        jnp.concatenate([x[:, s * TILE : (s + 1) * TILE], x[:, LANES + s * TILE : LANES + (s + 1) * TILE]], 1)
        for s in range(SAMPLES)
    ]


def by_samples(pieces):
    return jnp.concatenate([halves(p)[h] for h in range(2) for p in pieces], 1)


def composite(small, o8, c8, row):
    density = over_samples(softplus(small))
    rad = over_samples(1.0 / (1.0 + jnp.exp(-small)))
    off = o8 - c8
    off2 = jnp.sum(jnp.where(row < 3, off * off, 0.0), 0, keepdims=True)
    inv = 1.0 / (1.0 + off2)
    depth = jnp.zeros((1, 2 * TILE), jnp.float32)
    before = jnp.ones((1, 2 * TILE), jnp.float32)
    weights, after = [], []
    for s in range(SAMPLES):
        u = density[s][3:4] * SPACING
        weights.append(before * (1.0 - jnp.exp(-u)))
        depth = depth + u
        before = jnp.exp(-depth)
        after.append(before)
    color = sum(w * r for w, r in zip(weights, rad))
    opacity = sum(weights)
    return rad, weights, after, color, (0.1 + opacity) * inv, inv


def list_live(live_ref, slots):
    total = jnp.int32(0)
    for s in range(SLOTS):
        slots[total] = jnp.int32(s)
        total = total + (live_ref[s] > 0).astype(jnp.int32)

    @pl.when(total % 2 == 1)
    def _():
        slots[total] = slots[total - 1]

    return total, (total + 1) // 2


def pair_copies(buf, saved_ref, sem, j, out):
    slot = lax.rem(j, DEEP)
    copies = []
    for n, (lo, hi) in enumerate(((0, 256), (256, 512), (512, 752), (752, R_END))):
        near, far = buf.at[slot, lo:hi], saved_ref.at[j, lo:hi]
        src, dst = (near, far) if out else (far, near)
        copies.append(pltpu.make_async_copy(src, dst, sem.at[slot, n]))
    return copies


def hot_lanes(ids):
    lo, hi = ids & (LO - 1), ids >> 8
    return (row_iota(LO, 2 * TILE) == lo).astype(jnp.float32).astype(jnp.bfloat16), hi


def lane_parts(parts):
    width = 2 * LANES // parts
    return [slice(p * width, (p + 1) * width) for p in range(parts)]


def forward_kernel(
    live_ref, center_ref, rays_ref, pos_ref, trunk_ref, density_ref, feature_ref, view_ref,
    code_ref, radiance_ref, table_ref, pos_select_ref, view_select_ref,
    part_ref, saved_ref, raycode_ref, small_ref,
    wp, wfd, wray, wrad, tab, buf, slots, sem,
):
    row = row_iota(8, 2 * TILE)
    c8 = center_rows(center_ref, row)
    wp[...] = mm_tn(pos_select_ref[...], pos_ref[0]).T.astype(jnp.bfloat16)
    wray[...] = jnp.concatenate(
        [mm_tn(view_select_ref[...], view_ref[0]), code_ref[0].astype(jnp.float32)], 0
    ).T.astype(jnp.bfloat16)
    wfd[:CHID, :] = feature_ref[0]
    row16 = row_iota(16, HID)
    wfd[CHID:, :] = jnp.where(row16 == 3, density_ref[...].astype(jnp.float32), 0.0).astype(jnp.bfloat16)
    wrad[...] = jnp.concatenate(
        [radiance_ref[0].astype(jnp.float32), jnp.zeros((5, CHID), jnp.float32)], 0
    ).astype(jnp.bfloat16)
    for h in range(SLOTS):
        tab[h * E : (h + 1) * E, :] = table_ref[0, :, h * LO : (h + 1) * LO]
    pos_scale = jnp.where(row < 3, 1.0, 32.0)
    view_scale = jnp.where(row < 3, 1.0, 4.0)
    total, pairs = list_live(live_ref, slots)

    def finish_pair(j):
        s0, s1 = slots[2 * j], slots[2 * j + 1]
        o8, _ = ray_rows(jnp.concatenate([rays_ref[s0], rays_ref[s1]], 1), row)
        _, _, _, color, share, _ = composite(small_ref[j], o8, c8, row)
        first, second = halves(jnp.where(row < 3, color * share, share)[:4])
        part_ref[s0] = first
        part_ref[s1] = second

    def pair(j, carry):
        @pl.when(j >= DEEP)
        def _():
            for copy in pair_copies(buf, saved_ref, sem, j - DEEP, True):
                copy.wait()

        out = buf.at[lax.rem(j, DEEP)]
        s0, s1 = slots[2 * j], slots[2 * j + 1]
        ray = jnp.concatenate([rays_ref[s0], rays_ref[s1]], 1)
        o8, d8 = ray_rows(ray, row)
        points = by_samples(
            [(o8 + (t + 0.5) * SPACING * d8 - c8) * pos_scale for t in range(SAMPLES)]
        )
        out[:PC, :] = code_groups(points, 5)
        finish_pair(jnp.maximum(j - 1, 0))
        lanes = lane_parts(PARTS_F)
        for w, lo, mid, hi_row in (
            (wp, 0, R_H1, R_H2), (trunk_ref.at[0, 0], R_H1, R_H2, R_H3), (trunk_ref.at[0, 1], R_H2, R_H3, R_S)
        ):
            for part in lanes:
                out[mid:hi_row, part] = softplus(mm(w[...], out[lo:mid, part])).astype(jnp.bfloat16)
            if mid == GATHER_AFTER:
                hot, hi = hot_lanes(ray[6:7].astype(jnp.int32))
                rows = mm(tab[...], hot)
                picks = [rows[h * E : (h + 1) * E] for h in range(SLOTS)]
                for bit in range(5):
                    on = ((hi >> bit) & 1) == 1
                    picks = [jnp.where(on, b, a) for a, b in zip(picks[::2], picks[1::2])]
                app = picks[0]
                raycode = jnp.concatenate([code_groups(d8 * view_scale, 2), app.astype(jnp.bfloat16)], 0)
                raycode_ref[j] = raycode
                per_ray = mm(wray[...], raycode)
        ray_lanes = by_samples([per_ray] * SAMPLES)
        small = []
        for part in lanes:
            both = mm(wfd[...], out[R_H3:R_S, part])
            shaded = softplus(both[:CHID] + ray_lanes[:, part]).astype(jnp.bfloat16)
            out[R_S:R_END, part] = shaded
            logits = mm(wrad[...], shaded)
            small.append(jnp.where(row_iota(8, logits.shape[1]) == 3, both[CHID : CHID + 8], logits))
        small = jnp.concatenate(small, 1)
        small_ref[j] = small
        for copy in pair_copies(buf, saved_ref, sem, j, True):
            copy.start()
        return carry

    small_ref[0] = jnp.zeros_like(small_ref[0])
    lax.fori_loop(0, pairs, pair, jnp.int32(0))

    @pl.when(pairs > 0)
    def _():
        finish_pair(pairs - 1)

    def drain(j, carry):
        for copy in pair_copies(buf, saved_ref, sem, j, True):
            copy.wait()
        return carry

    lax.fori_loop(jnp.maximum(pairs - DEEP, 0), pairs, drain, jnp.int32(0))


def backward_kernel(
    live_ref, center_ref, rays_ref, cot_ref, saved_ref, raycode_ref, small_ref, trunk_ref,
    density_ref, feature_ref, code_ref, radiance_ref, pos_select_ref, view_select_ref,
    g_ref,
    t1, t2, fdt, radt, dz0, dz1, dz2, dz3, d_logits, g_pos, g_ray, g_rad, buf, slots, sem,
):
    total, pairs = list_live(live_ref, slots)

    def fetch(j, carry):
        for copy in pair_copies(buf, saved_ref, sem, j, False):
            copy.start()
        return carry

    lax.fori_loop(0, jnp.minimum(pairs, DEEP - 1), fetch, jnp.int32(0))
    row = row_iota(8, 2 * TILE)
    lane = lax.broadcasted_iota(jnp.int32, (1, 2 * TILE), 1)
    c8 = center_rows(center_ref, row)

    def flip(x):
        return x.astype(jnp.float32).T.astype(jnp.bfloat16)

    t1[...] = flip(trunk_ref[0, 0])
    t2[...] = flip(trunk_ref[0, 1])
    fdt[:, :CHID] = flip(feature_ref[0])
    row16 = row_iota(16, HID)
    fdt[:, CHID:] = jnp.where(row16 == 3, density_ref[...].astype(jnp.float32), 0.0).T.astype(jnp.bfloat16)
    radt[...] = jnp.concatenate(
        [radiance_ref[0].astype(jnp.float32), jnp.zeros((13, CHID), jnp.float32)], 0
    ).T.astype(jnp.bfloat16)
    g_ref[...] = jnp.zeros_like(g_ref)
    g_pos[...] = jnp.zeros_like(g_pos)
    g_ray[...] = jnp.zeros_like(g_ray)
    g_rad[...] = jnp.zeros_like(g_rad)

    def start_pair(j):
        s0, s1 = slots[2 * j], slots[2 * j + 1]
        ray = jnp.concatenate([rays_ref[s0], rays_ref[s1]], 1)
        o8, _ = ray_rows(ray, row)
        small = small_ref[j]
        rad, weights, after, color, share, inv = composite(small, o8, c8, row)
        cot = jnp.concatenate([cot_ref[s0], cot_ref[s1]], 1)
        cot = jnp.where((lane < TILE) | (2 * j + 1 < total), cot, 0.0)
        cot = jnp.concatenate([cot, jnp.zeros_like(cot)], 0)
        d_share = jnp.sum(
            jnp.where(row < 3, cot * color, jnp.where(row == 3, cot, 0.0)), 0, keepdims=True
        )
        d_color = jnp.where(row < 3, cot * share, 0.0)
        d_opacity = d_share * inv
        sig = rad
        later = jnp.zeros((1, 2 * TILE), jnp.float32)
        pieces = [None] * SAMPLES
        for t in reversed(range(SAMPLES)):
            d_w = jnp.sum(d_color * rad[t], 0, keepdims=True) + d_opacity
            d_u = d_w * after[t] - later
            later = later + d_w * weights[t]
            d_logit = d_color * weights[t] * rad[t] * (1.0 - rad[t])
            pieces[t] = jnp.where(
                row < 3, d_logit, jnp.where(row == 3, d_u * SPACING * sig[t], 0.0)
            )
        d_small = by_samples(pieces)
        d_logits[...] = jnp.concatenate([d_small, jnp.zeros_like(d_small)], 0).astype(jnp.bfloat16)

    @pl.when(pairs > 0)
    def _():
        start_pair(0)

    def pair(j, carry):
        for copy in pair_copies(buf, saved_ref, sem, j, False):
            copy.wait()

        @pl.when(j + DEEP - 1 < pairs)
        def _():
            fetch(j + DEEP - 1, carry)

        act = buf.at[lax.rem(j, DEEP)]
        ray = jnp.concatenate([rays_ref[slots[2 * j]], rays_ref[slots[2 * j + 1]]], 1)
        dz3[CHID:, :] = d_logits[...]

        def through(grad, lo_row, hi_row, part):
            value = act[lo_row:hi_row, part].astype(jnp.float32)
            return grad * (1.0 - jnp.exp(-value))

        lanes = lane_parts(PARTS_B)
        d_feature = []
        for part in lanes:
            piece = through(mm(radt[...], dz3[CHID:, part]), R_S, R_END, part)
            dz3[:CHID, part] = piece.astype(jnp.bfloat16)
            d_feature.append(piece)
        d_ray = sum(over_samples(jnp.concatenate(d_feature, 1))).astype(jnp.bfloat16)
        start_pair(jnp.minimum(j + 1, pairs - 1))
        for wt, src, dst, lo, hi in (
            (fdt, dz3, dz2, R_H3, R_S), (t2, dz2, dz1, R_H2, R_H3), (t1, dz1, dz0, R_H1, R_H2)
        ):
            for part in lanes:
                dst[:, part] = through(mm(wt[...], src[:, part]), lo, hi, part).astype(jnp.bfloat16)
            if src is dz3:
                d_app = mm(code_ref[0], d_ray)
                hot, high = hot_lanes(ray[6:7].astype(jnp.int32))
                spread = jnp.concatenate(
                    [jnp.where(high == h, d_app, 0.0).astype(jnp.bfloat16) for h in range(SLOTS)], 0
                )
                g_ray[...] += mm_nt(d_ray, raycode_ref[j])
                g_rad[...] += mm_nt(act[R_S:R_END, :], dz3[CHID:, :])
                d_both = mm_nt(dz3[...], act[R_H3:R_S, :])
                g_ref[G_FEAT:G_TAB, :] += d_both[:CHID]
                g_ref[G_DEN : G_DEN + 16, 128:256] += d_both[CHID:, :128]
                g_ref[G_DEN + 16 : G_DEN + 32, 128:256] += d_both[CHID:, 128:]
                g_ref[G_TAB:G_POS, :] += mm_nt(spread, hot)
            elif src is dz2:
                g_ref[G_T2:G_FEAT, :] += mm_nt(dz2[...], act[R_H2:R_H3, :])
            else:
                g_ref[G_T1:G_T2, :] += mm_nt(dz1[...], act[R_H1:R_H2, :])
        g_pos[...] += mm_nt(dz0[...], act[:PC, :])
        return carry

    lax.fori_loop(0, pairs, pair, jnp.int32(0))

    def pick(a, select):
        return lax.dot_general(
            select.astype(jnp.float32), a, (((1,), (1,)), ((), ())),
            preferred_element_type=jnp.float32, precision=lax.Precision.HIGHEST,
        )

    g_ref[G_POS : G_POS + 63, :] = pick(g_pos[...], pos_select_ref[...])
    g_ref[G_VIEW : G_VIEW + 27, :128] = pick(g_ray[:, :VC], view_select_ref[...])
    g_ref[G_CODE : G_CODE + E, :128] = g_ray[...].T[VC:]
    g_ref[G_RAD:G_DEN, 128:256] = g_rad[...].T


def unpack_kernel(
    g_ref, got_colors_ref,
    colors_ref, pos_ref, trunk_ref, density_ref, feature_ref, view_ref, code_ref, radiance_ref, table_ref,
):
    colors_ref[...] = got_colors_ref[...]
    for n in range(63):
        pos_ref[n] = g_ref[G_POS + n : G_POS + n + 1, :]
    trunk_ref[0, 0] = g_ref[G_T1:G_T2, :]
    trunk_ref[0, 1] = g_ref[G_T2:G_FEAT, :]
    feature_ref[0] = g_ref[G_FEAT:G_TAB, :]
    density_ref[:, :128] = g_ref[G_DEN + 3 : G_DEN + 4, 128:256]
    density_ref[:, 128:] = g_ref[G_DEN + 19 : G_DEN + 20, 128:256]
    for n in range(27):
        view_ref[n] = g_ref[G_VIEW + n : G_VIEW + n + 1, :128]
    code_ref[0] = g_ref[G_CODE : G_CODE + E, :128]
    for n in range(3):
        radiance_ref[n] = g_ref[G_RAD + n : G_RAD + n + 1, 128:256]
    for h in range(SLOTS):
        table_ref[0, :, h * LO : (h + 1) * LO] = g_ref[G_TAB + h * E : G_TAB + (h + 1) * E, :]


VMEM = pl.BlockSpec(memory_space=pltpu.VMEM)
SMEM = pl.BlockSpec(memory_space=pltpu.SMEM)
ANY = pl.BlockSpec(memory_space=pl.ANY)
HBM = pl.BlockSpec(memory_space=pltpu.HBM)


def run_forward(live, center, rays, pos, trunk, density, feature, view, code, radiance, table):
    bf = jnp.bfloat16
    return pl.pallas_call(
        forward_kernel,
        name="forward_tiles",
        out_shape=(
            jax.ShapeDtypeStruct((SLOTS, 4, TILE), jnp.float32),
            jax.ShapeDtypeStruct((SLOTS // 2, R_END, 2 * LANES), bf),
            jax.ShapeDtypeStruct((SLOTS // 2, RC, 2 * TILE), bf),
            jax.ShapeDtypeStruct((SLOTS // 2, 8, 2 * LANES), jnp.float32),
        ),
        in_specs=[SMEM, SMEM] + [VMEM] * 11,
        out_specs=(VMEM, ANY, VMEM, VMEM),
        scratch_shapes=[
            pltpu.VMEM((HID, PC), bf),
            pltpu.VMEM((CHID + 16, HID), bf),
            pltpu.VMEM((CHID, RC), bf),
            pltpu.VMEM((8, CHID), bf),
            pltpu.VMEM((SLOTS * E, LO), bf),
            pltpu.VMEM((DEEP, R_END, 2 * LANES), bf),
            pltpu.SMEM((SLOTS + 1,), jnp.int32),
            pltpu.SemaphoreType.DMA((DEEP, 4)),
        ],
        compiler_params=pltpu.CompilerParams(vmem_limit_bytes=40 * 1024 * 1024),
        cost_estimate=pl.CostEstimate(flops=10**10, bytes_accessed=3 * 10**7, transcendentals=0),
    )(live, center, rays, pos, trunk, density, feature, view, code, radiance, table,
      jnp.asarray(POS_SELECT, bf), jnp.asarray(VIEW_SELECT, bf))


def run_backward(live, center, rays, cot, saved, raycode, small, trunk, density, feature, code, radiance):
    bf = jnp.bfloat16
    return pl.pallas_call(
        backward_kernel,
        name="backward_tiles",
        out_shape=jax.ShapeDtypeStruct((G_ROWS, 256), jnp.float32),
        in_specs=[SMEM, SMEM, VMEM, VMEM, ANY] + [VMEM] * 9,
        out_specs=VMEM,
        scratch_shapes=[
            pltpu.VMEM((HID, HID), bf),
            pltpu.VMEM((HID, HID), bf),
            pltpu.VMEM((HID, CHID + 16), bf),
            pltpu.VMEM((CHID, 16), bf),
            pltpu.VMEM((HID, 2 * LANES), bf),
            pltpu.VMEM((HID, 2 * LANES), bf),
            pltpu.VMEM((HID, 2 * LANES), bf),
            pltpu.VMEM((CHID + 16, 2 * LANES), bf),
            pltpu.VMEM((16, 2 * LANES), bf),
            pltpu.VMEM((HID, PC), jnp.float32),
            pltpu.VMEM((CHID, RC), jnp.float32),
            pltpu.VMEM((CHID, 16), jnp.float32),
            pltpu.VMEM((DEEP, R_END, 2 * LANES), bf),
            pltpu.SMEM((SLOTS + 1,), jnp.int32),
            pltpu.SemaphoreType.DMA((DEEP, 4)),
        ],
        compiler_params=pltpu.CompilerParams(vmem_limit_bytes=40 * 1024 * 1024),
        cost_estimate=pl.CostEstimate(flops=2 * 10**10, bytes_accessed=3 * 10**7, transcendentals=0),
    )(live, center, rays, cot, saved, raycode, small, trunk, density, feature, code, radiance,
      jnp.asarray(POS_SELECT, bf), jnp.asarray(VIEW_SELECT, bf))


def run_unpack(packed, colors):
    f32 = jnp.float32
    shapes = [colors.shape, (63, 1, 256), (1, 2, 256, 256), (1, 256), (1, 128, 256), (27, 1, 128),
              (1, 32, 128), (3, 1, 128), (1, 32, 8192)]
    outs = pl.pallas_call(
        unpack_kernel,
        name="unpack_gradients",
        out_shape=tuple(jax.ShapeDtypeStruct(s, f32) for s in shapes),
        in_specs=[VMEM] * 2,
        out_specs=tuple(VMEM for _ in shapes),
        compiler_params=pltpu.CompilerParams(vmem_limit_bytes=32 * 1024 * 1024),
    )(packed, colors)
    colors, pos, trunk, density, feature, view, code, radiance, table = outs
    return (
        colors, pos.transpose(1, 2, 0), trunk, density, feature, view.transpose(1, 2, 0),
        code.transpose(0, 2, 1), radiance.transpose(1, 0, 2), table,
    )


MESH = pl.DeviceIdType.MESH
GROUP = SLOTS
REPS = 4
CHUNK = G_ROWS // (4 * REPS)


def place():
    return lax.axis_index("blk"), lax.axis_index("rep")


def partner(blk, rep, i):
    return lax.rem(blk + i, GROUP), lax.rem(rep + GROUP * REPS - i, REPS)


def greet(blk, rep):
    barrier = pltpu.get_barrier_semaphore()
    for i in range(1, GROUP):
        pl.semaphore_signal(barrier, inc=1, device_id=partner(blk, rep, i), device_id_type=MESH)


def await_all():
    pl.semaphore_wait(pltpu.get_barrier_semaphore(), GROUP - 1)


def exchange(blk, rep, src, dst, send_sem, recv_sem):
    for i in range(1, GROUP):
        to_blk, to_rep = partner(blk, rep, i)
        pltpu.make_async_remote_copy(
            src_ref=src.at[to_blk], dst_ref=dst.at[blk], send_sem=send_sem,
            recv_sem=recv_sem, device_id=(to_blk, to_rep), device_id_type=MESH,
        ).start()
    dst[blk] = src[blk]
    most = pl.ds(0, GROUP - 1)
    return pltpu.make_async_remote_copy(
        src_ref=src.at[most], dst_ref=dst.at[most], send_sem=send_sem, recv_sem=recv_sem,
        device_id=partner(blk, rep, 1), device_id_type=MESH,
    )


def finish(everything):
    everything.wait_recv()
    everything.wait_send()


def find_tiles(ids_ref, tile_of, live):
    for k in range(GROUP):
        where, count = jnp.int32(0), jnp.int32(0)
        for t in range(ids_ref.shape[1]):
            for n in range(3):
                hit = ids_ref[n, t] == k
                where, count = jnp.where(hit, t, where), jnp.where(hit, 1, count)
        tile_of[k] = where
        if live is not None:
            live[k] = count


def scatter_kernel(
    ids_ref, anchors_ref, directions_ref, codes_ref, out_ref,
    tiles, send, anchors, directions, codes, tile_of, live, send_sem, recv_sem, sem,
):
    blk, rep = place()
    fetches = [
        pltpu.make_async_copy(src, dst, sem.at[n])
        for n, (src, dst) in enumerate(
            ((anchors_ref, anchors), (directions_ref, directions), (codes_ref, codes))
        )
    ]
    for fetch in fetches:
        fetch.start()
    greet(blk, rep)
    find_tiles(ids_ref, tile_of, live)
    for fetch in fetches:
        fetch.wait()
    row = row_iota(8, TILE)
    for t in range(tiles.shape[0]):
        lanes = slice(t * TILE, (t + 1) * TILE)
        tiles[t, 0:3] = anchors[:, lanes]
        tiles[t, 3:6] = directions[:, lanes]
        tiles[t, 6:7] = codes[t : t + 1, :].astype(jnp.float32)
        tiles[t, 7:8] = jnp.zeros((1, TILE), jnp.float32)
    for k in range(GROUP):
        send[k] = jnp.where(row == 7, live[k].astype(jnp.float32), tiles[tile_of[k]])
    await_all()
    finish(exchange(blk, rep, send, out_ref, send_sem, recv_sem))


def blend_kernel(
    ids_ref, part_ref, grad_ref, colors_ref, cot_ref,
    back, cots, send, tile_of, send_sem, recv_sem, send_sem2, recv_sem2,
):
    blk, rep = place()
    greet(blk, rep)
    await_all()
    partials = exchange(blk, rep, part_ref, back, send_sem, recv_sem)
    find_tiles(ids_ref, tile_of, None)
    finish(partials)
    for t in range(cots.shape[0]):
        summed = back[ids_ref[0, t]] + back[ids_ref[1, t]] + back[ids_ref[2, t]]
        lanes = slice(t * TILE, (t + 1) * TILE)
        colors = summed[:3] / summed[3:4]
        colors_ref[:, lanes] = colors
        cot = grad_ref[:, lanes] * LOSS_SCALE / summed[3:4]
        cots[t] = jnp.concatenate([cot, -jnp.sum(cot * colors, 0, keepdims=True)], 0)
    for k in range(GROUP):
        send[k] = cots[tile_of[k]]
    finish(exchange(blk, rep, send, cot_ref, send_sem2, recv_sem2))


def total_kernel(g_ref, out_ref, got, held, send_sem, recv_sem):
    blk, rep = place()
    up, down = lax.rem(rep + 1, REPS), lax.rem(rep + REPS - 1, REPS)
    barrier = pltpu.get_barrier_semaphore()
    for other in (up, down):
        pl.semaphore_signal(barrier, inc=1, device_id=(blk, other), device_id_type=MESH)
    pl.semaphore_wait(barrier, 2)
    rings = range(4)

    def chunk(ring, ahead):
        sign = 1 if ring % 2 == 0 else REPS - 1
        which = lax.rem(rep + sign * (ahead + REPS), REPS)
        return pl.ds(pl.multiple_of((ring * REPS + which) * CHUNK, 8), CHUNK)

    def copy(ring, step):
        if step == 0:
            src, dst = g_ref.at[chunk(ring, 0)], got.at[ring, 0]
        elif step < 3:
            src, dst = held.at[ring, step - 1], got.at[ring, step]
        else:
            rows = chunk(ring, 4 - step)
            src, dst = out_ref.at[rows], out_ref.at[rows]
        return pltpu.make_async_remote_copy(
            src_ref=src, dst_ref=dst, send_sem=send_sem.at[ring, step],
            recv_sem=recv_sem.at[ring, step],
            device_id=(blk, up if ring % 2 == 0 else down), device_id_type=MESH,
        )

    for ring in rings:
        copy(ring, 0).start()
    for step in range(6):
        for ring in rings:
            copy(ring, step).wait_recv()
            if step < 2:
                held[ring, step] = got[ring, step] + g_ref[chunk(ring, -step - 1), :]
            elif step == 2:
                out_ref[chunk(ring, 1), :] = got[ring, 2] + g_ref[chunk(ring, 1), :]
            if step < 5:
                copy(ring, step + 1).start()
    for step in range(6):
        for ring in rings:
            copy(ring, step).wait_send()


def communicate(kernel, name, number, args, specs, shapes, scratch):
    return pl.pallas_call(
        kernel,
        name=name,
        out_shape=shapes,
        in_specs=specs,
        out_specs=jax.tree.map(lambda _: VMEM, shapes),
        scratch_shapes=scratch,
        compiler_params=pltpu.CompilerParams(
            collective_id=number, has_side_effects=True, vmem_limit_bytes=16 * 1024 * 1024
        ),
        cost_estimate=pl.CostEstimate(flops=10**10, bytes_accessed=10**6, transcendentals=0),
    )(*args)


def run_scatter(ids, anchors, directions, codes):
    f32, i32 = jnp.float32, jnp.int32
    return communicate(
        scatter_kernel, "scatter_rays", 0, (ids, anchors, directions, codes), [SMEM, HBM, HBM, HBM],
        jax.ShapeDtypeStruct((GROUP, 8, TILE), f32),
        [pltpu.VMEM((codes.shape[0], 8, TILE), f32), pltpu.VMEM((GROUP, 8, TILE), f32),
         pltpu.VMEM(anchors.shape, f32), pltpu.VMEM(directions.shape, f32),
         pltpu.VMEM(codes.shape, i32), pltpu.SMEM((GROUP,), i32), pltpu.SMEM((GROUP,), i32)]
        + [pltpu.SemaphoreType.DMA] * 2 + [pltpu.SemaphoreType.DMA((3,))],
    )


def run_blend(ids, part, grad):
    tiles = grad.shape[1] // TILE
    small = (GROUP, 4, TILE)
    return communicate(
        blend_kernel, "blend_colors", 1, (ids, part, grad), [SMEM, VMEM, VMEM],
        (jax.ShapeDtypeStruct(grad.shape, jnp.float32), jax.ShapeDtypeStruct(small, jnp.float32)),
        [pltpu.VMEM(small, jnp.float32), pltpu.VMEM((tiles, 4, TILE), jnp.float32),
         pltpu.VMEM(small, jnp.float32), pltpu.SMEM((GROUP,), jnp.int32)]
        + [pltpu.SemaphoreType.DMA] * 4,
    )


def run_total(packed):
    return communicate(
        total_kernel, "total_gradients", 2, (packed,), [VMEM],
        jax.ShapeDtypeStruct((G_ROWS, 256), jnp.float32),
        [pltpu.VMEM((4, 3, CHUNK, 256), jnp.float32), pltpu.VMEM((4, 2, CHUNK, 256), jnp.float32)]
        + [pltpu.SemaphoreType.DMA((4, 6))] * 2,
    )


def local(
    anchors, directions, app_ids, block_ids, color_grad, block_centers, pos_weight, trunk_weight,
    density_weight, feature_weight, view_weight, code_weight, radiance_weight, code_table,
):
    tiles = block_ids.shape[0]
    ids = block_ids.T
    rays = run_scatter(ids, anchors, directions, app_ids.reshape(tiles, TILE))
    live = (rays[:, 7, 0] > 0.5).astype(jnp.int32)
    center = block_centers.T
    code = code_weight.transpose(0, 2, 1)
    part, saved, raycode, small = run_forward(
        live, center, rays, pos_weight.transpose(0, 2, 1), trunk_weight, density_weight, feature_weight,
        view_weight.transpose(0, 2, 1), code, radiance_weight, code_table,
    )
    colors, cot = run_blend(ids, part, color_grad)
    packed = run_backward(
        live, center, rays, cot, saved, raycode, small, trunk_weight, density_weight,
        feature_weight, code, radiance_weight,
    )
    return run_unpack(run_total(packed), colors)


def solution(mesh):
    weights = (P("blk", None, None), P("blk", None, None, None), P("blk", None)) + (
        P("blk", None, None),
    ) * 5
    ray = P(None, ("blk", "rep"))
    return jax.shard_map(
        local,
        mesh=mesh,
        in_specs=(ray, ray, P(("blk", "rep")), P(("blk", "rep"), None), ray, P(None, "blk")) + weights,
        out_specs=(ray,) + weights,
        check_vma=False,
    )
```

```python
import numpy as np

import jax
import jax.numpy as jnp
from jax import lax
from jax.experimental import pallas as pl
from jax.experimental.pallas import tpu as pltpu
from jax.sharding import PartitionSpec as P

TILE = 128
SAMPLES = 4
SLOTS = 32
LANES = SAMPLES * TILE
HID = 256
CHID = 128
PC = 96
VC = 48
E = 32
RC = VC + E
LO = 256
SPACING = 0.5
LOSS_SCALE = 0.03125
DEEP = 3
PARTS_F = 4
PARTS_B = 4

R_H1 = PC
R_H2 = R_H1 + HID
R_H3 = R_H2 + HID
R_S = R_H3 + HID
R_END = R_S + CHID
GATHER_AFTER = R_H2

G_TAB = 0
G_FEAT = 1024
G_VIEW = 1152
G_CODE = 1184
G_RAD = 1152
G_DEN = 1168
A_ROWS = 1280
G_T1 = 1280
G_T2 = 1536
G_POS = 1792
G_ROWS = 1920
PAIRS = SLOTS // 2
LOW = ((0, 208), (208, 416), (416, R_H3))
HIGH = ((R_H3, 736), (736, R_S), (R_S, R_END))
ALL = LOW + HIGH


def code_places(levels, half):
    raw = list(range(3))
    sines, cosines = [], []
    for level in range(levels):
        for c in range(3):
            row = (level // half) * 3 + c
            group = 2 * (level % half)
            sines.append(8 * (1 + group) + row)
            cosines.append(8 * (2 + group) + row)
    return raw + sines + cosines


def selection(places, width):
    out = np.zeros((len(places), width), np.float32)
    out[np.arange(len(places)), places] = 1.0
    return out


POS_SELECT = selection(code_places(10, 5), PC)
VIEW_SELECT = selection(code_places(4, 2), VC)


def mm(a, b):
    return lax.dot_general(a, b, (((1,), (0,)), ((), ())), preferred_element_type=jnp.float32)


def mm_nt(a, b):
    return lax.dot_general(a, b, (((1,), (1,)), ((), ())), preferred_element_type=jnp.float32)


def mm_tn(a, b):
    return lax.dot_general(a, b, (((0,), (0,)), ((), ())), preferred_element_type=jnp.float32)


def softplus(v):
    return jnp.maximum(v, jnp.log(1.0 + jnp.exp(jnp.minimum(v, 80.0))))


def row_iota(rows, lanes):
    return lax.broadcasted_iota(jnp.int32, (rows, lanes), 0)


def ray_rows(ray, row):
    o8 = jnp.where(row < 3, ray, jnp.where(row < 6, pltpu.roll(ray, 3, 0), 0.0))
    d8 = jnp.where(row < 3, pltpu.roll(ray, 5, 0), jnp.where(row < 6, ray, 0.0))
    return o8, d8


def center_rows(center_ref, row):
    third = jnp.where(row >= 3, row - 3, row)
    return jnp.where(
        third == 0,
        center_ref[0, 0],
        jnp.where(third == 1, center_ref[0, 1], jnp.where(third == 2, center_ref[0, 2], 0.0)),
    )


def sine_cosine(x):
    turns = jnp.round(x * 0.6366197723675814)
    r = x - turns * 1.5703125
    r = r - turns * 4.837512969970703e-4
    r = r - turns * 7.549789948768648e-8
    q = turns.astype(jnp.int32)
    z = r * r
    sine = r + r * z * (-1.6666654611e-1 + z * (8.3321608736e-3 - z * 1.9515295891e-4))
    cosine = 1.0 - 0.5 * z + z * z * (
        4.166664568298827e-2 + z * (-1.388731625493765e-3 + z * 2.443315711809948e-5)
    )
    odd = (q & 1) == 1
    first = jnp.where(odd, cosine, sine)
    second = jnp.where(odd, sine, cosine)
    return (
        jnp.where((q & 2) == 2, -first, first),
        jnp.where(((q + 1) & 2) == 2, -second, second),
    )


def code_groups(values, doublings):
    groups = [values]
    sine, cosine = sine_cosine(values)
    for step in range(doublings):
        groups += [sine, cosine]
        if step + 1 < doublings:
            sine, cosine = 2.0 * sine * cosine, (cosine - sine) * (cosine + sine)
    groups.append(jnp.zeros_like(values))
    return jnp.concatenate(groups, 0).astype(jnp.bfloat16)


def halves(x):
    return x[:, :TILE], x[:, TILE:]


def over_samples(x):
    return [
        jnp.concatenate([x[:, s * TILE : (s + 1) * TILE], x[:, LANES + s * TILE : LANES + (s + 1) * TILE]], 1)
        for s in range(SAMPLES)
    ]


def by_samples(pieces):
    return jnp.concatenate([halves(p)[h] for h in range(2) for p in pieces], 1)


def composite(small, o8, c8, row):
    density = over_samples(softplus(small))
    rad = over_samples(1.0 / (1.0 + jnp.exp(-small)))
    off = o8 - c8
    off2 = jnp.sum(jnp.where(row < 3, off * off, 0.0), 0, keepdims=True)
    inv = 1.0 / (1.0 + off2)
    depth = jnp.zeros((1, 2 * TILE), jnp.float32)
    before = jnp.ones((1, 2 * TILE), jnp.float32)
    weights, after = [], []
    for s in range(SAMPLES):
        u = density[s][3:4] * SPACING
        weights.append(before * (1.0 - jnp.exp(-u)))
        depth = depth + u
        before = jnp.exp(-depth)
        after.append(before)
    color = sum(w * r for w, r in zip(weights, rad))
    opacity = sum(weights)
    return rad, weights, after, color, (0.1 + opacity) * inv, inv


def list_live(live_ref, slots):
    total = jnp.int32(0)
    for s in range(SLOTS):
        slots[total] = jnp.int32(s)
        total = total + (live_ref[s] > 0).astype(jnp.int32)

    @pl.when(total % 2 == 1)
    def _():
        slots[total] = slots[total - 1]

    return total, (total + 1) // 2


def pair_copies(buf, saved_ref, sem, j, out, ranges):
    slot = lax.rem(j, DEEP)
    base = ranges[0][0]
    copies = []
    for n, (lo, hi) in enumerate(ranges):
        near, far = buf.at[slot, lo - base : hi - base], saved_ref.at[j, lo:hi]
        src, dst = (near, far) if out else (far, near)
        copies.append(pltpu.make_async_copy(src, dst, sem.at[slot, n]))
    return copies


def hot_lanes(ids):
    lo, hi = ids & (LO - 1), ids >> 8
    return (row_iota(LO, 2 * TILE) == lo).astype(jnp.float32).astype(jnp.bfloat16), hi


def lane_parts(parts):
    width = 2 * LANES // parts
    return [slice(p * width, (p + 1) * width) for p in range(parts)]


def forward_kernel(
    live_ref, center_ref, rays_ref, pos_ref, trunk_ref, density_ref, feature_ref, view_ref,
    code_ref, radiance_ref, table_ref, pos_select_ref, view_select_ref,
    part_ref, saved_ref, raycode_ref, small_ref,
    wp, wfd, wray, wrad, tab, buf, slots, sem, blank_sem,
):
    row = row_iota(8, 2 * TILE)
    c8 = center_rows(center_ref, row)
    wp[...] = mm_tn(pos_select_ref[...], pos_ref[0]).T.astype(jnp.bfloat16)
    wray[...] = jnp.concatenate(
        [mm_tn(view_select_ref[...], view_ref[0]), code_ref[0].astype(jnp.float32)], 0
    ).T.astype(jnp.bfloat16)
    wfd[:CHID, :] = feature_ref[0]
    row16 = row_iota(16, HID)
    wfd[CHID:, :] = jnp.where(row16 == 3, density_ref[...].astype(jnp.float32), 0.0).astype(jnp.bfloat16)
    wrad[...] = jnp.concatenate(
        [radiance_ref[0].astype(jnp.float32), jnp.zeros((5, CHID), jnp.float32)], 0
    ).astype(jnp.bfloat16)
    for h in range(SLOTS):
        tab[h * E : (h + 1) * E, :] = table_ref[0, :, h * LO : (h + 1) * LO]
    pos_scale = jnp.where(row < 3, 1.0, 32.0)
    view_scale = jnp.where(row < 3, 1.0, 4.0)
    total, pairs = list_live(live_ref, slots)

    def finish_pair(j):
        s0, s1 = slots[2 * j], slots[2 * j + 1]
        o8, _ = ray_rows(jnp.concatenate([rays_ref[s0], rays_ref[s1]], 1), row)
        _, _, _, color, share, _ = composite(small_ref[j], o8, c8, row)
        first, second = halves(jnp.where(row < 3, color * share, share)[:4])
        part_ref[s0] = first
        part_ref[s1] = second

    def pair(j, carry):
        @pl.when(j >= DEEP)
        def _():
            for copy in pair_copies(buf, saved_ref, sem, j - DEEP, True, ALL):
                copy.wait()

        out = buf.at[lax.rem(j, DEEP)]
        s0, s1 = slots[2 * j], slots[2 * j + 1]
        ray = jnp.concatenate([rays_ref[s0], rays_ref[s1]], 1)
        o8, d8 = ray_rows(ray, row)
        points = by_samples(
            [(o8 + (t + 0.5) * SPACING * d8 - c8) * pos_scale for t in range(SAMPLES)]
        )
        out[:PC, :] = code_groups(points, 5)
        finish_pair(jnp.maximum(j - 1, 0))
        lanes = lane_parts(PARTS_F)
        for w, lo, mid, hi_row in (
            (wp, 0, R_H1, R_H2), (trunk_ref.at[0, 0], R_H1, R_H2, R_H3), (trunk_ref.at[0, 1], R_H2, R_H3, R_S)
        ):
            for part in lanes:
                out[mid:hi_row, part] = softplus(mm(w[...], out[lo:mid, part])).astype(jnp.bfloat16)
            if mid == GATHER_AFTER:
                hot, hi = hot_lanes(ray[6:7].astype(jnp.int32))
                rows = mm(tab[...], hot)
                picks = [rows[h * E : (h + 1) * E] for h in range(SLOTS)]
                for bit in range(5):
                    on = ((hi >> bit) & 1) == 1
                    picks = [jnp.where(on, b, a) for a, b in zip(picks[::2], picks[1::2])]
                app = picks[0]
                raycode = jnp.concatenate([code_groups(d8 * view_scale, 2), app.astype(jnp.bfloat16)], 0)
                raycode_ref[j] = raycode
                per_ray = mm(wray[...], raycode)
        ray_lanes = by_samples([per_ray] * SAMPLES)
        small = []
        for part in lanes:
            both = mm(wfd[...], out[R_H3:R_S, part])
            shaded = softplus(both[:CHID] + ray_lanes[:, part]).astype(jnp.bfloat16)
            out[R_S:R_END, part] = shaded
            logits = mm(wrad[...], shaded)
            small.append(jnp.where(row_iota(8, logits.shape[1]) == 3, both[CHID : CHID + 8], logits))
        small = jnp.concatenate(small, 1)
        small_ref[j] = small
        for copy in pair_copies(buf, saved_ref, sem, j, True, ALL):
            copy.start()
        return carry

    small_ref[0] = jnp.zeros_like(small_ref[0])
    lax.fori_loop(0, pairs, pair, jnp.int32(0))

    @pl.when(pairs > 0)
    def _():
        finish_pair(pairs - 1)

    def drain(j, carry):
        for copy in pair_copies(buf, saved_ref, sem, j, True, ALL):
            copy.wait()
        return carry

    lax.fori_loop(jnp.maximum(pairs - DEEP, 0), pairs, drain, jnp.int32(0))
    buf[0, :R_H3, :] = jnp.zeros((R_H3, 2 * LANES), jnp.bfloat16)

    def blank(j):
        return pltpu.make_async_copy(buf.at[0, :R_H3], saved_ref.at[j, :R_H3], blank_sem.at[j])

    def begin_blank(j, carry):
        blank(j).start()
        return carry

    def end_blank(j, carry):
        blank(j).wait()
        return carry

    lax.fori_loop(pairs, PAIRS, begin_blank, jnp.int32(0))
    lax.fori_loop(pairs, PAIRS, end_blank, jnp.int32(0))


def flip(x):
    return x.astype(jnp.float32).T.astype(jnp.bfloat16)


def pick(a, select):
    return lax.dot_general(
        select.astype(jnp.float32), a, (((1,), (1,)), ((), ())),
        preferred_element_type=jnp.float32, precision=lax.Precision.HIGHEST,
    )


def backward_kernel(
    live_ref, center_ref, rays_ref, cot_ref, saved_ref, raycode_ref, small_ref,
    density_ref, feature_ref, code_ref, radiance_ref, view_select_ref,
    g_ref, dz_ref,
    fdt, radt, dz3, d_logits, g_ray, g_rad, buf, slots, sem,
):
    total, pairs = list_live(live_ref, slots)

    def fetch(j, carry):
        for copy in pair_copies(buf, saved_ref, sem, j, False, HIGH):
            copy.start()
        return carry

    lax.fori_loop(0, jnp.minimum(pairs, DEEP - 1), fetch, jnp.int32(0))
    row = row_iota(8, 2 * TILE)
    lane = lax.broadcasted_iota(jnp.int32, (1, 2 * TILE), 1)
    c8 = center_rows(center_ref, row)

    fdt[:, :CHID] = flip(feature_ref[0])
    row16 = row_iota(16, HID)
    fdt[:, CHID:] = jnp.where(row16 == 3, density_ref[...].astype(jnp.float32), 0.0).T.astype(jnp.bfloat16)
    radt[...] = jnp.concatenate(
        [radiance_ref[0].astype(jnp.float32), jnp.zeros((13, CHID), jnp.float32)], 0
    ).T.astype(jnp.bfloat16)
    g_ref[...] = jnp.zeros_like(g_ref)

    def blank(j, carry):
        dz_ref[j] = jnp.zeros((HID, 2 * LANES), jnp.bfloat16)
        return carry

    lax.fori_loop(pairs, PAIRS, blank, jnp.int32(0))
    g_ray[...] = jnp.zeros_like(g_ray)
    g_rad[...] = jnp.zeros_like(g_rad)

    def start_pair(j):
        s0, s1 = slots[2 * j], slots[2 * j + 1]
        ray = jnp.concatenate([rays_ref[s0], rays_ref[s1]], 1)
        o8, _ = ray_rows(ray, row)
        small = small_ref[j]
        rad, weights, after, color, share, inv = composite(small, o8, c8, row)
        cot = jnp.concatenate([cot_ref[s0], cot_ref[s1]], 1)
        cot = jnp.where((lane < TILE) | (2 * j + 1 < total), cot, 0.0)
        cot = jnp.concatenate([cot, jnp.zeros_like(cot)], 0)
        d_share = jnp.sum(
            jnp.where(row < 3, cot * color, jnp.where(row == 3, cot, 0.0)), 0, keepdims=True
        )
        d_color = jnp.where(row < 3, cot * share, 0.0)
        d_opacity = d_share * inv
        sig = rad
        later = jnp.zeros((1, 2 * TILE), jnp.float32)
        pieces = [None] * SAMPLES
        for t in reversed(range(SAMPLES)):
            d_w = jnp.sum(d_color * rad[t], 0, keepdims=True) + d_opacity
            d_u = d_w * after[t] - later
            later = later + d_w * weights[t]
            d_logit = d_color * weights[t] * rad[t] * (1.0 - rad[t])
            pieces[t] = jnp.where(
                row < 3, d_logit, jnp.where(row == 3, d_u * SPACING * sig[t], 0.0)
            )
        d_small = by_samples(pieces)
        d_logits[...] = jnp.concatenate([d_small, jnp.zeros_like(d_small)], 0).astype(jnp.bfloat16)

    @pl.when(pairs > 0)
    def _():
        start_pair(0)

    def pair(j, carry):
        for copy in pair_copies(buf, saved_ref, sem, j, False, HIGH):
            copy.wait()

        @pl.when(j + DEEP - 1 < pairs)
        def _():
            fetch(j + DEEP - 1, carry)

        act = buf.at[lax.rem(j, DEEP)]
        ray = jnp.concatenate([rays_ref[slots[2 * j]], rays_ref[slots[2 * j + 1]]], 1)
        dz3[CHID:, :] = d_logits[...]

        def through(grad, lo_row, hi_row, part):
            value = act[lo_row - R_H3 : hi_row - R_H3, part].astype(jnp.float32)
            return grad * (1.0 - jnp.exp(-value))

        lanes = lane_parts(PARTS_B)
        d_feature = []
        for part in lanes:
            piece = through(mm(radt[...], dz3[CHID:, part]), R_S, R_END, part)
            dz3[:CHID, part] = piece.astype(jnp.bfloat16)
            d_feature.append(piece)
        d_ray = sum(over_samples(jnp.concatenate(d_feature, 1))).astype(jnp.bfloat16)
        start_pair(jnp.minimum(j + 1, pairs - 1))
        for part in lanes:
            dz_ref[j, :, part] = through(mm(fdt[...], dz3[:, part]), R_H3, R_S, part).astype(jnp.bfloat16)
        d_app = mm(code_ref[0], d_ray)
        hot, high = hot_lanes(ray[6:7].astype(jnp.int32))
        spread = jnp.concatenate(
            [jnp.where(high == h, d_app, 0.0).astype(jnp.bfloat16) for h in range(SLOTS)], 0
        )
        g_ray[...] += mm_nt(d_ray, raycode_ref[j])
        g_rad[...] += mm_nt(act[HID:, :], dz3[CHID:, :])
        d_both = mm_nt(dz3[...], act[:HID, :])
        g_ref[G_FEAT:G_VIEW, :] += d_both[:CHID]
        g_ref[G_DEN : G_DEN + 16, 128:256] += d_both[CHID:, :128]
        g_ref[G_DEN + 16 : G_DEN + 32, 128:256] += d_both[CHID:, 128:]
        g_ref[G_TAB:G_FEAT, :] += mm_nt(spread, hot)
        return carry

    lax.fori_loop(0, pairs, pair, jnp.int32(0))
    g_ref[G_VIEW : G_VIEW + 27, :128] = pick(g_ray[:, :VC], view_select_ref[...])
    g_ref[G_CODE : G_CODE + E, :128] = g_ray[...].T[VC:]
    g_ref[G_RAD:G_DEN, 128:256] = g_rad[...].T


def unpack_kernel(
    g_ref, got_colors_ref,
    colors_ref, pos_ref, trunk_ref, density_ref, feature_ref, view_ref, code_ref, radiance_ref, table_ref,
):
    colors_ref[...] = got_colors_ref[...]
    for n in range(63):
        pos_ref[n] = g_ref[G_POS + n : G_POS + n + 1, :]
    trunk_ref[0, 0] = g_ref[G_T1:G_T2, :]
    trunk_ref[0, 1] = g_ref[G_T2:G_POS, :]
    feature_ref[0] = g_ref[G_FEAT:G_VIEW, :]
    density_ref[:, :128] = g_ref[G_DEN + 3 : G_DEN + 4, 128:256]
    density_ref[:, 128:] = g_ref[G_DEN + 19 : G_DEN + 20, 128:256]
    for n in range(27):
        view_ref[n] = g_ref[G_VIEW + n : G_VIEW + n + 1, :128]
    code_ref[0] = g_ref[G_CODE : G_CODE + E, :128]
    for n in range(3):
        radiance_ref[n] = g_ref[G_RAD + n : G_RAD + n + 1, 128:256]
    for h in range(SLOTS):
        table_ref[0, :, h * LO : (h + 1) * LO] = g_ref[G_TAB + h * E : G_TAB + (h + 1) * E, :]


VMEM = pl.BlockSpec(memory_space=pltpu.VMEM)
SMEM = pl.BlockSpec(memory_space=pltpu.SMEM)
ANY = pl.BlockSpec(memory_space=pl.ANY)
HBM = pl.BlockSpec(memory_space=pltpu.HBM)


def run_forward(live, center, rays, pos, trunk, density, feature, view, code, radiance, table):
    bf = jnp.bfloat16
    return pl.pallas_call(
        forward_kernel,
        name="forward_tiles",
        out_shape=(
            jax.ShapeDtypeStruct((SLOTS, 4, TILE), jnp.float32),
            jax.ShapeDtypeStruct((SLOTS // 2, R_END, 2 * LANES), bf),
            jax.ShapeDtypeStruct((SLOTS // 2, RC, 2 * TILE), bf),
            jax.ShapeDtypeStruct((SLOTS // 2, 8, 2 * LANES), jnp.float32),
        ),
        in_specs=[SMEM, SMEM] + [VMEM] * 11,
        out_specs=(VMEM, ANY, VMEM, VMEM),
        scratch_shapes=[
            pltpu.VMEM((HID, PC), bf),
            pltpu.VMEM((CHID + 16, HID), bf),
            pltpu.VMEM((CHID, RC), bf),
            pltpu.VMEM((8, CHID), bf),
            pltpu.VMEM((SLOTS * E, LO), bf),
            pltpu.VMEM((DEEP, R_END, 2 * LANES), bf),
            pltpu.SMEM((SLOTS + 1,), jnp.int32),
            pltpu.SemaphoreType.DMA((DEEP, len(ALL))),
            pltpu.SemaphoreType.DMA((PAIRS,)),
        ],
        compiler_params=pltpu.CompilerParams(vmem_limit_bytes=32 * 1024 * 1024),
        cost_estimate=pl.CostEstimate(flops=10**10, bytes_accessed=3 * 10**7, transcendentals=0),
    )(live, center, rays, pos, trunk, density, feature, view, code, radiance, table,
      jnp.asarray(POS_SELECT, bf), jnp.asarray(VIEW_SELECT, bf))


def run_backward(live, center, rays, cot, saved, raycode, small, density, feature, code, radiance):
    bf = jnp.bfloat16
    return pl.pallas_call(
        backward_kernel,
        name="backward_tiles",
        out_shape=(
            jax.ShapeDtypeStruct((A_ROWS, 256), jnp.float32),
            jax.ShapeDtypeStruct((PAIRS, HID, 2 * LANES), bf),
        ),
        in_specs=[SMEM, SMEM, VMEM, VMEM, ANY] + [VMEM] * 7,
        out_specs=(VMEM, VMEM),
        scratch_shapes=[
            pltpu.VMEM((HID, CHID + 16), bf),
            pltpu.VMEM((CHID, 16), bf),
            pltpu.VMEM((CHID + 16, 2 * LANES), bf),
            pltpu.VMEM((16, 2 * LANES), bf),
            pltpu.VMEM((CHID, RC), jnp.float32),
            pltpu.VMEM((CHID, 16), jnp.float32),
            pltpu.VMEM((DEEP, R_END - R_H3, 2 * LANES), bf),
            pltpu.SMEM((SLOTS + 1,), jnp.int32),
            pltpu.SemaphoreType.DMA((DEEP, len(HIGH))),
        ],
        compiler_params=pltpu.CompilerParams(vmem_limit_bytes=32 * 1024 * 1024),
        cost_estimate=pl.CostEstimate(flops=10**10, bytes_accessed=10**7, transcendentals=0),
    )(live, center, rays, cot, saved, raycode, small, density, feature, code, radiance,
      jnp.asarray(VIEW_SELECT, bf))


def run_unpack(packed, colors):
    f32 = jnp.float32
    shapes = [colors.shape, (63, 1, 256), (1, 2, 256, 256), (1, 256), (1, 128, 256), (27, 1, 128),
              (1, 32, 128), (3, 1, 128), (1, 32, 8192)]
    outs = pl.pallas_call(
        unpack_kernel,
        name="unpack_gradients",
        out_shape=tuple(jax.ShapeDtypeStruct(s, f32) for s in shapes),
        in_specs=[VMEM] * 2,
        out_specs=tuple(VMEM for _ in shapes),
        compiler_params=pltpu.CompilerParams(vmem_limit_bytes=32 * 1024 * 1024),
    )(packed, colors)
    colors, pos, trunk, density, feature, view, code, radiance, table = outs
    return (
        colors, pos.transpose(1, 2, 0), trunk, density, feature, view.transpose(1, 2, 0),
        code.transpose(0, 2, 1), radiance.transpose(1, 0, 2), table,
    )


MESH = pl.DeviceIdType.MESH
GROUP = SLOTS
REPS = 4


def place():
    return lax.axis_index("blk"), lax.axis_index("rep")


def partner(blk, rep, i):
    return lax.rem(blk + i, GROUP), lax.rem(rep + GROUP * REPS - i, REPS)


def greet(blk, rep):
    barrier = pltpu.get_barrier_semaphore()
    for i in range(1, GROUP):
        pl.semaphore_signal(barrier, inc=1, device_id=partner(blk, rep, i), device_id_type=MESH)


def await_all():
    pl.semaphore_wait(pltpu.get_barrier_semaphore(), GROUP - 1)


def exchange(blk, rep, src, dst, send_sem, recv_sem):
    for i in range(1, GROUP):
        to_blk, to_rep = partner(blk, rep, i)
        pltpu.make_async_remote_copy(
            src_ref=src.at[to_blk], dst_ref=dst.at[blk], send_sem=send_sem,
            recv_sem=recv_sem, device_id=(to_blk, to_rep), device_id_type=MESH,
        ).start()
    dst[blk] = src[blk]
    most = pl.ds(0, GROUP - 1)
    return pltpu.make_async_remote_copy(
        src_ref=src.at[most], dst_ref=dst.at[most], send_sem=send_sem, recv_sem=recv_sem,
        device_id=partner(blk, rep, 1), device_id_type=MESH,
    )


def finish(everything):
    everything.wait_recv()
    everything.wait_send()


def find_tiles(ids_ref, tile_of, live):
    for k in range(GROUP):
        where, count = jnp.int32(0), jnp.int32(0)
        for t in range(ids_ref.shape[1]):
            for n in range(3):
                hit = ids_ref[n, t] == k
                where, count = jnp.where(hit, t, where), jnp.where(hit, 1, count)
        tile_of[k] = where
        if live is not None:
            live[k] = count


def scatter_kernel(
    ids_ref, anchors_ref, directions_ref, codes_ref, out_ref,
    tiles, send, anchors, directions, codes, tile_of, live, send_sem, recv_sem, sem,
):
    blk, rep = place()
    fetches = [
        pltpu.make_async_copy(src, dst, sem.at[n])
        for n, (src, dst) in enumerate(
            ((anchors_ref, anchors), (directions_ref, directions), (codes_ref, codes))
        )
    ]
    for fetch in fetches:
        fetch.start()
    greet(blk, rep)
    find_tiles(ids_ref, tile_of, live)
    for fetch in fetches:
        fetch.wait()
    row = row_iota(8, TILE)
    for t in range(tiles.shape[0]):
        lanes = slice(t * TILE, (t + 1) * TILE)
        tiles[t, 0:3] = anchors[:, lanes]
        tiles[t, 3:6] = directions[:, lanes]
        tiles[t, 6:7] = codes[t : t + 1, :].astype(jnp.float32)
        tiles[t, 7:8] = jnp.zeros((1, TILE), jnp.float32)
    for k in range(GROUP):
        send[k] = jnp.where(row == 7, live[k].astype(jnp.float32), tiles[tile_of[k]])
    await_all()
    finish(exchange(blk, rep, send, out_ref, send_sem, recv_sem))


def blend_kernel(
    ids_ref, part_ref, grad_ref, colors_ref, cot_ref,
    back, cots, send, tile_of, send_sem, recv_sem, send_sem2, recv_sem2,
):
    blk, rep = place()
    greet(blk, rep)
    await_all()
    partials = exchange(blk, rep, part_ref, back, send_sem, recv_sem)
    find_tiles(ids_ref, tile_of, None)
    finish(partials)
    for t in range(cots.shape[0]):
        summed = back[ids_ref[0, t]] + back[ids_ref[1, t]] + back[ids_ref[2, t]]
        lanes = slice(t * TILE, (t + 1) * TILE)
        colors = summed[:3] / summed[3:4]
        colors_ref[:, lanes] = colors
        cot = grad_ref[:, lanes] * LOSS_SCALE / summed[3:4]
        cots[t] = jnp.concatenate([cot, -jnp.sum(cot * colors, 0, keepdims=True)], 0)
    for k in range(GROUP):
        send[k] = cots[tile_of[k]]
    finish(exchange(blk, rep, send, cot_ref, send_sem2, recv_sem2))


class Rings:
    def __init__(self, blk, rep, g, out, base, got, held, send_sem, recv_sem):
        self.blk, self.rep, self.g, self.out, self.base = blk, rep, g, out, base
        self.got, self.held, self.send_sem, self.recv_sem = got, held, send_sem, recv_sem
        self.rows = g.shape[0] // (4 * REPS)

    def chunk(self, ring, ahead, base):
        sign = 1 + (REPS - 2) * lax.rem(ring, 2)
        which = lax.rem(self.rep + sign * (ahead + REPS), REPS)
        return pl.ds(pl.multiple_of(base + (ring * REPS + which) * self.rows, 8), self.rows)

    def copy(self, ring, step):
        if step == 0:
            src, dst = self.g.at[self.chunk(ring, 0, 0)], self.got.at[ring, 0]
        elif step < 3:
            src, dst = self.held.at[ring, step - 1], self.got.at[ring, step]
        else:
            rows = self.chunk(ring, 4 - step, self.base)
            src, dst = self.out.at[rows], self.out.at[rows]
        to = lax.rem(self.rep + 1 + (REPS - 2) * lax.rem(ring, 2), REPS)
        return pltpu.make_async_remote_copy(
            src_ref=src, dst_ref=dst, send_sem=self.send_sem.at[ring, step],
            recv_sem=self.recv_sem.at[ring, step], device_id=(self.blk, to), device_id_type=MESH,
        )

    def each(self, action):
        def body(ring, carry):
            action(ring)
            return carry

        lax.fori_loop(0, 4, body, 0)

    def begin(self):
        self.each(lambda ring: self.copy(ring, 0).start())

    def advance(self, ring, step):
        self.copy(ring, step).wait_recv()
        if step < 2:
            mine = self.g[self.chunk(ring, -step - 1, 0), :]
            self.held[ring, step] = self.got[ring, step] + mine
        elif step == 2:
            mine = self.g[self.chunk(ring, 1, 0), :]
            self.out[self.chunk(ring, 1, self.base), :] = self.got[ring, 2] + mine
        if step < 5:
            self.copy(ring, step + 1).start()

    def drain(self):
        for step in range(6):
            self.each(lambda ring: self.copy(ring, step).wait_send())


def trunk_kernel(
    ga_ref, dz_ref, trunk_ref, pos_select_ref, saved_ref, out_ref,
    t1, t2, dz0, dz1, gb, g_pos, buf, sem, got_a, held_a, got_b, held_b, send_a, recv_a, send_b, recv_b,
):
    blk, rep = place()
    barrier = pltpu.get_barrier_semaphore()
    for other in (lax.rem(rep + 1, REPS), lax.rem(rep + REPS - 1, REPS)):
        pl.semaphore_signal(barrier, inc=1, device_id=(blk, other), device_id_type=MESH)
    for first in range(DEEP - 1):
        for copy in pair_copies(buf, saved_ref, sem, jnp.int32(first), False, LOW):
            copy.start()
    t1[...] = flip(trunk_ref[0, 0])
    t2[...] = flip(trunk_ref[0, 1])
    gb[...] = jnp.zeros_like(gb)
    g_pos[...] = jnp.zeros_like(g_pos)
    pl.semaphore_wait(barrier, 2)
    color = Rings(blk, rep, ga_ref, out_ref, 0, got_a, held_a, send_a, recv_a)
    trunk = Rings(blk, rep, gb, out_ref, A_ROWS, got_b, held_b, send_b, recv_b)
    color.begin()
    lanes = lane_parts(PARTS_B)

    def pair(j):
        for copy in pair_copies(buf, saved_ref, sem, j, False, LOW):
            copy.wait()

        @pl.when(j + DEEP - 1 < PAIRS)
        def _():
            for copy in pair_copies(buf, saved_ref, sem, j + DEEP - 1, False, LOW):
                copy.start()

        act = buf.at[lax.rem(j, DEEP)]
        dz2 = dz_ref.at[j]
        for wt, src, dst, lo, hi in ((t2, dz2, dz1, R_H2, R_H3), (t1, dz1, dz0, R_H1, R_H2)):
            for part in lanes:
                value = act[lo:hi, part].astype(jnp.float32)
                grad = mm(wt[...], src[:, part]) * (1.0 - jnp.exp(-value))
                dst[:, part] = grad.astype(jnp.bfloat16)
            if src is dz2:
                gb[HID : 2 * HID, :] += mm_nt(dz2[...], act[R_H2:R_H3, :])
        gb[:HID, :] += mm_nt(dz1[...], act[R_H1:R_H2, :])
        g_pos[...] += mm_nt(dz0[...], act[:PC, :])

    for step in range(4):

        def both(ring, carry):
            pair(4 * step + ring)
            color.advance(ring, step)
            return carry

        lax.fori_loop(0, 4, both, 0)
    gb[2 * HID : 2 * HID + 63, :] = pick(g_pos[...], pos_select_ref[...])
    trunk.begin()
    for step in (4, 5):
        color.each(lambda ring: color.advance(ring, step))
    for step in range(6):
        trunk.each(lambda ring: trunk.advance(ring, step))
    color.drain()
    trunk.drain()


def communicate(kernel, name, number, args, specs, shapes, scratch):
    return pl.pallas_call(
        kernel,
        name=name,
        out_shape=shapes,
        in_specs=specs,
        out_specs=jax.tree.map(lambda _: VMEM, shapes),
        scratch_shapes=scratch,
        compiler_params=pltpu.CompilerParams(
            collective_id=number, has_side_effects=True, vmem_limit_bytes=(32 if number == 2 else 16) * 1024 * 1024
        ),
        cost_estimate=pl.CostEstimate(flops=10**10, bytes_accessed=10**6, transcendentals=0),
    )(*args)


def run_scatter(ids, anchors, directions, codes):
    f32, i32 = jnp.float32, jnp.int32
    return communicate(
        scatter_kernel, "scatter_rays", 0, (ids, anchors, directions, codes), [SMEM, HBM, HBM, HBM],
        jax.ShapeDtypeStruct((GROUP, 8, TILE), f32),
        [pltpu.VMEM((codes.shape[0], 8, TILE), f32), pltpu.VMEM((GROUP, 8, TILE), f32),
         pltpu.VMEM(anchors.shape, f32), pltpu.VMEM(directions.shape, f32),
         pltpu.VMEM(codes.shape, i32), pltpu.SMEM((GROUP,), i32), pltpu.SMEM((GROUP,), i32)]
        + [pltpu.SemaphoreType.DMA] * 2 + [pltpu.SemaphoreType.DMA((3,))],
    )


def run_blend(ids, part, grad):
    tiles = grad.shape[1] // TILE
    small = (GROUP, 4, TILE)
    return communicate(
        blend_kernel, "blend_colors", 1, (ids, part, grad), [SMEM, VMEM, VMEM],
        (jax.ShapeDtypeStruct(grad.shape, jnp.float32), jax.ShapeDtypeStruct(small, jnp.float32)),
        [pltpu.VMEM(small, jnp.float32), pltpu.VMEM((tiles, 4, TILE), jnp.float32),
         pltpu.VMEM(small, jnp.float32), pltpu.SMEM((GROUP,), jnp.int32)]
        + [pltpu.SemaphoreType.DMA] * 4,
    )


def run_trunk(color_grads, dz, trunk, saved):
    f32, bf = jnp.float32, jnp.bfloat16
    rows_a, rows_b = A_ROWS // 16, (G_ROWS - A_ROWS) // 16
    return communicate(
        trunk_kernel, "trunk_and_total", 2,
        (color_grads, dz, trunk, jnp.asarray(POS_SELECT, bf), saved), [VMEM, VMEM, VMEM, VMEM, ANY],
        jax.ShapeDtypeStruct((G_ROWS, 256), f32),
        [pltpu.VMEM((HID, HID), bf), pltpu.VMEM((HID, HID), bf), pltpu.VMEM((HID, 2 * LANES), bf),
         pltpu.VMEM((HID, 2 * LANES), bf), pltpu.VMEM((G_ROWS - A_ROWS, 256), f32),
         pltpu.VMEM((HID, PC), f32), pltpu.VMEM((DEEP, R_H3, 2 * LANES), bf),
         pltpu.SemaphoreType.DMA((DEEP, len(LOW))),
         pltpu.VMEM((4, 3, rows_a, 256), f32), pltpu.VMEM((4, 2, rows_a, 256), f32),
         pltpu.VMEM((4, 3, rows_b, 256), f32), pltpu.VMEM((4, 2, rows_b, 256), f32)]
        + [pltpu.SemaphoreType.DMA((4, 6))] * 4,
    )


def local(
    anchors, directions, app_ids, block_ids, color_grad, block_centers, pos_weight, trunk_weight,
    density_weight, feature_weight, view_weight, code_weight, radiance_weight, code_table,
):
    tiles = block_ids.shape[0]
    ids = block_ids.T
    rays = run_scatter(ids, anchors, directions, app_ids.reshape(tiles, TILE))
    live = (rays[:, 7, 0] > 0.5).astype(jnp.int32)
    center = block_centers.T
    code = code_weight.transpose(0, 2, 1)
    part, saved, raycode, small = run_forward(
        live, center, rays, pos_weight.transpose(0, 2, 1), trunk_weight, density_weight, feature_weight,
        view_weight.transpose(0, 2, 1), code, radiance_weight, code_table,
    )
    colors, cot = run_blend(ids, part, color_grad)
    color_grads, dz = run_backward(
        live, center, rays, cot, saved, raycode, small, density_weight, feature_weight, code,
        radiance_weight,
    )
    return run_unpack(run_trunk(color_grads, dz, trunk_weight, saved), colors)


def solution(mesh):
    weights = (P("blk", None, None), P("blk", None, None, None), P("blk", None)) + (
        P("blk", None, None),
    ) * 5
    ray = P(None, ("blk", "rep"))
    return jax.shard_map(
        local,
        mesh=mesh,
        in_specs=(ray, ray, P(("blk", "rep")), P(("blk", "rep"), None), ray, P(None, "blk")) + weights,
        out_specs=(ray,) + weights,
        check_vma=False,
    )
```

```python
import numpy as np

import jax
import jax.numpy as jnp
from jax import lax
from jax.experimental import pallas as pl
from jax.experimental.pallas import tpu as pltpu
from jax.sharding import PartitionSpec as P

TILE = 128
SAMPLES = 4
SLOTS = 32
LANES = SAMPLES * TILE
HID = 256
CHID = 128
PC = 96
VC = 48
E = 32
RC = VC + E
LO = 256
SPACING = 0.5
LOSS_SCALE = 0.03125
DEEP = 3
PARTS_F = 4
PARTS_B = 4

R_H1 = PC
R_H2 = R_H1 + HID
R_H3 = R_H2 + HID
R_S = R_H3 + HID
R_END = R_S + CHID
GATHER_AFTER = R_H2

G_TAB = 0
G_FEAT = 1024
G_VIEW = 1152
G_CODE = 1184
G_RAD = 1152
G_DEN = 1168
A_ROWS = 1280
G_T1 = 1280
G_T2 = 1536
G_POS = 1792
G_ROWS = 1920
PAIRS = SLOTS // 2
LOW = ((0, 208), (208, 416), (416, R_H3))
HIGH = ((R_H3, 736), (736, R_S), (R_S, R_END))
ALL = LOW + HIGH


def code_places(levels, half):
    raw = list(range(3))
    sines, cosines = [], []
    for level in range(levels):
        for c in range(3):
            row = (level // half) * 3 + c
            group = 2 * (level % half)
            sines.append(8 * (1 + group) + row)
            cosines.append(8 * (2 + group) + row)
    return raw + sines + cosines


def selection(places, width):
    out = np.zeros((len(places), width), np.float32)
    out[np.arange(len(places)), places] = 1.0
    return out


POS_SELECT = selection(code_places(10, 5), PC)
VIEW_SELECT = selection(code_places(4, 2), VC)


def mm(a, b):
    return lax.dot_general(a, b, (((1,), (0,)), ((), ())), preferred_element_type=jnp.float32)


def mm_nt(a, b):
    return lax.dot_general(a, b, (((1,), (1,)), ((), ())), preferred_element_type=jnp.float32)


def mm_tn(a, b):
    return lax.dot_general(a, b, (((0,), (0,)), ((), ())), preferred_element_type=jnp.float32)


def softplus(v):
    return jnp.maximum(v, jnp.log(1.0 + jnp.exp(jnp.minimum(v, 80.0))))


def row_iota(rows, lanes):
    return lax.broadcasted_iota(jnp.int32, (rows, lanes), 0)


def ray_rows(ray, row):
    o8 = jnp.where(row < 3, ray, jnp.where(row < 6, pltpu.roll(ray, 3, 0), 0.0))
    d8 = jnp.where(row < 3, pltpu.roll(ray, 5, 0), jnp.where(row < 6, ray, 0.0))
    return o8, d8


def center_rows(center_ref, row):
    third = jnp.where(row >= 3, row - 3, row)
    return jnp.where(
        third == 0,
        center_ref[0, 0],
        jnp.where(third == 1, center_ref[0, 1], jnp.where(third == 2, center_ref[0, 2], 0.0)),
    )


def sine_cosine(x):
    turns = jnp.round(x * 0.6366197723675814)
    r = x - turns * 1.5703125
    r = r - turns * 4.837512969970703e-4
    r = r - turns * 7.549789948768648e-8
    q = turns.astype(jnp.int32)
    z = r * r
    sine = r + r * z * (-1.6666654611e-1 + z * (8.3321608736e-3 - z * 1.9515295891e-4))
    cosine = 1.0 - 0.5 * z + z * z * (
        4.166664568298827e-2 + z * (-1.388731625493765e-3 + z * 2.443315711809948e-5)
    )
    odd = (q & 1) == 1
    first = jnp.where(odd, cosine, sine)
    second = jnp.where(odd, sine, cosine)
    return (
        jnp.where((q & 2) == 2, -first, first),
        jnp.where(((q + 1) & 2) == 2, -second, second),
    )


def code_groups(values, doublings):
    groups = [values]
    sine, cosine = sine_cosine(values)
    for step in range(doublings):
        groups += [sine, cosine]
        if step + 1 < doublings:
            sine, cosine = 2.0 * sine * cosine, (cosine - sine) * (cosine + sine)
    groups.append(jnp.zeros_like(values))
    return jnp.concatenate(groups, 0).astype(jnp.bfloat16)


def halves(x):
    return x[:, :TILE], x[:, TILE:]


def over_samples(x):
    return [
        jnp.concatenate([x[:, s * TILE : (s + 1) * TILE], x[:, LANES + s * TILE : LANES + (s + 1) * TILE]], 1)
        for s in range(SAMPLES)
    ]


def by_samples(pieces):
    return jnp.concatenate([halves(p)[h] for h in range(2) for p in pieces], 1)


def composite(small, o8, c8, row):
    density = over_samples(softplus(small))
    rad = over_samples(1.0 / (1.0 + jnp.exp(-small)))
    off = o8 - c8
    off2 = jnp.sum(jnp.where(row < 3, off * off, 0.0), 0, keepdims=True)
    inv = 1.0 / (1.0 + off2)
    depth = jnp.zeros((1, 2 * TILE), jnp.float32)
    before = jnp.ones((1, 2 * TILE), jnp.float32)
    weights, after = [], []
    for s in range(SAMPLES):
        u = density[s][3:4] * SPACING
        weights.append(before * (1.0 - jnp.exp(-u)))
        depth = depth + u
        before = jnp.exp(-depth)
        after.append(before)
    color = sum(w * r for w, r in zip(weights, rad))
    opacity = sum(weights)
    return rad, weights, after, color, (0.1 + opacity) * inv, inv


def list_live(live_ref, slots):
    total = jnp.int32(0)
    for s in range(SLOTS):
        slots[total] = jnp.int32(s)
        total = total + (live_ref[s] > 0).astype(jnp.int32)

    @pl.when(total % 2 == 1)
    def _():
        slots[total] = slots[total - 1]

    return total, (total + 1) // 2


def pair_copies(buf, saved_ref, sem, j, out, ranges):
    slot = lax.rem(j, DEEP)
    base = ranges[0][0]
    copies = []
    for n, (lo, hi) in enumerate(ranges):
        near, far = buf.at[slot, lo - base : hi - base], saved_ref.at[j, lo:hi]
        src, dst = (near, far) if out else (far, near)
        copies.append(pltpu.make_async_copy(src, dst, sem.at[slot, n]))
    return copies


def hot_lanes(ids):
    lo, hi = ids & (LO - 1), ids >> 8
    return (row_iota(LO, 2 * TILE) == lo).astype(jnp.float32).astype(jnp.bfloat16), hi


def lane_parts(parts):
    width = 2 * LANES // parts
    return [slice(p * width, (p + 1) * width) for p in range(parts)]


def forward_kernel(
    live_ref, center_ref, rays_ref, pos_ref, trunk_ref, density_ref, feature_ref, view_ref,
    code_ref, radiance_ref, table_ref, pos_select_ref, view_select_ref,
    part_ref, saved_ref, raycode_ref, small_ref,
    wp, wfd, wray, wrad, tab, buf, zeros, slots, sem, blank_sem,
):
    row = row_iota(8, 2 * TILE)
    c8 = center_rows(center_ref, row)
    wp[...] = mm_tn(pos_select_ref[...], pos_ref[0]).T.astype(jnp.bfloat16)
    wray[...] = jnp.concatenate(
        [mm_tn(view_select_ref[...], view_ref[0]), code_ref[0].astype(jnp.float32)], 0
    ).T.astype(jnp.bfloat16)
    wfd[:CHID, :] = feature_ref[0]
    row16 = row_iota(16, HID)
    wfd[CHID:, :] = jnp.where(row16 == 3, density_ref[...].astype(jnp.float32), 0.0).astype(jnp.bfloat16)
    wrad[...] = jnp.concatenate(
        [radiance_ref[0].astype(jnp.float32), jnp.zeros((5, CHID), jnp.float32)], 0
    ).astype(jnp.bfloat16)
    for h in range(SLOTS):
        tab[h * E : (h + 1) * E, :] = table_ref[0, :, h * LO : (h + 1) * LO]
    pos_scale = jnp.where(row < 3, 1.0, 32.0)
    view_scale = jnp.where(row < 3, 1.0, 4.0)
    total, pairs = list_live(live_ref, slots)
    zeros[...] = jnp.zeros_like(zeros)

    def blank(j):
        return pltpu.make_async_copy(zeros, saved_ref.at[j, :R_H3], blank_sem.at[j])

    def begin_blank(j, carry):
        blank(j).start()
        return carry

    lax.fori_loop(pairs, PAIRS, begin_blank, jnp.int32(0))

    def finish_pair(j):
        s0, s1 = slots[2 * j], slots[2 * j + 1]
        o8, _ = ray_rows(jnp.concatenate([rays_ref[s0], rays_ref[s1]], 1), row)
        _, _, _, color, share, _ = composite(small_ref[j], o8, c8, row)
        first, second = halves(jnp.where(row < 3, color * share, share)[:4])
        part_ref[s0] = first
        part_ref[s1] = second

    def pair(j, carry):
        @pl.when(j >= DEEP)
        def _():
            for copy in pair_copies(buf, saved_ref, sem, j - DEEP, True, ALL):
                copy.wait()

        out = buf.at[lax.rem(j, DEEP)]
        s0, s1 = slots[2 * j], slots[2 * j + 1]
        ray = jnp.concatenate([rays_ref[s0], rays_ref[s1]], 1)
        o8, d8 = ray_rows(ray, row)
        points = by_samples(
            [(o8 + (t + 0.5) * SPACING * d8 - c8) * pos_scale for t in range(SAMPLES)]
        )
        out[:PC, :] = code_groups(points, 5)
        finish_pair(jnp.maximum(j - 1, 0))
        lanes = lane_parts(PARTS_F)
        for w, lo, mid, hi_row in (
            (wp, 0, R_H1, R_H2), (trunk_ref.at[0, 0], R_H1, R_H2, R_H3), (trunk_ref.at[0, 1], R_H2, R_H3, R_S)
        ):
            for part in lanes:
                out[mid:hi_row, part] = softplus(mm(w[...], out[lo:mid, part])).astype(jnp.bfloat16)
            if mid == GATHER_AFTER:
                hot, hi = hot_lanes(ray[6:7].astype(jnp.int32))
                rows = mm(tab[...], hot)
                picks = [rows[h * E : (h + 1) * E] for h in range(SLOTS)]
                for bit in range(5):
                    on = ((hi >> bit) & 1) == 1
                    picks = [jnp.where(on, b, a) for a, b in zip(picks[::2], picks[1::2])]
                app = picks[0]
                raycode = jnp.concatenate([code_groups(d8 * view_scale, 2), app.astype(jnp.bfloat16)], 0)
                raycode_ref[j] = raycode
                per_ray = mm(wray[...], raycode)
        ray_lanes = by_samples([per_ray] * SAMPLES)
        small = []
        for part in lanes:
            both = mm(wfd[...], out[R_H3:R_S, part])
            shaded = softplus(both[:CHID] + ray_lanes[:, part]).astype(jnp.bfloat16)
            out[R_S:R_END, part] = shaded
            logits = mm(wrad[...], shaded)
            small.append(jnp.where(row_iota(8, logits.shape[1]) == 3, both[CHID : CHID + 8], logits))
        small = jnp.concatenate(small, 1)
        small_ref[j] = small
        for copy in pair_copies(buf, saved_ref, sem, j, True, ALL):
            copy.start()
        return carry

    small_ref[0] = jnp.zeros_like(small_ref[0])
    lax.fori_loop(0, pairs, pair, jnp.int32(0))

    @pl.when(pairs > 0)
    def _():
        finish_pair(pairs - 1)

    def drain(j, carry):
        for copy in pair_copies(buf, saved_ref, sem, j, True, ALL):
            copy.wait()
        return carry

    lax.fori_loop(jnp.maximum(pairs - DEEP, 0), pairs, drain, jnp.int32(0))

    def end_blank(j, carry):
        blank(j).wait()
        return carry

    lax.fori_loop(pairs, PAIRS, end_blank, jnp.int32(0))


def flip(x):
    return x.astype(jnp.float32).T.astype(jnp.bfloat16)


def pick(a, select):
    return lax.dot_general(
        select.astype(jnp.float32), a, (((1,), (1,)), ((), ())),
        preferred_element_type=jnp.float32, precision=lax.Precision.HIGHEST,
    )


def backward_kernel(
    live_ref, center_ref, rays_ref, cot_ref, saved_ref, raycode_ref, small_ref,
    density_ref, feature_ref, code_ref, radiance_ref, view_select_ref,
    g_ref, dz_ref,
    fdt, radt, dz3, d_logits, g_ray, g_rad, buf, slots, sem,
):
    total, pairs = list_live(live_ref, slots)

    def fetch(j, carry):
        for copy in pair_copies(buf, saved_ref, sem, j, False, HIGH):
            copy.start()
        return carry

    lax.fori_loop(0, jnp.minimum(pairs, DEEP - 1), fetch, jnp.int32(0))
    row = row_iota(8, 2 * TILE)
    lane = lax.broadcasted_iota(jnp.int32, (1, 2 * TILE), 1)
    c8 = center_rows(center_ref, row)

    fdt[:, :CHID] = flip(feature_ref[0])
    row16 = row_iota(16, HID)
    fdt[:, CHID:] = jnp.where(row16 == 3, density_ref[...].astype(jnp.float32), 0.0).T.astype(jnp.bfloat16)
    radt[...] = jnp.concatenate(
        [radiance_ref[0].astype(jnp.float32), jnp.zeros((13, CHID), jnp.float32)], 0
    ).T.astype(jnp.bfloat16)
    g_ref[...] = jnp.zeros_like(g_ref)

    def blank(j, carry):
        dz_ref[j] = jnp.zeros((HID, 2 * LANES), jnp.bfloat16)
        return carry

    lax.fori_loop(pairs, PAIRS, blank, jnp.int32(0))
    g_ray[...] = jnp.zeros_like(g_ray)
    g_rad[...] = jnp.zeros_like(g_rad)

    def start_pair(j):
        s0, s1 = slots[2 * j], slots[2 * j + 1]
        ray = jnp.concatenate([rays_ref[s0], rays_ref[s1]], 1)
        o8, _ = ray_rows(ray, row)
        small = small_ref[j]
        rad, weights, after, color, share, inv = composite(small, o8, c8, row)
        cot = jnp.concatenate([cot_ref[s0], cot_ref[s1]], 1)
        cot = jnp.where((lane < TILE) | (2 * j + 1 < total), cot, 0.0)
        cot = jnp.concatenate([cot, jnp.zeros_like(cot)], 0)
        d_share = jnp.sum(
            jnp.where(row < 3, cot * color, jnp.where(row == 3, cot, 0.0)), 0, keepdims=True
        )
        d_color = jnp.where(row < 3, cot * share, 0.0)
        d_opacity = d_share * inv
        sig = rad
        later = jnp.zeros((1, 2 * TILE), jnp.float32)
        pieces = [None] * SAMPLES
        for t in reversed(range(SAMPLES)):
            d_w = jnp.sum(d_color * rad[t], 0, keepdims=True) + d_opacity
            d_u = d_w * after[t] - later
            later = later + d_w * weights[t]
            d_logit = d_color * weights[t] * rad[t] * (1.0 - rad[t])
            pieces[t] = jnp.where(
                row < 3, d_logit, jnp.where(row == 3, d_u * SPACING * sig[t], 0.0)
            )
        d_small = by_samples(pieces)
        d_logits[...] = jnp.concatenate([d_small, jnp.zeros_like(d_small)], 0).astype(jnp.bfloat16)

    @pl.when(pairs > 0)
    def _():
        start_pair(0)

    def pair(j, carry):
        for copy in pair_copies(buf, saved_ref, sem, j, False, HIGH):
            copy.wait()

        @pl.when(j + DEEP - 1 < pairs)
        def _():
            fetch(j + DEEP - 1, carry)

        act = buf.at[lax.rem(j, DEEP)]
        ray = jnp.concatenate([rays_ref[slots[2 * j]], rays_ref[slots[2 * j + 1]]], 1)
        dz3[CHID:, :] = d_logits[...]

        def through(grad, lo_row, hi_row, part):
            value = act[lo_row - R_H3 : hi_row - R_H3, part].astype(jnp.float32)
            return grad * (1.0 - jnp.exp(-value))

        lanes = lane_parts(PARTS_B)
        d_feature = []
        for part in lanes:
            piece = through(mm(radt[...], dz3[CHID:, part]), R_S, R_END, part)
            dz3[:CHID, part] = piece.astype(jnp.bfloat16)
            d_feature.append(piece)
        d_ray = sum(over_samples(jnp.concatenate(d_feature, 1))).astype(jnp.bfloat16)
        start_pair(jnp.minimum(j + 1, pairs - 1))
        for part in lanes:
            dz_ref[j, :, part] = through(mm(fdt[...], dz3[:, part]), R_H3, R_S, part).astype(jnp.bfloat16)
        d_app = mm(code_ref[0], d_ray)
        hot, high = hot_lanes(ray[6:7].astype(jnp.int32))
        spread = jnp.concatenate(
            [jnp.where(high == h, d_app, 0.0).astype(jnp.bfloat16) for h in range(SLOTS)], 0
        )
        g_ray[...] += mm_nt(d_ray, raycode_ref[j])
        g_rad[...] += mm_nt(act[HID:, :], dz3[CHID:, :])
        d_both = mm_nt(dz3[...], act[:HID, :])
        g_ref[G_FEAT:G_VIEW, :] += d_both[:CHID]
        g_ref[G_DEN : G_DEN + 16, 128:256] += d_both[CHID:, :128]
        g_ref[G_DEN + 16 : G_DEN + 32, 128:256] += d_both[CHID:, 128:]
        g_ref[G_TAB:G_FEAT, :] += mm_nt(spread, hot)
        return carry

    lax.fori_loop(0, pairs, pair, jnp.int32(0))
    g_ref[G_VIEW : G_VIEW + 27, :128] = pick(g_ray[:, :VC], view_select_ref[...])
    g_ref[G_CODE : G_CODE + E, :128] = g_ray[...].T[VC:]
    g_ref[G_RAD:G_DEN, 128:256] = g_rad[...].T


def unpack_kernel(
    g_ref, got_colors_ref,
    colors_ref, pos_ref, trunk_ref, density_ref, feature_ref, view_ref, code_ref, radiance_ref, table_ref,
):
    colors_ref[...] = got_colors_ref[...]
    for n in range(63):
        pos_ref[n] = g_ref[G_POS + n : G_POS + n + 1, :]
    trunk_ref[0, 0] = g_ref[G_T1:G_T2, :]
    trunk_ref[0, 1] = g_ref[G_T2:G_POS, :]
    feature_ref[0] = g_ref[G_FEAT:G_VIEW, :]
    density_ref[:, :128] = g_ref[G_DEN + 3 : G_DEN + 4, 128:256]
    density_ref[:, 128:] = g_ref[G_DEN + 19 : G_DEN + 20, 128:256]
    for n in range(27):
        view_ref[n] = g_ref[G_VIEW + n : G_VIEW + n + 1, :128]
    code_ref[0] = g_ref[G_CODE : G_CODE + E, :128]
    for n in range(3):
        radiance_ref[n] = g_ref[G_RAD + n : G_RAD + n + 1, 128:256]
    for h in range(SLOTS):
        table_ref[0, :, h * LO : (h + 1) * LO] = g_ref[G_TAB + h * E : G_TAB + (h + 1) * E, :]


VMEM = pl.BlockSpec(memory_space=pltpu.VMEM)
SMEM = pl.BlockSpec(memory_space=pltpu.SMEM)
ANY = pl.BlockSpec(memory_space=pl.ANY)
HBM = pl.BlockSpec(memory_space=pltpu.HBM)


def run_forward(live, center, rays, pos, trunk, density, feature, view, code, radiance, table):
    bf = jnp.bfloat16
    return pl.pallas_call(
        forward_kernel,
        name="forward_tiles",
        out_shape=(
            jax.ShapeDtypeStruct((SLOTS, 4, TILE), jnp.float32),
            jax.ShapeDtypeStruct((SLOTS // 2, R_END, 2 * LANES), bf),
            jax.ShapeDtypeStruct((SLOTS // 2, RC, 2 * TILE), bf),
            jax.ShapeDtypeStruct((SLOTS // 2, 8, 2 * LANES), jnp.float32),
        ),
        in_specs=[SMEM, SMEM] + [VMEM] * 11,
        out_specs=(VMEM, ANY, VMEM, VMEM),
        scratch_shapes=[
            pltpu.VMEM((HID, PC), bf),
            pltpu.VMEM((CHID + 16, HID), bf),
            pltpu.VMEM((CHID, RC), bf),
            pltpu.VMEM((8, CHID), bf),
            pltpu.VMEM((SLOTS * E, LO), bf),
            pltpu.VMEM((DEEP, R_END, 2 * LANES), bf),
            pltpu.VMEM((R_H3, 2 * LANES), bf),
            pltpu.SMEM((SLOTS + 1,), jnp.int32),
            pltpu.SemaphoreType.DMA((DEEP, len(ALL))),
            pltpu.SemaphoreType.DMA((PAIRS,)),
        ],
        compiler_params=pltpu.CompilerParams(vmem_limit_bytes=32 * 1024 * 1024),
        cost_estimate=pl.CostEstimate(flops=10**10, bytes_accessed=3 * 10**7, transcendentals=0),
    )(live, center, rays, pos, trunk, density, feature, view, code, radiance, table,
      jnp.asarray(POS_SELECT, bf), jnp.asarray(VIEW_SELECT, bf))


def run_backward(live, center, rays, cot, saved, raycode, small, density, feature, code, radiance):
    bf = jnp.bfloat16
    return pl.pallas_call(
        backward_kernel,
        name="backward_tiles",
        out_shape=(
            jax.ShapeDtypeStruct((A_ROWS, 256), jnp.float32),
            jax.ShapeDtypeStruct((PAIRS, HID, 2 * LANES), bf),
        ),
        in_specs=[SMEM, SMEM, VMEM, VMEM, ANY] + [VMEM] * 7,
        out_specs=(VMEM, VMEM),
        scratch_shapes=[
            pltpu.VMEM((HID, CHID + 16), bf),
            pltpu.VMEM((CHID, 16), bf),
            pltpu.VMEM((CHID + 16, 2 * LANES), bf),
            pltpu.VMEM((16, 2 * LANES), bf),
            pltpu.VMEM((CHID, RC), jnp.float32),
            pltpu.VMEM((CHID, 16), jnp.float32),
            pltpu.VMEM((DEEP, R_END - R_H3, 2 * LANES), bf),
            pltpu.SMEM((SLOTS + 1,), jnp.int32),
            pltpu.SemaphoreType.DMA((DEEP, len(HIGH))),
        ],
        compiler_params=pltpu.CompilerParams(vmem_limit_bytes=32 * 1024 * 1024),
        cost_estimate=pl.CostEstimate(flops=10**10, bytes_accessed=10**7, transcendentals=0),
    )(live, center, rays, cot, saved, raycode, small, density, feature, code, radiance,
      jnp.asarray(VIEW_SELECT, bf))


def run_unpack(packed, colors):
    f32 = jnp.float32
    shapes = [colors.shape, (63, 1, 256), (1, 2, 256, 256), (1, 256), (1, 128, 256), (27, 1, 128),
              (1, 32, 128), (3, 1, 128), (1, 32, 8192)]
    outs = pl.pallas_call(
        unpack_kernel,
        name="unpack_gradients",
        out_shape=tuple(jax.ShapeDtypeStruct(s, f32) for s in shapes),
        in_specs=[VMEM] * 2,
        out_specs=tuple(VMEM for _ in shapes),
        compiler_params=pltpu.CompilerParams(vmem_limit_bytes=32 * 1024 * 1024),
    )(packed, colors)
    colors, pos, trunk, density, feature, view, code, radiance, table = outs
    return (
        colors, pos.transpose(1, 2, 0), trunk, density, feature, view.transpose(1, 2, 0),
        code.transpose(0, 2, 1), radiance.transpose(1, 0, 2), table,
    )


MESH = pl.DeviceIdType.MESH
GROUP = SLOTS
REPS = 4


def place():
    return lax.axis_index("blk"), lax.axis_index("rep")


def partner(blk, rep, i):
    return lax.rem(blk + i, GROUP), lax.rem(rep + GROUP * REPS - i, REPS)


def greet(blk, rep):
    barrier = pltpu.get_barrier_semaphore()
    for i in range(1, GROUP):
        pl.semaphore_signal(barrier, inc=1, device_id=partner(blk, rep, i), device_id_type=MESH)


def await_all():
    pl.semaphore_wait(pltpu.get_barrier_semaphore(), GROUP - 1)


def exchange(blk, rep, src, dst, send_sem, recv_sem):
    for i in range(1, GROUP):
        to_blk, to_rep = partner(blk, rep, i)
        pltpu.make_async_remote_copy(
            src_ref=src.at[to_blk], dst_ref=dst.at[blk], send_sem=send_sem,
            recv_sem=recv_sem, device_id=(to_blk, to_rep), device_id_type=MESH,
        ).start()
    dst[blk] = src[blk]
    most = pl.ds(0, GROUP - 1)
    return pltpu.make_async_remote_copy(
        src_ref=src.at[most], dst_ref=dst.at[most], send_sem=send_sem, recv_sem=recv_sem,
        device_id=partner(blk, rep, 1), device_id_type=MESH,
    )


def finish(everything):
    everything.wait_recv()
    everything.wait_send()


def find_tiles(ids_ref, tile_of, live):
    for k in range(GROUP):
        where, count = jnp.int32(0), jnp.int32(0)
        for t in range(ids_ref.shape[1]):
            for n in range(3):
                hit = ids_ref[n, t] == k
                where, count = jnp.where(hit, t, where), jnp.where(hit, 1, count)
        tile_of[k] = where
        if live is not None:
            live[k] = count


def scatter_kernel(
    ids_ref, anchors_ref, directions_ref, codes_ref, out_ref,
    tiles, send, anchors, directions, codes, tile_of, live, send_sem, recv_sem, sem,
):
    blk, rep = place()
    fetches = [
        pltpu.make_async_copy(src, dst, sem.at[n])
        for n, (src, dst) in enumerate(
            ((anchors_ref, anchors), (directions_ref, directions), (codes_ref, codes))
        )
    ]
    for fetch in fetches:
        fetch.start()
    greet(blk, rep)
    find_tiles(ids_ref, tile_of, live)
    for fetch in fetches:
        fetch.wait()
    row = row_iota(8, TILE)
    for t in range(tiles.shape[0]):
        lanes = slice(t * TILE, (t + 1) * TILE)
        tiles[t, 0:3] = anchors[:, lanes]
        tiles[t, 3:6] = directions[:, lanes]
        tiles[t, 6:7] = codes[t : t + 1, :].astype(jnp.float32)
        tiles[t, 7:8] = jnp.zeros((1, TILE), jnp.float32)
    for k in range(GROUP):
        send[k] = jnp.where(row == 7, live[k].astype(jnp.float32), tiles[tile_of[k]])
    await_all()
    finish(exchange(blk, rep, send, out_ref, send_sem, recv_sem))


def blend_kernel(
    ids_ref, part_ref, grad_ref, colors_ref, cot_ref,
    back, cots, send, tile_of, send_sem, recv_sem, send_sem2, recv_sem2,
):
    blk, rep = place()
    greet(blk, rep)
    await_all()
    partials = exchange(blk, rep, part_ref, back, send_sem, recv_sem)
    find_tiles(ids_ref, tile_of, None)
    finish(partials)
    for t in range(cots.shape[0]):
        summed = back[ids_ref[0, t]] + back[ids_ref[1, t]] + back[ids_ref[2, t]]
        lanes = slice(t * TILE, (t + 1) * TILE)
        colors = summed[:3] / summed[3:4]
        colors_ref[:, lanes] = colors
        cot = grad_ref[:, lanes] * LOSS_SCALE / summed[3:4]
        cots[t] = jnp.concatenate([cot, -jnp.sum(cot * colors, 0, keepdims=True)], 0)
    for k in range(GROUP):
        send[k] = cots[tile_of[k]]
    finish(exchange(blk, rep, send, cot_ref, send_sem2, recv_sem2))


class Rings:
    def __init__(self, blk, rep, g, out, base, got, held, send_sem, recv_sem):
        self.blk, self.rep, self.g, self.out, self.base = blk, rep, g, out, base
        self.got, self.held, self.send_sem, self.recv_sem = got, held, send_sem, recv_sem
        self.rows = g.shape[0] // (4 * REPS)

    def chunk(self, ring, ahead, base):
        sign = 1 + (REPS - 2) * lax.rem(ring, 2)
        which = lax.rem(self.rep + sign * (ahead + REPS), REPS)
        return pl.ds(pl.multiple_of(base + (ring * REPS + which) * self.rows, 8), self.rows)

    def copy(self, ring, step):
        if step == 0:
            src, dst = self.g.at[self.chunk(ring, 0, 0)], self.got.at[ring, 0]
        elif step < 3:
            src, dst = self.held.at[ring, step - 1], self.got.at[ring, step]
        else:
            rows = self.chunk(ring, 4 - step, self.base)
            src, dst = self.out.at[rows], self.out.at[rows]
        to = lax.rem(self.rep + 1 + (REPS - 2) * lax.rem(ring, 2), REPS)
        return pltpu.make_async_remote_copy(
            src_ref=src, dst_ref=dst, send_sem=self.send_sem.at[ring, step],
            recv_sem=self.recv_sem.at[ring, step], device_id=(self.blk, to), device_id_type=MESH,
        )

    def each(self, action):
        def body(ring, carry):
            action(ring)
            return carry

        lax.fori_loop(0, 4, body, 0)

    def begin(self):
        self.each(lambda ring: self.copy(ring, 0).start())

    def advance(self, ring, step):
        self.copy(ring, step).wait_recv()
        if step < 2:
            mine = self.g[self.chunk(ring, -step - 1, 0), :]
            self.held[ring, step] = self.got[ring, step] + mine
        elif step == 2:
            mine = self.g[self.chunk(ring, 1, 0), :]
            self.out[self.chunk(ring, 1, self.base), :] = self.got[ring, 2] + mine
        if step < 5:
            self.copy(ring, step + 1).start()

    def drain(self):
        for step in range(6):
            self.each(lambda ring: self.copy(ring, step).wait_send())


def trunk_kernel(
    ga_ref, dz_ref, trunk_ref, pos_select_ref, saved_ref, out_ref,
    t1, t2, dz0, dz1, gb, g_pos, buf, sem, got_a, held_a, got_b, held_b, send_a, recv_a, send_b, recv_b,
):
    blk, rep = place()
    barrier = pltpu.get_barrier_semaphore()
    for other in (lax.rem(rep + 1, REPS), lax.rem(rep + REPS - 1, REPS)):
        pl.semaphore_signal(barrier, inc=1, device_id=(blk, other), device_id_type=MESH)
    for first in range(DEEP - 1):
        for copy in pair_copies(buf, saved_ref, sem, jnp.int32(first), False, LOW):
            copy.start()
    t1[...] = flip(trunk_ref[0, 0])
    t2[...] = flip(trunk_ref[0, 1])
    gb[...] = jnp.zeros_like(gb)
    g_pos[...] = jnp.zeros_like(g_pos)
    pl.semaphore_wait(barrier, 2)
    color = Rings(blk, rep, ga_ref, out_ref, 0, got_a, held_a, send_a, recv_a)
    trunk = Rings(blk, rep, gb, out_ref, A_ROWS, got_b, held_b, send_b, recv_b)
    color.begin()
    lanes = lane_parts(PARTS_B)

    def pair(j):
        for copy in pair_copies(buf, saved_ref, sem, j, False, LOW):
            copy.wait()

        @pl.when(j + DEEP - 1 < PAIRS)
        def _():
            for copy in pair_copies(buf, saved_ref, sem, j + DEEP - 1, False, LOW):
                copy.start()

        act = buf.at[lax.rem(j, DEEP)]
        dz2 = dz_ref.at[j]
        for wt, src, dst, lo, hi in ((t2, dz2, dz1, R_H2, R_H3), (t1, dz1, dz0, R_H1, R_H2)):
            for part in lanes:
                value = act[lo:hi, part].astype(jnp.float32)
                grad = mm(wt[...], src[:, part]) * (1.0 - jnp.exp(-value))
                dst[:, part] = grad.astype(jnp.bfloat16)
            if src is dz2:
                gb[HID : 2 * HID, :] += mm_nt(dz2[...], act[R_H2:R_H3, :])
        gb[:HID, :] += mm_nt(dz1[...], act[R_H1:R_H2, :])
        g_pos[...] += mm_nt(dz0[...], act[:PC, :])

    for step in range(4):

        def both(ring, carry):
            pair(4 * step + ring)
            color.advance(ring, step)
            return carry

        lax.fori_loop(0, 4, both, 0)
    gb[2 * HID : 2 * HID + 63, :] = pick(g_pos[...], pos_select_ref[...])
    trunk.begin()
    for step in range(6):
        if step < 2:
            color.each(lambda ring: color.advance(ring, 4 + step))
        trunk.each(lambda ring: trunk.advance(ring, step))
    color.drain()
    trunk.drain()


def communicate(kernel, name, number, args, specs, shapes, scratch):
    return pl.pallas_call(
        kernel,
        name=name,
        out_shape=shapes,
        in_specs=specs,
        out_specs=jax.tree.map(lambda _: VMEM, shapes),
        scratch_shapes=scratch,
        compiler_params=pltpu.CompilerParams(
            collective_id=number, has_side_effects=True, vmem_limit_bytes=(32 if number == 2 else 16) * 1024 * 1024
        ),
        cost_estimate=pl.CostEstimate(flops=10**10, bytes_accessed=10**6, transcendentals=0),
    )(*args)


def run_scatter(ids, anchors, directions, codes):
    f32, i32 = jnp.float32, jnp.int32
    return communicate(
        scatter_kernel, "scatter_rays", 0, (ids, anchors, directions, codes), [SMEM, HBM, HBM, HBM],
        jax.ShapeDtypeStruct((GROUP, 8, TILE), f32),
        [pltpu.VMEM((codes.shape[0], 8, TILE), f32), pltpu.VMEM((GROUP, 8, TILE), f32),
         pltpu.VMEM(anchors.shape, f32), pltpu.VMEM(directions.shape, f32),
         pltpu.VMEM(codes.shape, i32), pltpu.SMEM((GROUP,), i32), pltpu.SMEM((GROUP,), i32)]
        + [pltpu.SemaphoreType.DMA] * 2 + [pltpu.SemaphoreType.DMA((3,))],
    )


def run_blend(ids, part, grad):
    tiles = grad.shape[1] // TILE
    small = (GROUP, 4, TILE)
    return communicate(
        blend_kernel, "blend_colors", 1, (ids, part, grad), [SMEM, VMEM, VMEM],
        (jax.ShapeDtypeStruct(grad.shape, jnp.float32), jax.ShapeDtypeStruct(small, jnp.float32)),
        [pltpu.VMEM(small, jnp.float32), pltpu.VMEM((tiles, 4, TILE), jnp.float32),
         pltpu.VMEM(small, jnp.float32), pltpu.SMEM((GROUP,), jnp.int32)]
        + [pltpu.SemaphoreType.DMA] * 4,
    )


def run_trunk(color_grads, dz, trunk, saved):
    f32, bf = jnp.float32, jnp.bfloat16
    rows_a, rows_b = A_ROWS // 16, (G_ROWS - A_ROWS) // 16
    return communicate(
        trunk_kernel, "trunk_and_total", 2,
        (color_grads, dz, trunk, jnp.asarray(POS_SELECT, bf), saved), [VMEM, VMEM, VMEM, VMEM, ANY],
        jax.ShapeDtypeStruct((G_ROWS, 256), f32),
        [pltpu.VMEM((HID, HID), bf), pltpu.VMEM((HID, HID), bf), pltpu.VMEM((HID, 2 * LANES), bf),
         pltpu.VMEM((HID, 2 * LANES), bf), pltpu.VMEM((G_ROWS - A_ROWS, 256), f32),
         pltpu.VMEM((HID, PC), f32), pltpu.VMEM((DEEP, R_H3, 2 * LANES), bf),
         pltpu.SemaphoreType.DMA((DEEP, len(LOW))),
         pltpu.VMEM((4, 3, rows_a, 256), f32), pltpu.VMEM((4, 2, rows_a, 256), f32),
         pltpu.VMEM((4, 3, rows_b, 256), f32), pltpu.VMEM((4, 2, rows_b, 256), f32)]
        + [pltpu.SemaphoreType.DMA((4, 6))] * 4,
    )


def local(
    anchors, directions, app_ids, block_ids, color_grad, block_centers, pos_weight, trunk_weight,
    density_weight, feature_weight, view_weight, code_weight, radiance_weight, code_table,
):
    tiles = block_ids.shape[0]
    ids = block_ids.T
    rays = run_scatter(ids, anchors, directions, app_ids.reshape(tiles, TILE))
    live = (rays[:, 7, 0] > 0.5).astype(jnp.int32)
    center = block_centers.T
    code = code_weight.transpose(0, 2, 1)
    part, saved, raycode, small = run_forward(
        live, center, rays, pos_weight.transpose(0, 2, 1), trunk_weight, density_weight, feature_weight,
        view_weight.transpose(0, 2, 1), code, radiance_weight, code_table,
    )
    colors, cot = run_blend(ids, part, color_grad)
    color_grads, dz = run_backward(
        live, center, rays, cot, saved, raycode, small, density_weight, feature_weight, code,
        radiance_weight,
    )
    return run_unpack(run_trunk(color_grads, dz, trunk_weight, saved), colors)


def solution(mesh):
    weights = (P("blk", None, None), P("blk", None, None, None), P("blk", None)) + (
        P("blk", None, None),
    ) * 5
    ray = P(None, ("blk", "rep"))
    return jax.shard_map(
        local,
        mesh=mesh,
        in_specs=(ray, ray, P(("blk", "rep")), P(("blk", "rep"), None), ray, P(None, "blk")) + weights,
        out_specs=(ray,) + weights,
        check_vma=False,
    )
```

```python
import numpy as np

import jax
import jax.numpy as jnp
from jax import lax
from jax.experimental import pallas as pl
from jax.experimental.pallas import tpu as pltpu
from jax.sharding import PartitionSpec as P

TILE = 128
SAMPLES = 4
SLOTS = 32
LANES = SAMPLES * TILE
HID = 256
CHID = 128
PC = 96
VC = 48
E = 32
RC = VC + E
LO = 256
SPACING = 0.5
LOSS_SCALE = 0.03125
DEEP = 3
PARTS_F = 4
PARTS_B = 4

R_H1 = PC
R_H2 = R_H1 + HID
R_H3 = R_H2 + HID
R_S = R_H3 + HID
R_END = R_S + CHID
GATHER_AFTER = R_H2

G_T1 = 0
G_T2 = 256
G_FEAT = 512
G_TAB = 640
G_POS = 1664
G_VIEW = 1728
G_CODE = 1760
G_RAD = 1728
G_DEN = 1744
G_ROWS = 1792


def code_places(levels, half):
    raw = list(range(3))
    sines, cosines = [], []
    for level in range(levels):
        for c in range(3):
            row = (level // half) * 3 + c
            group = 2 * (level % half)
            sines.append(8 * (1 + group) + row)
            cosines.append(8 * (2 + group) + row)
    return raw + sines + cosines


def selection(places, width):
    out = np.zeros((len(places), width), np.float32)
    out[np.arange(len(places)), places] = 1.0
    return out


POS_SELECT = selection(code_places(10, 5), PC)
VIEW_SELECT = selection(code_places(4, 2), VC)


def mm(a, b):
    return lax.dot_general(a, b, (((1,), (0,)), ((), ())), preferred_element_type=jnp.float32)


def mm_nt(a, b):
    return lax.dot_general(a, b, (((1,), (1,)), ((), ())), preferred_element_type=jnp.float32)


def mm_tn(a, b):
    return lax.dot_general(a, b, (((0,), (0,)), ((), ())), preferred_element_type=jnp.float32)


def softplus(v):
    return jnp.maximum(v, jnp.log(1.0 + jnp.exp(jnp.minimum(v, 80.0))))


def row_iota(rows, lanes):
    return lax.broadcasted_iota(jnp.int32, (rows, lanes), 0)


def ray_rows(ray, row):
    o8 = jnp.where(row < 3, ray, jnp.where(row < 6, pltpu.roll(ray, 3, 0), 0.0))
    d8 = jnp.where(row < 3, pltpu.roll(ray, 5, 0), jnp.where(row < 6, ray, 0.0))
    return o8, d8


def center_rows(center_ref, row):
    third = jnp.where(row >= 3, row - 3, row)
    return jnp.where(
        third == 0,
        center_ref[0, 0],
        jnp.where(third == 1, center_ref[0, 1], jnp.where(third == 2, center_ref[0, 2], 0.0)),
    )


def sine_cosine(x):
    turns = jnp.round(x * 0.6366197723675814)
    r = x - turns * 1.5703125
    r = r - turns * 4.837512969970703e-4
    r = r - turns * 7.549789948768648e-8
    q = turns.astype(jnp.int32)
    z = r * r
    sine = r + r * z * (-1.6666654611e-1 + z * (8.3321608736e-3 - z * 1.9515295891e-4))
    cosine = 1.0 - 0.5 * z + z * z * (
        4.166664568298827e-2 + z * (-1.388731625493765e-3 + z * 2.443315711809948e-5)
    )
    odd = (q & 1) == 1
    first = jnp.where(odd, cosine, sine)
    second = jnp.where(odd, sine, cosine)
    return (
        jnp.where((q & 2) == 2, -first, first),
        jnp.where(((q + 1) & 2) == 2, -second, second),
    )


def code_groups(values, doublings):
    groups = [values]
    sine, cosine = sine_cosine(values)
    for step in range(doublings):
        groups += [sine, cosine]
        if step + 1 < doublings:
            sine, cosine = 2.0 * sine * cosine, (cosine - sine) * (cosine + sine)
    groups.append(jnp.zeros_like(values))
    return jnp.concatenate(groups, 0).astype(jnp.bfloat16)


def halves(x):
    return x[:, :TILE], x[:, TILE:]


def over_samples(x):
    return [
        jnp.concatenate([x[:, s * TILE : (s + 1) * TILE], x[:, LANES + s * TILE : LANES + (s + 1) * TILE]], 1)
        for s in range(SAMPLES)
    ]


def by_samples(pieces):
    return jnp.concatenate([halves(p)[h] for h in range(2) for p in pieces], 1)


def composite(small, o8, c8, row):
    density = over_samples(softplus(small))
    rad = over_samples(1.0 / (1.0 + jnp.exp(-small)))
    off = o8 - c8
    off2 = jnp.sum(jnp.where(row < 3, off * off, 0.0), 0, keepdims=True)
    inv = 1.0 / (1.0 + off2)
    depth = jnp.zeros((1, 2 * TILE), jnp.float32)
    before = jnp.ones((1, 2 * TILE), jnp.float32)
    weights, after = [], []
    for s in range(SAMPLES):
        u = density[s][3:4] * SPACING
        weights.append(before * (1.0 - jnp.exp(-u)))
        depth = depth + u
        before = jnp.exp(-depth)
        after.append(before)
    color = sum(w * r for w, r in zip(weights, rad))
    opacity = sum(weights)
    return rad, weights, after, color, (0.1 + opacity) * inv, inv


def list_live(live_ref, slots):
    total = jnp.int32(0)
    for s in range(SLOTS):
        slots[total] = jnp.int32(s)
        total = total + (live_ref[s] > 0).astype(jnp.int32)

    @pl.when(total % 2 == 1)
    def _():
        slots[total] = slots[total - 1]

    return total, (total + 1) // 2


def pair_copies(buf, saved_ref, sem, j, out):
    slot = lax.rem(j, DEEP)
    copies = []
    for n, (lo, hi) in enumerate(((0, 256), (256, 512), (512, 752), (752, R_END))):
        near, far = buf.at[slot, lo:hi], saved_ref.at[j, lo:hi]
        src, dst = (near, far) if out else (far, near)
        copies.append(pltpu.make_async_copy(src, dst, sem.at[slot, n]))
    return copies


def hot_lanes(ids):
    lo, hi = ids & (LO - 1), ids >> 8
    return (row_iota(LO, 2 * TILE) == lo).astype(jnp.float32).astype(jnp.bfloat16), hi


def lane_parts(parts):
    width = 2 * LANES // parts
    return [slice(p * width, (p + 1) * width) for p in range(parts)]


def forward_kernel(
    live_ref, center_ref, rays_ref, pos_ref, trunk_ref, density_ref, feature_ref, view_ref,
    code_ref, radiance_ref, table_ref, pos_select_ref, view_select_ref,
    part_ref, saved_ref, raycode_ref, small_ref,
    wp, wfd, wray, wrad, tab, buf, slots, sem,
):
    row = row_iota(8, 2 * TILE)
    c8 = center_rows(center_ref, row)
    wp[...] = mm_tn(pos_select_ref[...], pos_ref[0]).T.astype(jnp.bfloat16)
    wray[...] = jnp.concatenate(
        [mm_tn(view_select_ref[...], view_ref[0]), code_ref[0].astype(jnp.float32)], 0
    ).T.astype(jnp.bfloat16)
    wfd[:CHID, :] = feature_ref[0]
    row16 = row_iota(16, HID)
    wfd[CHID:, :] = jnp.where(row16 == 3, density_ref[...].astype(jnp.float32), 0.0).astype(jnp.bfloat16)
    wrad[...] = jnp.concatenate(
        [radiance_ref[0].astype(jnp.float32), jnp.zeros((5, CHID), jnp.float32)], 0
    ).astype(jnp.bfloat16)
    for h in range(SLOTS):
        tab[h * E : (h + 1) * E, :] = table_ref[0, :, h * LO : (h + 1) * LO]
    pos_scale = jnp.where(row < 3, 1.0, 32.0)
    view_scale = jnp.where(row < 3, 1.0, 4.0)
    total, pairs = list_live(live_ref, slots)

    def finish_pair(j):
        s0, s1 = slots[2 * j], slots[2 * j + 1]
        o8, _ = ray_rows(jnp.concatenate([rays_ref[s0], rays_ref[s1]], 1), row)
        _, _, _, color, share, _ = composite(small_ref[j], o8, c8, row)
        first, second = halves(jnp.where(row < 3, color * share, share)[:4])
        part_ref[s0] = first
        part_ref[s1] = second

    def pair(j, carry):
        @pl.when(j >= DEEP)
        def _():
            for copy in pair_copies(buf, saved_ref, sem, j - DEEP, True):
                copy.wait()

        out = buf.at[lax.rem(j, DEEP)]
        s0, s1 = slots[2 * j], slots[2 * j + 1]
        ray = jnp.concatenate([rays_ref[s0], rays_ref[s1]], 1)
        o8, d8 = ray_rows(ray, row)
        points = by_samples(
            [(o8 + (t + 0.5) * SPACING * d8 - c8) * pos_scale for t in range(SAMPLES)]
        )
        out[:PC, :] = code_groups(points, 5)
        finish_pair(jnp.maximum(j - 1, 0))
        lanes = lane_parts(PARTS_F)
        for w, lo, mid, hi_row in (
            (wp, 0, R_H1, R_H2), (trunk_ref.at[0, 0], R_H1, R_H2, R_H3), (trunk_ref.at[0, 1], R_H2, R_H3, R_S)
        ):
            for part in lanes:
                out[mid:hi_row, part] = softplus(mm(w[...], out[lo:mid, part])).astype(jnp.bfloat16)
            if mid == GATHER_AFTER:
                hot, hi = hot_lanes(ray[6:7].astype(jnp.int32))
                rows = mm(tab[...], hot)
                picks = [rows[h * E : (h + 1) * E] for h in range(SLOTS)]
                for bit in range(5):
                    on = ((hi >> bit) & 1) == 1
                    picks = [jnp.where(on, b, a) for a, b in zip(picks[::2], picks[1::2])]
                app = picks[0]
                raycode = jnp.concatenate([code_groups(d8 * view_scale, 2), app.astype(jnp.bfloat16)], 0)
                raycode_ref[j] = raycode
                per_ray = mm(wray[...], raycode)
        ray_lanes = by_samples([per_ray] * SAMPLES)
        small = []
        for part in lanes:
            both = mm(wfd[...], out[R_H3:R_S, part])
            shaded = softplus(both[:CHID] + ray_lanes[:, part]).astype(jnp.bfloat16)
            out[R_S:R_END, part] = shaded
            logits = mm(wrad[...], shaded)
            small.append(jnp.where(row_iota(8, logits.shape[1]) == 3, both[CHID : CHID + 8], logits))
        small = jnp.concatenate(small, 1)
        small_ref[j] = small
        for copy in pair_copies(buf, saved_ref, sem, j, True):
            copy.start()
        return carry

    small_ref[0] = jnp.zeros_like(small_ref[0])
    lax.fori_loop(0, pairs, pair, jnp.int32(0))

    @pl.when(pairs > 0)
    def _():
        finish_pair(pairs - 1)

    def drain(j, carry):
        for copy in pair_copies(buf, saved_ref, sem, j, True):
            copy.wait()
        return carry

    lax.fori_loop(jnp.maximum(pairs - DEEP, 0), pairs, drain, jnp.int32(0))


def backward_kernel(
    live_ref, center_ref, rays_ref, cot_ref, saved_ref, raycode_ref, small_ref, trunk_ref,
    density_ref, feature_ref, code_ref, radiance_ref, pos_select_ref, view_select_ref,
    g_ref,
    t1, t2, fdt, radt, dz0, dz1, dz2, dz3, d_logits, g_pos, g_ray, g_rad, buf, slots, sem,
):
    total, pairs = list_live(live_ref, slots)

    def fetch(j, carry):
        for copy in pair_copies(buf, saved_ref, sem, j, False):
            copy.start()
        return carry

    lax.fori_loop(0, jnp.minimum(pairs, DEEP - 1), fetch, jnp.int32(0))
    row = row_iota(8, 2 * TILE)
    lane = lax.broadcasted_iota(jnp.int32, (1, 2 * TILE), 1)
    c8 = center_rows(center_ref, row)

    def flip(x):
        return x.astype(jnp.float32).T.astype(jnp.bfloat16)

    t1[...] = flip(trunk_ref[0, 0])
    t2[...] = flip(trunk_ref[0, 1])
    fdt[:, :CHID] = flip(feature_ref[0])
    row16 = row_iota(16, HID)
    fdt[:, CHID:] = jnp.where(row16 == 3, density_ref[...].astype(jnp.float32), 0.0).T.astype(jnp.bfloat16)
    radt[...] = jnp.concatenate(
        [radiance_ref[0].astype(jnp.float32), jnp.zeros((13, CHID), jnp.float32)], 0
    ).T.astype(jnp.bfloat16)
    g_ref[...] = jnp.zeros_like(g_ref)
    g_pos[...] = jnp.zeros_like(g_pos)
    g_ray[...] = jnp.zeros_like(g_ray)
    g_rad[...] = jnp.zeros_like(g_rad)

    def start_pair(j):
        s0, s1 = slots[2 * j], slots[2 * j + 1]
        ray = jnp.concatenate([rays_ref[s0], rays_ref[s1]], 1)
        o8, _ = ray_rows(ray, row)
        small = small_ref[j]
        rad, weights, after, color, share, inv = composite(small, o8, c8, row)
        cot = jnp.concatenate([cot_ref[s0], cot_ref[s1]], 1)
        cot = jnp.where((lane < TILE) | (2 * j + 1 < total), cot, 0.0)
        cot = jnp.concatenate([cot, jnp.zeros_like(cot)], 0)
        d_share = jnp.sum(
            jnp.where(row < 3, cot * color, jnp.where(row == 3, cot, 0.0)), 0, keepdims=True
        )
        d_color = jnp.where(row < 3, cot * share, 0.0)
        d_opacity = d_share * inv
        sig = rad
        later = jnp.zeros((1, 2 * TILE), jnp.float32)
        pieces = [None] * SAMPLES
        for t in reversed(range(SAMPLES)):
            d_w = jnp.sum(d_color * rad[t], 0, keepdims=True) + d_opacity
            d_u = d_w * after[t] - later
            later = later + d_w * weights[t]
            d_logit = d_color * weights[t] * rad[t] * (1.0 - rad[t])
            pieces[t] = jnp.where(
                row < 3, d_logit, jnp.where(row == 3, d_u * SPACING * sig[t], 0.0)
            )
        d_small = by_samples(pieces)
        d_logits[...] = jnp.concatenate([d_small, jnp.zeros_like(d_small)], 0).astype(jnp.bfloat16)

    @pl.when(pairs > 0)
    def _():
        start_pair(0)

    def pair(j, carry):
        for copy in pair_copies(buf, saved_ref, sem, j, False):
            copy.wait()

        @pl.when(j + DEEP - 1 < pairs)
        def _():
            fetch(j + DEEP - 1, carry)

        act = buf.at[lax.rem(j, DEEP)]
        ray = jnp.concatenate([rays_ref[slots[2 * j]], rays_ref[slots[2 * j + 1]]], 1)
        dz3[CHID:, :] = d_logits[...]

        def through(grad, lo_row, hi_row, part):
            value = act[lo_row:hi_row, part].astype(jnp.float32)
            return grad * (1.0 - jnp.exp(-value))

        lanes = lane_parts(PARTS_B)
        d_feature = []
        for part in lanes:
            piece = through(mm(radt[...], dz3[CHID:, part]), R_S, R_END, part)
            dz3[:CHID, part] = piece.astype(jnp.bfloat16)
            d_feature.append(piece)
        d_ray = sum(over_samples(jnp.concatenate(d_feature, 1))).astype(jnp.bfloat16)
        start_pair(jnp.minimum(j + 1, pairs - 1))
        for wt, src, dst, lo, hi in (
            (fdt, dz3, dz2, R_H3, R_S), (t2, dz2, dz1, R_H2, R_H3), (t1, dz1, dz0, R_H1, R_H2)
        ):
            for part in lanes:
                dst[:, part] = through(mm(wt[...], src[:, part]), lo, hi, part).astype(jnp.bfloat16)
            if src is dz3:
                d_app = mm(code_ref[0], d_ray)
                hot, high = hot_lanes(ray[6:7].astype(jnp.int32))
                spread = jnp.concatenate(
                    [jnp.where(high == h, d_app, 0.0).astype(jnp.bfloat16) for h in range(SLOTS)], 0
                )
                g_ray[...] += mm_nt(d_ray, raycode_ref[j])
                g_rad[...] += mm_nt(act[R_S:R_END, :], dz3[CHID:, :])
                d_both = mm_nt(dz3[...], act[R_H3:R_S, :])
                g_ref[G_FEAT:G_TAB, :] += d_both[:CHID]
                g_ref[G_DEN : G_DEN + 16, 128:256] += d_both[CHID:, :128]
                g_ref[G_DEN + 16 : G_DEN + 32, 128:256] += d_both[CHID:, 128:]
                g_ref[G_TAB:G_POS, :] += mm_nt(spread, hot)
            elif src is dz2:
                g_ref[G_T2:G_FEAT, :] += mm_nt(dz2[...], act[R_H2:R_H3, :])
            else:
                g_ref[G_T1:G_T2, :] += mm_nt(dz1[...], act[R_H1:R_H2, :])
        g_pos[...] += mm_nt(dz0[...], act[:PC, :])
        return carry

    lax.fori_loop(0, pairs, pair, jnp.int32(0))

    def pick(a, select):
        return lax.dot_general(
            select.astype(jnp.float32), a, (((1,), (1,)), ((), ())),
            preferred_element_type=jnp.float32, precision=lax.Precision.HIGHEST,
        )

    g_ref[G_POS : G_POS + 63, :] = pick(g_pos[...], pos_select_ref[...])
    g_ref[G_VIEW : G_VIEW + 27, :128] = pick(g_ray[:, :VC], view_select_ref[...])
    g_ref[G_CODE : G_CODE + E, :128] = g_ray[...].T[VC:]
    g_ref[G_RAD:G_DEN, 128:256] = g_rad[...].T


def unpack_kernel(
    g_ref, got_colors_ref,
    colors_ref, pos_ref, trunk_ref, density_ref, feature_ref, view_ref, code_ref, radiance_ref, table_ref,
):
    colors_ref[...] = got_colors_ref[...]
    for n in range(63):
        pos_ref[n] = g_ref[G_POS + n : G_POS + n + 1, :]
    trunk_ref[0, 0] = g_ref[G_T1:G_T2, :]
    trunk_ref[0, 1] = g_ref[G_T2:G_FEAT, :]
    feature_ref[0] = g_ref[G_FEAT:G_TAB, :]
    density_ref[:, :128] = g_ref[G_DEN + 3 : G_DEN + 4, 128:256]
    density_ref[:, 128:] = g_ref[G_DEN + 19 : G_DEN + 20, 128:256]
    for n in range(27):
        view_ref[n] = g_ref[G_VIEW + n : G_VIEW + n + 1, :128]
    code_ref[0] = g_ref[G_CODE : G_CODE + E, :128]
    for n in range(3):
        radiance_ref[n] = g_ref[G_RAD + n : G_RAD + n + 1, 128:256]
    for h in range(SLOTS):
        table_ref[0, :, h * LO : (h + 1) * LO] = g_ref[G_TAB + h * E : G_TAB + (h + 1) * E, :]


VMEM = pl.BlockSpec(memory_space=pltpu.VMEM)
SMEM = pl.BlockSpec(memory_space=pltpu.SMEM)
ANY = pl.BlockSpec(memory_space=pl.ANY)


def run_forward(live, center, rays, pos, trunk, density, feature, view, code, radiance, table):
    bf = jnp.bfloat16
    return pl.pallas_call(
        forward_kernel,
        name="forward_tiles",
        out_shape=(
            jax.ShapeDtypeStruct((SLOTS, 4, TILE), jnp.float32),
            jax.ShapeDtypeStruct((SLOTS // 2, R_END, 2 * LANES), bf),
            jax.ShapeDtypeStruct((SLOTS // 2, RC, 2 * TILE), bf),
            jax.ShapeDtypeStruct((SLOTS // 2, 8, 2 * LANES), jnp.float32),
        ),
        in_specs=[SMEM, SMEM] + [VMEM] * 11,
        out_specs=(VMEM, ANY, VMEM, VMEM),
        scratch_shapes=[
            pltpu.VMEM((HID, PC), bf),
            pltpu.VMEM((CHID + 16, HID), bf),
            pltpu.VMEM((CHID, RC), bf),
            pltpu.VMEM((8, CHID), bf),
            pltpu.VMEM((SLOTS * E, LO), bf),
            pltpu.VMEM((DEEP, R_END, 2 * LANES), bf),
            pltpu.SMEM((SLOTS + 1,), jnp.int32),
            pltpu.SemaphoreType.DMA((DEEP, 4)),
        ],
        compiler_params=pltpu.CompilerParams(vmem_limit_bytes=40 * 1024 * 1024),
        cost_estimate=pl.CostEstimate(flops=10**10, bytes_accessed=3 * 10**7, transcendentals=0),
    )(live, center, rays, pos, trunk, density, feature, view, code, radiance, table,
      jnp.asarray(POS_SELECT, bf), jnp.asarray(VIEW_SELECT, bf))


def run_backward(live, center, rays, cot, saved, raycode, small, trunk, density, feature, code, radiance):
    bf = jnp.bfloat16
    return pl.pallas_call(
        backward_kernel,
        name="backward_tiles",
        out_shape=jax.ShapeDtypeStruct((G_ROWS, 256), jnp.float32),
        in_specs=[SMEM, SMEM, VMEM, VMEM, ANY] + [VMEM] * 9,
        out_specs=VMEM,
        scratch_shapes=[
            pltpu.VMEM((HID, HID), bf),
            pltpu.VMEM((HID, HID), bf),
            pltpu.VMEM((HID, CHID + 16), bf),
            pltpu.VMEM((CHID, 16), bf),
            pltpu.VMEM((HID, 2 * LANES), bf),
            pltpu.VMEM((HID, 2 * LANES), bf),
            pltpu.VMEM((HID, 2 * LANES), bf),
            pltpu.VMEM((CHID + 16, 2 * LANES), bf),
            pltpu.VMEM((16, 2 * LANES), bf),
            pltpu.VMEM((HID, PC), jnp.float32),
            pltpu.VMEM((CHID, RC), jnp.float32),
            pltpu.VMEM((CHID, 16), jnp.float32),
            pltpu.VMEM((DEEP, R_END, 2 * LANES), bf),
            pltpu.SMEM((SLOTS + 1,), jnp.int32),
            pltpu.SemaphoreType.DMA((DEEP, 4)),
        ],
        compiler_params=pltpu.CompilerParams(vmem_limit_bytes=40 * 1024 * 1024),
        cost_estimate=pl.CostEstimate(flops=2 * 10**10, bytes_accessed=3 * 10**7, transcendentals=0),
    )(live, center, rays, cot, saved, raycode, small, trunk, density, feature, code, radiance,
      jnp.asarray(POS_SELECT, bf), jnp.asarray(VIEW_SELECT, bf))


def run_unpack(packed, colors):
    f32 = jnp.float32
    shapes = [colors.shape, (63, 1, 256), (1, 2, 256, 256), (1, 256), (1, 128, 256), (27, 1, 128),
              (1, 32, 128), (3, 1, 128), (1, 32, 8192)]
    outs = pl.pallas_call(
        unpack_kernel,
        name="unpack_gradients",
        out_shape=tuple(jax.ShapeDtypeStruct(s, f32) for s in shapes),
        in_specs=[VMEM] * 2,
        out_specs=tuple(VMEM for _ in shapes),
        compiler_params=pltpu.CompilerParams(vmem_limit_bytes=32 * 1024 * 1024),
    )(packed, colors)
    colors, pos, trunk, density, feature, view, code, radiance, table = outs
    return (
        colors, pos.transpose(1, 2, 0), trunk, density, feature, view.transpose(1, 2, 0),
        code.transpose(0, 2, 1), radiance.transpose(1, 0, 2), table,
    )


MESH = pl.DeviceIdType.MESH
GROUP = SLOTS
REPS = 4
CHUNK = G_ROWS // (4 * REPS)


def place():
    return lax.axis_index("blk"), lax.axis_index("rep")


def partner(blk, rep, i):
    return lax.rem(blk + i, GROUP), lax.rem(rep + GROUP * REPS - i, REPS)


def meet(blk, rep):
    barrier = pltpu.get_barrier_semaphore()
    for i in range(1, GROUP):
        pl.semaphore_signal(barrier, inc=1, device_id=partner(blk, rep, i), device_id_type=MESH)
    pl.semaphore_wait(barrier, GROUP - 1)


def exchange(blk, rep, src, dst, send_sem, recv_sem):
    for i in range(1, GROUP):
        to_blk, to_rep = partner(blk, rep, i)
        pltpu.make_async_remote_copy(
            src_ref=src.at[to_blk], dst_ref=dst.at[blk], send_sem=send_sem,
            recv_sem=recv_sem, device_id=(to_blk, to_rep), device_id_type=MESH,
        ).start()
    dst[blk] = src[blk]
    most = pl.ds(0, GROUP - 1)
    return pltpu.make_async_remote_copy(
        src_ref=src.at[most], dst_ref=dst.at[most], send_sem=send_sem, recv_sem=recv_sem,
        device_id=partner(blk, rep, 1), device_id_type=MESH,
    )


def finish(everything):
    everything.wait_recv()
    everything.wait_send()


def scatter_kernel(
    tile_ref, live_ref, anchors_ref, directions_ref, codes_ref, out_ref, tiles, send, send_sem, recv_sem
):
    blk, rep = place()
    row = row_iota(8, TILE)
    for t in range(tiles.shape[0]):
        lanes = slice(t * TILE, (t + 1) * TILE)
        tiles[t, 0:3] = anchors_ref[:, lanes]
        tiles[t, 3:6] = directions_ref[:, lanes]
        tiles[t, 6:7] = codes_ref[t : t + 1, :].astype(jnp.float32)
        tiles[t, 7:8] = jnp.zeros((1, TILE), jnp.float32)
    for k in range(GROUP):
        flag = live_ref[k].astype(jnp.float32)
        send[k] = jnp.where(row == 7, flag, tiles[tile_ref[k]])
    meet(blk, rep)
    finish(exchange(blk, rep, send, out_ref, send_sem, recv_sem))


def blend_kernel(
    ids_ref, tile_ref, part_ref, grad_ref, colors_ref, cot_ref,
    back, cots, send, send_sem, recv_sem, send_sem2, recv_sem2,
):
    blk, rep = place()
    meet(blk, rep)
    finish(exchange(blk, rep, part_ref, back, send_sem, recv_sem))
    for t in range(cots.shape[0]):
        summed = back[ids_ref[0, t]] + back[ids_ref[1, t]] + back[ids_ref[2, t]]
        lanes = slice(t * TILE, (t + 1) * TILE)
        colors = summed[:3] / summed[3:4]
        colors_ref[:, lanes] = colors
        cot = grad_ref[:, lanes] * LOSS_SCALE / summed[3:4]
        cots[t] = jnp.concatenate([cot, -jnp.sum(cot * colors, 0, keepdims=True)], 0)
    for k in range(GROUP):
        send[k] = cots[tile_ref[k]]
    finish(exchange(blk, rep, send, cot_ref, send_sem2, recv_sem2))


def total_kernel(g_ref, out_ref, got, held, send_sem, recv_sem):
    blk, rep = place()
    up, down = lax.rem(rep + 1, REPS), lax.rem(rep + REPS - 1, REPS)
    barrier = pltpu.get_barrier_semaphore()
    for other in (up, down):
        pl.semaphore_signal(barrier, inc=1, device_id=(blk, other), device_id_type=MESH)
    pl.semaphore_wait(barrier, 2)
    rings = range(4)

    def chunk(ring, ahead):
        sign = 1 if ring % 2 == 0 else REPS - 1
        which = lax.rem(rep + sign * (ahead + REPS), REPS)
        return pl.ds(pl.multiple_of((ring * REPS + which) * CHUNK, 8), CHUNK)

    def copy(ring, step):
        if step == 0:
            src, dst = g_ref.at[chunk(ring, 0)], got.at[ring, 0]
        elif step < 3:
            src, dst = held.at[ring, step - 1], got.at[ring, step]
        else:
            rows = chunk(ring, 4 - step)
            src, dst = out_ref.at[rows], out_ref.at[rows]
        return pltpu.make_async_remote_copy(
            src_ref=src, dst_ref=dst, send_sem=send_sem.at[ring, step],
            recv_sem=recv_sem.at[ring, step],
            device_id=(blk, up if ring % 2 == 0 else down), device_id_type=MESH,
        )

    for ring in rings:
        copy(ring, 0).start()
    for step in range(6):
        for ring in rings:
            copy(ring, step).wait_recv()
            if step < 2:
                held[ring, step] = got[ring, step] + g_ref[chunk(ring, -step - 1), :]
            elif step == 2:
                out_ref[chunk(ring, 1), :] = got[ring, 2] + g_ref[chunk(ring, 1), :]
            if step < 5:
                copy(ring, step + 1).start()
    for step in range(6):
        for ring in rings:
            copy(ring, step).wait_send()


def communicate(kernel, name, number, args, specs, shapes, scratch):
    return pl.pallas_call(
        kernel,
        name=name,
        out_shape=shapes,
        in_specs=specs,
        out_specs=jax.tree.map(lambda _: VMEM, shapes),
        scratch_shapes=scratch,
        compiler_params=pltpu.CompilerParams(
            collective_id=number, has_side_effects=True, vmem_limit_bytes=16 * 1024 * 1024
        ),
        cost_estimate=pl.CostEstimate(flops=10**10, bytes_accessed=10**6, transcendentals=0),
    )(*args)


def run_scatter(tile_of, live, anchors, directions, codes):
    return communicate(
        scatter_kernel, "scatter_rays", 0, (tile_of, live, anchors, directions, codes),
        [SMEM, SMEM, VMEM, VMEM, VMEM],
        jax.ShapeDtypeStruct((GROUP, 8, TILE), jnp.float32),
        [pltpu.VMEM((codes.shape[0], 8, TILE), jnp.float32), pltpu.VMEM((GROUP, 8, TILE), jnp.float32)] + [pltpu.SemaphoreType.DMA] * 2,
    )


def run_blend(ids, tile_of, part, grad):
    tiles = grad.shape[1] // TILE
    small = (GROUP, 4, TILE)
    return communicate(
        blend_kernel, "blend_colors", 1, (ids, tile_of, part, grad), [SMEM, SMEM, VMEM, VMEM],
        (jax.ShapeDtypeStruct(grad.shape, jnp.float32), jax.ShapeDtypeStruct(small, jnp.float32)),
        [pltpu.VMEM(small, jnp.float32), pltpu.VMEM((tiles, 4, TILE), jnp.float32),
         pltpu.VMEM(small, jnp.float32)] + [pltpu.SemaphoreType.DMA] * 4,
    )


def run_total(packed):
    return communicate(
        total_kernel, "total_gradients", 2, (packed,), [VMEM],
        jax.ShapeDtypeStruct((G_ROWS, 256), jnp.float32),
        [pltpu.VMEM((4, 3, CHUNK, 256), jnp.float32), pltpu.VMEM((4, 2, CHUNK, 256), jnp.float32)]
        + [pltpu.SemaphoreType.DMA((4, 6))] * 2,
    )


def local(
    anchors, directions, app_ids, block_ids, color_grad, block_centers, pos_weight, trunk_weight,
    density_weight, feature_weight, view_weight, code_weight, radiance_weight, code_table,
):
    tiles = block_ids.shape[0]
    ids = block_ids.T
    peers = jnp.arange(SLOTS, dtype=jnp.int32)
    matches = (ids[:, :, None] == peers[None, None, :]).astype(jnp.int32)
    is_live = jnp.sum(matches, (0, 1))
    source_tile = jnp.sum(matches * jnp.arange(tiles, dtype=jnp.int32)[None, :, None], (0, 1))
    rays = run_scatter(source_tile, is_live, anchors, directions, app_ids.reshape(tiles, TILE))
    live = (rays[:, 7, 0] > 0.5).astype(jnp.int32)
    center = block_centers.T
    code = code_weight.transpose(0, 2, 1)
    part, saved, raycode, small = run_forward(
        live, center, rays, pos_weight.transpose(0, 2, 1), trunk_weight, density_weight, feature_weight,
        view_weight.transpose(0, 2, 1), code, radiance_weight, code_table,
    )
    colors, cot = run_blend(ids, source_tile, part, color_grad)
    packed = run_backward(
        live, center, rays, cot, saved, raycode, small, trunk_weight, density_weight,
        feature_weight, code, radiance_weight,
    )
    return run_unpack(run_total(packed), colors)


def solution(mesh):
    weights = (P("blk", None, None), P("blk", None, None, None), P("blk", None)) + (
        P("blk", None, None),
    ) * 5
    ray = P(None, ("blk", "rep"))
    return jax.shard_map(
        local,
        mesh=mesh,
        in_specs=(ray, ray, P(("blk", "rep")), P(("blk", "rep"), None), ray, P(None, "blk")) + weights,
        out_specs=(ray,) + weights,
        check_vma=False,
    )
```
